32 devices in a mesh: sample: 2 (over x), fsdp: 4 (over z), seq: 4 (over y, core).
Axes of the slice: x: 2, y: 2, z: 4, core: 2. Of those that a mesh axis runs over, the one named last changes fastest.
Arguments:
- token_act: bfloat16 [8, 512, 768], P(('sample', 'fsdp'), 'seq'), may hold values from -40 to 40
- token_cond: bfloat16 [8, 512, 768], P(('sample', 'fsdp'), 'seq'), may hold values from -40 to 40
- pair_bias: bfloat16 [16, 512, 512], P('fsdp', 'seq'), may hold values from -8 to 296
- token_mask: int32 [512], P('seq'), may hold values 0 or 1
- ada_weights: bfloat16 [4, 768, 768], P(None, None, 'fsdp'), may hold values from -0.21875 to 0.21875
- attention_in: bfloat16 [4, 768, 768], P(None, None, 'fsdp'), may hold values from -0.21875 to 0.21875
- attention_out: bfloat16 [768, 768], P('fsdp'), may hold values from -0.21875 to 0.21875
- transition_in: bfloat16 [2, 768, 1536], P(None, None, 'fsdp'), may hold values from -0.21875 to 0.21875
- transition_out: bfloat16 [1536, 768], P('fsdp'), may hold values from -0.15625 to 0.15625
- token_vectors: float32 [3, 768], replicated, may hold values from -4 to 4
- atom_skip: bfloat16 [8, 4096, 128], P(('sample', 'fsdp'), 'seq'), may hold values from -40 to 40
- atom_cond: bfloat16 [4096, 128], P('seq'), may hold values from -40 to 40
- atom_bias: bfloat16 [4, 4096, 128], P(None, 'seq'), may hold values from -6 to 296
- window_bounds: int32 [128, 2], P('seq'), may hold values from 0 to 4096, as said below
- atom_token: int32 [4096], P('seq'), may hold values from 0 to 511, as said below
- atom_weights: bfloat16 [7, 128, 128], P(None, None, 'fsdp'), may hold values from -0.5 to 0.5
- token_to_atom: bfloat16 [768, 128], P('fsdp'), may hold values from -0.21875 to 0.21875
- atom_vectors: float32 [2, 128], replicated, may hold values from -4 to 4
- position_out: bfloat16 [3, 128], replicated, may hold values from -0.5 to 0.5
Outputs:
- token_out: bfloat16 [8, 512, 768], P(('sample', 'fsdp'), 'seq')
- position_update: float32 [8, 3, 4096], P(('sample', 'fsdp'), None, 'seq')
The draws below stay inside these ranges and needn't reach their ends.
Inputs may be any that keep to these rules, and one draw needn't show every extreme that they name: `window_bounds`: row b belongs to the atoms 32 * b to 32 * b + 31; column 0 is at least 0 and at least 32 * b - 48, and at most 32 * b; column 1 is at least 32 * b + 32, at most 32 * b + 80 and at most 4096. `atom_token`: atoms are numbered in token order: the value never falls from one atom to the next, the first atom belongs to token 0, the last to token 511, and every token owns 1 to 24 atoms.
All inputs are finite; a program needn't handle non-finite values. No bound on the sum of `token_mask` on one device may be relied on, other than what follows from the above.
Results may differ from the reference program's by a relative error of at most 0.014.
Values may be sent and summed in bfloat16 or wider, within the bound.
A program may use at most 128 MiB of HBM per device.

```python
import math
import jax
import jax.numpy as jnp
from jax import lax

D = 768
H = 16
FF = 1536
CA = 128
HA = 4
WQ = 32
WK = 128
TOKENS = 512
ATOMS = 4096
BLOCKS = 128
SAMPLES = 8
HD = 48


def feature_draw(key, shape):
    base = jnp.clip(jax.random.normal(jax.random.fold_in(key, 11), shape, jnp.float32), -4.0, 4.0)
    return base.astype(jnp.bfloat16)


def draw_token_act(key, part):
    return feature_draw(jax.random.fold_in(key, 101), (SAMPLES, TOKENS, D))


def draw_token_cond(key, part):
    return feature_draw(jax.random.fold_in(key, 102), (SAMPLES, TOKENS, D))


def draw_atom_skip(key, part):
    return feature_draw(jax.random.fold_in(key, 103), (SAMPLES, ATOMS, CA))


def draw_atom_cond(key, part):
    return feature_draw(jax.random.fold_in(key, 104), (ATOMS, CA))


def draw_pair_bias(key, part):
    key = jax.random.fold_in(key, 301)
    values = jnp.clip(2.0 * jax.random.normal(jax.random.fold_in(key, 1), (H, TOKENS, TOKENS), jnp.float32), -8.0, 8.0)
    return values.astype(jnp.bfloat16)


def draw_atom_bias(key, part):
    key = jax.random.fold_in(key, 401)
    values = jnp.clip(1.5 * jax.random.normal(jax.random.fold_in(key, 1), (HA, ATOMS, WK), jnp.float32), -6.0, 6.0)
    return values.astype(jnp.bfloat16)


def draw_window_bounds(key, part):
    key = jax.random.fold_in(key, 501)
    rim_width = (WK - WQ) // 2
    block_start = WQ * jnp.arange(BLOCKS, dtype=jnp.int32)
    lower_end = jnp.maximum(block_start - jax.random.randint(jax.random.fold_in(key, 1), (BLOCKS,), 0, rim_width + 1), 0)
    upper_end = jnp.minimum(block_start + WQ + jax.random.randint(jax.random.fold_in(key, 2), (BLOCKS,), 0, rim_width + 1), ATOMS)
    return jnp.stack([lower_end, upper_end], axis=1).astype(jnp.int32)


def paired_runs(key, pair_count, pair_total):
    first = jax.random.randint(key, (pair_count,), 1, pair_total)
    return jnp.stack([first, pair_total - first], axis=1).reshape(-1).astype(jnp.int32)


def draw_atom_token(key, part):
    key = jax.random.fold_in(key, 601)
    quarter = TOKENS // 4
    group_size = TOKENS // 16
    long_runs = jnp.full((quarter,), 24, jnp.int32)
    middle_runs = paired_runs(jax.random.fold_in(key, 1), quarter // 2, 8)
    short_runs = paired_runs(jax.random.fold_in(key, 2), quarter, 4)
    lengths = jnp.concatenate([long_runs, middle_runs, short_runs]).astype(jnp.int32)
    rest_order = jax.random.permutation(jax.random.fold_in(key, 3), 12).astype(jnp.int32) + 4
    order = jnp.concatenate([jnp.arange(4, dtype=jnp.int32), rest_order]).astype(jnp.int32)
    lengths = jnp.take(lengths.reshape(16, group_size), order, axis=0).reshape(-1).astype(jnp.int32)
    run_ends = jnp.cumsum(lengths)
    marks = jnp.zeros((ATOMS,), jnp.int32).at[run_ends[:-1]].add(1)
    return jnp.cumsum(marks).astype(jnp.int32)


def place_ends(drawn, key, smallest, largest):
    longest = drawn.shape.index(max(drawn.shape))
    spots = []
    for shift in (0, 1):
        where = [jax.random.randint(jax.random.fold_in(key, axis), (), 0, length) for axis, length in enumerate(drawn.shape)]
        where[longest] = (where[longest] + shift) % drawn.shape[longest]
        spots.append(tuple(where))
    return drawn.at[spots[0]].set(smallest).at[spots[1]].set(largest)


def steps_of(key, dims, split, low, largest):
    def one(dim, shards_of):
        steps = jax.random.uniform(jax.random.fold_in(jax.random.fold_in(key, 6), dim), (shards_of,), jnp.float32, low / len(split), largest / len(split))
        return jnp.repeat(jnp.exp(steps), dims[dim] // shards_of).reshape((-1,) + (1,) * (len(dims) - dim - 1))

    loudness = one(*split[0])
    for cut in split[1:]:
        loudness = loudness * one(*cut)
    return loudness


def bell_draw(stream_key, shape, scale, limit, shards=(), kind=jnp.bfloat16):
    values = jax.random.normal(stream_key, shape, jnp.float32) * scale
    if len(shards) > 0:
        values = steps_of(stream_key, shape, shards, -0.22, 0.18) * values
    return jnp.clip(values, min=-limit, max=limit).astype(kind)


def setup_inputs(seed: int = 0) -> dict:
    arg_keys = jax.random.split(jax.random.key(seed), 20)
    token_act = draw_token_act(jax.random.fold_in(arg_keys[19], 71), 0)
    token_cond = draw_token_cond(jax.random.fold_in(arg_keys[19], 71), 0)
    pair_bias = draw_pair_bias(jax.random.fold_in(arg_keys[19], 71), 0)
    token_mask = place_ends((jax.random.randint(arg_keys[3], (TOKENS,), 0, 8) < 7).astype(jnp.int32), jax.random.fold_in(arg_keys[3], 1), 0, 1)
    ada_weights = bell_draw(arg_keys[4], (4, D, D), D ** -0.5, 0.21875, ((2, 4),))
    attention_in = bell_draw(arg_keys[5], (4, D, D), D ** -0.5, 0.21875, ((2, 4),))
    attention_out = bell_draw(arg_keys[6], (D, D), D ** -0.5, 0.21875, ((0, 4),))
    transition_in = bell_draw(arg_keys[7], (2, D, FF), D ** -0.5, 0.21875, ((2, 4),))
    transition_out = bell_draw(arg_keys[8], (FF, D), FF ** -0.5, 0.15625, ((0, 4),))
    token_vectors = bell_draw(arg_keys[9], (3, D), 1.0, 4.0, (), jnp.float32)
    atom_skip = draw_atom_skip(jax.random.fold_in(arg_keys[19], 71), 0)
    atom_cond = draw_atom_cond(jax.random.fold_in(arg_keys[19], 71), 0)
    atom_bias = draw_atom_bias(jax.random.fold_in(arg_keys[19], 71), 0)
    window_bounds = draw_window_bounds(jax.random.fold_in(arg_keys[19], 71), 0)
    atom_token = draw_atom_token(jax.random.fold_in(arg_keys[19], 71), 0)
    atom_weights = bell_draw(arg_keys[15], (7, CA, CA), CA ** -0.5, 0.5, ((2, 4),))
    token_to_atom = bell_draw(arg_keys[16], (D, CA), D ** -0.5, 0.21875, ((0, 4),))
    atom_vectors = bell_draw(arg_keys[17], (2, CA), 1.0, 4.0, (), jnp.float32)
    position_out = bell_draw(arg_keys[18], (3, CA), CA ** -0.5, 0.5)
    return {"token_act": token_act, "token_cond": token_cond, "pair_bias": pair_bias, "token_mask": token_mask, "ada_weights": ada_weights, "attention_in": attention_in, "attention_out": attention_out, "transition_in": transition_in, "transition_out": transition_out, "token_vectors": token_vectors, "atom_skip": atom_skip, "atom_cond": atom_cond, "atom_bias": atom_bias, "window_bounds": window_bounds, "atom_token": atom_token, "atom_weights": atom_weights, "token_to_atom": token_to_atom, "atom_vectors": atom_vectors, "position_out": position_out}


EPS = 1e-05
FAR = -1e+30

def layer_norm(values):
    values = values.astype(jnp.float32)
    center = values - lax.optimization_barrier(jnp.mean(values, axis=-1, keepdims=True))
    spread = lax.optimization_barrier(jnp.mean(center * center, axis=-1, keepdims=True))
    return center * lax.rsqrt(spread + EPS)

def matmul(left_side, right_side):
    return jnp.dot(left_side, right_side, preferred_element_type=jnp.float32)

def adaptive(values, normed_cond, scale_weight, shift_weight, offset):
    return jax.nn.sigmoid(matmul(normed_cond, scale_weight) + offset) * layer_norm(values) + matmul(normed_cond, shift_weight)

def window_attention(queries, pairs, bias_rows, bounds):
    atom_count, feature_count = queries.shape
    block_count = atom_count // WQ
    step_count = WK // WQ
    rim_width = (WK - WQ) // 2
    head_width = feature_count // HA
    padded = jnp.pad(pairs, ((rim_width, rim_width), (0, 0)))
    tile_rows = padded.reshape(block_count + step_count - 1, WQ, 2 * feature_count)
    windows = jnp.concatenate([tile_rows[position:position + block_count] for position in range(step_count)], axis=1)
    key_rows = windows[:, :, :feature_count].reshape(block_count, WK, HA, head_width)
    value_rows = windows[:, :, feature_count:].reshape(block_count, WK, HA, head_width)
    query_rows = queries.reshape(block_count, WQ, HA, head_width)
    scores = jnp.einsum('bqhd,bkhd->hbqk', query_rows.astype(jnp.float32), key_rows.astype(jnp.float32)) * (1.0 / math.sqrt(head_width))
    scores = scores + bias_rows.reshape(HA, block_count, WQ, WK).astype(jnp.float32)
    slot_atoms = WQ * jnp.arange(block_count, dtype=jnp.int32)[:, None] - rim_width + jnp.arange(WK, dtype=jnp.int32)[None, :]
    in_window = (slot_atoms >= bounds[:, 0:1]) & (slot_atoms < bounds[:, 1:2])
    scores = jnp.where(in_window[None, :, None, :], scores, FAR)
    maxima = lax.optimization_barrier(jnp.max(scores, axis=-1, keepdims=True))
    weights = jnp.exp(scores - maxima)
    totals = lax.optimization_barrier(jnp.sum(weights, axis=-1))
    attended = jnp.einsum('hbqk,bkhd->bqhd', weights.astype(jnp.bfloat16).astype(jnp.float32), value_rows.astype(jnp.float32))
    attended = attended / jnp.transpose(totals, (1, 2, 0))[..., None]
    return attended.reshape(atom_count, feature_count)

def reference(token_act, token_cond, pair_bias, token_mask, ada_weights, attention_in, attention_out, transition_in, transition_out, token_vectors, atom_skip, atom_cond, atom_bias, window_bounds, atom_token, atom_weights, token_to_atom, atom_vectors, position_out):
    cond_normed = layer_norm(token_cond).astype(jnp.bfloat16)
    attend_x = adaptive(token_act, cond_normed, ada_weights[0], ada_weights[1], token_vectors[0]).astype(jnp.bfloat16)
    transit_x = adaptive(token_act, cond_normed, ada_weights[2], ada_weights[3], token_vectors[1]).astype(jnp.bfloat16)
    query_rows = (matmul(attend_x, attention_in[0]) + token_vectors[2]).astype(jnp.bfloat16)
    key_rows = matmul(attend_x, attention_in[1]).astype(jnp.bfloat16)
    value_rows = matmul(attend_x, attention_in[2]).astype(jnp.bfloat16)
    gate_rows = matmul(attend_x, attention_in[3]).astype(jnp.bfloat16)
    query_heads = query_rows.reshape(SAMPLES, TOKENS, H, HD)
    key_heads = key_rows.reshape(SAMPLES, TOKENS, H, HD)
    value_heads = value_rows.reshape(SAMPLES, TOKENS, H, HD)
    live_keys = token_mask > 0
    score_scale = 1.0 / math.sqrt(HD)

    def one_head(combined):
        sample = (combined // H).astype(jnp.int32)
        head_id = (combined % H).astype(jnp.int32)
        query_one = lax.dynamic_index_in_dim(lax.dynamic_index_in_dim(query_heads, sample, 0, False), head_id, 1, False)
        key_one = lax.dynamic_index_in_dim(lax.dynamic_index_in_dim(key_heads, sample, 0, False), head_id, 1, False)
        value_one = lax.dynamic_index_in_dim(lax.dynamic_index_in_dim(value_heads, sample, 0, False), head_id, 1, False)
        bias_one = lax.dynamic_index_in_dim(pair_bias, head_id, 0, False).astype(jnp.float32)
        scores = jnp.dot(query_one, key_one.T, preferred_element_type=jnp.float32) * score_scale + bias_one
        scores = jnp.where(live_keys[None, :], scores, FAR)
        maxima = lax.optimization_barrier(jnp.max(scores, axis=-1, keepdims=True))
        weights = jnp.exp(scores - maxima)
        totals = lax.optimization_barrier(jnp.sum(weights, axis=-1, keepdims=True))
        return matmul(weights.astype(jnp.bfloat16), value_one) / totals
    head_outputs = lax.map(one_head, jnp.arange(SAMPLES * H, dtype=jnp.int32))
    attended = head_outputs.reshape(SAMPLES, H, TOKENS, HD).transpose(0, 2, 1, 3).reshape(SAMPLES, TOKENS, D)
    gated = (attended * jax.nn.sigmoid(gate_rows.astype(jnp.float32))).astype(jnp.bfloat16)
    hidden = (jax.nn.silu(matmul(transit_x, transition_in[0])) * matmul(transit_x, transition_in[1])).astype(jnp.bfloat16)
    token_out = (token_act.astype(jnp.float32) + matmul(gated, attention_out) + matmul(hidden, transition_out)).astype(jnp.bfloat16)
    token_rows = matmul(token_out, token_to_atom).astype(jnp.bfloat16)
    atom_state = atom_skip.astype(jnp.float32) + jnp.take(token_rows, atom_token, axis=1).astype(jnp.float32)
    atom_normed = layer_norm(atom_cond).astype(jnp.bfloat16)
    atom_x = adaptive(atom_state, atom_normed, atom_weights[0], atom_weights[1], atom_vectors[0]).astype(jnp.bfloat16)
    atom_query = (matmul(atom_x, atom_weights[2]) + atom_vectors[1]).astype(jnp.bfloat16)
    atom_key = matmul(atom_x, atom_weights[3]).astype(jnp.bfloat16)
    atom_value = matmul(atom_x, atom_weights[4]).astype(jnp.bfloat16)
    atom_gate = matmul(atom_x, atom_weights[5]).astype(jnp.bfloat16)
    pairs = jnp.concatenate([atom_key, atom_value], axis=-1)

    def one_sample(operands):
        return window_attention(operands[0], operands[1], atom_bias, window_bounds)
    atom_attended = lax.map(one_sample, (atom_query, pairs))
    atom_gated = (atom_attended * jax.nn.sigmoid(atom_gate.astype(jnp.float32))).astype(jnp.bfloat16)
    atom_new = atom_state + matmul(atom_gated, atom_weights[6])
    final_normed = layer_norm(atom_new).astype(jnp.bfloat16)
    position_update = jnp.einsum('ck,sak->sca', position_out.astype(jnp.float32), final_normed.astype(jnp.float32))
    return (token_out, position_update)
```

```python
import functools
import math
import types

import jax
import jax.numpy as jnp
from jax import lax
from jax.experimental import pallas as pl
from jax.experimental.pallas import tpu as pltpu
from jax.sharding import PartitionSpec as P

HA = 4
WQ = 32
WK = 128
HD = 48
EPS = 1e-05
FAR = -1e30
RIM = (WK - WQ) // 2
VMEM_LIMIT = 56 * 1024 * 1024
MESH = pl.DeviceIdType.MESH


def layer_norm(values):
    values = values.astype(jnp.float32)
    center = values - jnp.mean(values, axis=-1, keepdims=True)
    spread = jnp.mean(center * center, axis=-1, keepdims=True)
    return center * lax.rsqrt(spread + EPS)


def matmul(left_side, right_side):
    return jnp.dot(left_side, right_side, preferred_element_type=jnp.float32)


def matmul_t(left_side, right_side):
    return lax.dot_general(
        left_side, right_side, (((1,), (1,)), ((), ())), preferred_element_type=jnp.float32
    )


def pack(array):
    half = array.shape[-2] // 2
    return jnp.concatenate([array[..., :half, :], array[..., half:, :]], axis=-1)


def unpack(array):
    half = array.shape[-1] // 2
    return jnp.concatenate([array[..., :half], array[..., half:]], axis=-2)


def remote(source, target, send, recv, axis, peer):
    return pltpu.make_async_remote_copy(
        src_ref=source, dst_ref=target, send_sem=send, recv_sem=recv,
        device_id={axis: peer}, device_id_type=MESH,
    )


class Chain:
    def __init__(self, axis, size, view, send, recv, prefix):
        self.axis, self.size, self.view = axis, size, view
        self.send, self.recv, self.prefix = send, recv, prefix
        self.here = lax.axis_index(axis)

    def guards(self, side, step):
        here, last = self.here, self.size - 1
        if side == 0:
            return (here - step >= 0) & (here < last), here - 1 - step >= 0
        return (here + step <= last) & (here > 0), here + 1 + step <= last

    def copy(self, side, step, arriving):
        sign = 1 if side == 0 else -1
        block = self.view(self.here - sign * (step + (1 if arriving else 0)))
        at = self.prefix + (side, step)
        return remote(block, block, self.send.at[at], self.recv.at[at], self.axis, self.here + sign)

    def begin(self):
        for side in (0, 1):

            @pl.when(self.guards(side, 0)[0])
            def _():
                self.copy(side, 0, False).start()

    def arrive(self, step):
        for side in (0, 1):
            comes = self.guards(side, step)[1]

            @pl.when(comes)
            def _():
                self.copy(side, step, True).wait_recv()

            if step + 1 < self.size - 1:

                @pl.when(self.guards(side, step + 1)[0])
                def _():
                    self.copy(side, step + 1, False).start()

    def drain(self):
        for side in (0, 1):
            for step in range(self.size - 1):

                @pl.when(self.guards(side, step)[0])
                def _():
                    self.copy(side, step, False).wait_send()


class Pairs:
    def __init__(self, axis, size, view, send, recv, partner_send, partner_recv, prefix):
        self.axis, self.view, self.prefix = axis, view, prefix
        self.send, self.recv = send, recv
        self.partner_send, self.partner_recv = partner_send, partner_recv
        self.index = lax.axis_index(axis)
        self.length = size // 2
        self.position = self.index // 2
        self.parity = self.index - 2 * self.position

    def slot(self, position):
        return position * 2 + self.parity

    def partner(self):
        return self.index + 1 - 2 * self.parity

    def guards(self, side, step):
        here, last = self.position, self.length - 1
        if side == 0:
            return (here - step >= 0) & (here < last), here - 1 - step >= 0
        return (here + step <= last) & (here > 0), here + 1 + step <= last

    def copy(self, side, step, arriving):
        sign = 1 if side == 0 else -1
        block = self.view(self.slot(self.position - sign * (step + (1 if arriving else 0))))
        at = self.prefix + (side, step)
        return remote(
            block, block, self.send.at[at], self.recv.at[at], self.axis,
            self.slot(self.position + sign),
        )

    def hand(self, key, origin, arriving):
        block = self.view(origin * 2 + 1 - self.parity if arriving else self.slot(origin))
        at = self.prefix + (key,)
        return remote(
            block, block, self.partner_send.at[at], self.partner_recv.at[at], self.axis, self.partner()
        )

    def greet(self, signal):
        above, below = self.position > 0, self.position < self.length - 1

        @pl.when(above)
        def _():
            signal(self.axis, self.slot(self.position - 1))

        @pl.when(below)
        def _():
            signal(self.axis, self.slot(self.position + 1))

        signal(self.axis, self.partner())
        return jnp.where(above, 1, 0) + jnp.where(below, 1, 0) + 1

    def begin(self):
        for side in (0, 1):

            @pl.when(self.guards(side, 0)[0])
            def _():
                self.copy(side, 0, False).start()

        self.hand(0, self.position, False).start()

    def key(self, side, step):
        return 1 + side * (self.length - 1) + step

    def origin(self, side, step):
        return self.position - (step + 1) if side == 0 else self.position + step + 1

    def relay(self):
        for step in range(self.length - 1):
            for side in (0, 1):

                @pl.when(self.guards(side, step)[1])
                def _():
                    self.copy(side, step, True).wait_recv()
                    self.hand(self.key(side, step), self.origin(side, step), False).start()

                if step + 1 < self.length - 1:

                    @pl.when(self.guards(side, step + 1)[0])
                    def _():
                        self.copy(side, step + 1, False).start()

    def complete(self):
        self.hand(0, self.position, False).wait_send()
        self.hand(0, self.position, True).wait_recv()
        for step in range(self.length - 1):
            for side in (0, 1):
                goes, comes = self.guards(side, step)

                @pl.when(goes)
                def _():
                    self.copy(side, step, False).wait_send()

                @pl.when(comes)
                def _():
                    self.hand(self.key(side, step), self.origin(side, step), False).wait_send()
                    self.hand(self.key(side, step), self.origin(side, step), True).wait_recv()


def token_kernel(names, groups, ring, *refs):
    r = types.SimpleNamespace(**dict(zip(names, refs)))
    me, seat = lax.axis_index("fsdp"), lax.axis_index("seq")
    rows, depth = r.act.shape
    width = r.ada.shape[1]
    heads = r.bias.shape[0]
    half = rows // 2
    last = groups - 1
    barrier = pltpu.get_barrier_semaphore()

    def signal(axis, target):
        pl.semaphore_signal(barrier, inc=1, device_id={axis: target}, device_id_type=MESH)

    loads = {
        name: pltpu.make_async_copy(getattr(r, name + "_hbm"), getattr(r, name), r.load.at[number])
        for number, name in enumerate(("ada", "attn", "bias", "out", "tin", "tout"))
    }

    def pairs(view, *prefix):
        return Pairs("seq", ring, view, r.seq_send, r.seq_recv, r.hand_send, r.hand_recv, prefix)

    halos = [
        Halo("seq", ring, r.rim, r.rim_all, r.halo_send.at[0], r.halo_recv.at[0]),
        Halo("seq", ring, r.owner, r.owner_all, r.halo_send.at[1], r.halo_recv.at[1]),
    ]
    kv_flows = [pairs(lambda slot, g=g: r.kv.at[slot, g], g) for g in range(groups)]
    mask_flow = pairs(lambda slot: r.masks.at[slot], groups)
    rows_flow = pairs(lambda slot: r.rows_all.at[slot], groups + 1)

    for shift in range(1, groups):
        signal("fsdp", lax.rem(me + shift, groups))
    expected = last + mask_flow.greet(signal) + halos[0].greet(barrier)
    for load in loads.values():
        load.start()

    def chain(number, view):
        return Chain("fsdp", groups, view, r.line_send, r.line_recv, (number,))

    cond_chains = [
        chain(part, lambda slot, part=part: r.conds.at[slot, pl.ds(part * half, half)]) for part in (0, 1)
    ]
    attend_chains = [chain(2 + g, lambda slot, g=g: r.attend.at[slot, g]) for g in range(groups)]
    transit_chains = [
        chain(2 + groups + g, lambda slot, g=g: r.transit.at[slot, g]) for g in range(groups)
    ]
    parity = seat - 2 * (seat // 2)
    atom_half, project_half = r.atom_part.shape[0] // 2, r.project_part.shape[0] // 2
    atom_rows = pl.ds(pl.multiple_of(parity * atom_half, 16), atom_half)
    project_rows = pl.ds(pl.multiple_of(parity * project_half, 16), project_half)
    small_chains = [
        chain(2 + 2 * groups, lambda slot: r.atom_all.at[slot, atom_rows]),
        chain(3 + 2 * groups, lambda slot: r.project.at[slot, project_rows]),
    ]

    def swaps():
        partner = seat + 1 - 2 * parity
        blocks = (r.atom_all.at[:, atom_rows], r.project.at[:, project_rows])
        return [
            remote(block, block, r.swap_send.at[i], r.swap_recv.at[i], "seq", partner)
            for i, block in enumerate(blocks)
        ]

    r.conds[me] = layer_norm(r.cond[...]).astype(jnp.bfloat16)
    r.masks[seat] = r.mask[...]
    r.atom_all[me, atom_rows] = r.atom_part[atom_rows, :]
    r.project[me, project_rows] = r.project_part[project_rows, :]
    pl.semaphore_wait(barrier, expected)
    for flow in cond_chains:
        flow.begin()
    act_normed = layer_norm(r.act[...]).astype(jnp.bfloat16)
    for g in range(groups):
        r.act_out[g] = pack(act_normed[:, g * width : (g + 1) * width])

    def slots(shift, arriving):
        peer = lax.rem(me + shift, groups)
        landing = lax.rem(me + groups - shift, groups) if arriving else me
        return remote(
            r.act_out.at[peer], r.acts.at[landing], r.act_send.at[shift], r.act_recv.at[shift],
            "fsdp", peer,
        )

    for shift in range(1, groups):
        slots(shift, False).start()
    mask_flow.begin()
    for halo in halos:
        halo.begin()
    offsets = r.vectors[me]

    def adaptive(sample, packed):
        rows_in = r.conds[sample]
        values = unpack(packed).astype(jnp.float32)

        def one(scale, shift, vector):
            gate = jax.nn.sigmoid(matmul_t(rows_in, r.ada[scale]) + offsets[vector : vector + 1, :])
            return pack((gate * values + matmul_t(rows_in, r.ada[shift])).astype(jnp.bfloat16))

        r.attend[me, sample] = one(0, 1, 0)
        r.transit[me, sample] = one(2, 3, 1)

    loads["ada"].wait()
    adaptive(me, r.act_out[me])
    inner = sorted(range(groups), key=lambda g: max(g, last - g))
    outer = sorted(range(groups), key=lambda g: (-max(g, last - g), g))
    for step in range(last):
        for flow in cond_chains:
            flow.arrive(step)
        for side in (0, 1):

            @pl.when(cond_chains[0].guards(side, step)[1])
            def _():
                origin = me - (step + 1) if side == 0 else me + step + 1
                slots(step + 1 if side == 0 else last - step, True).wait_recv()
                adaptive(origin, r.acts[origin])

        for g in inner:
            if max(g, last - g) == step + 1:
                attend_chains[g].begin()

    def joined(ref, g):
        return jnp.concatenate([unpack(ref[origin, g]) for origin in range(groups)], axis=1)

    def projections(g):
        full = joined(r.attend, g)
        r.queries[g] = (matmul_t(full, r.attn[0]) + offsets[2:3, :]).astype(jnp.bfloat16)
        both = r.attn[1:3].reshape(2 * width, depth)
        r.kv[seat, g] = matmul_t(full, both).astype(jnp.bfloat16)
        kv_flows[g].begin()
        r.gates[g] = matmul_t(full, r.attn[3]).astype(jnp.bfloat16)

    for step in range(last - 1):
        for g in inner:
            attend_chains[g].arrive(step)
    for g in outer:
        transit_chains[g].begin()
    loads["attn"].wait()
    for g in inner:
        attend_chains[g].arrive(last - 1)
        projections(g)
    for flow in small_chains:
        flow.begin()

    def attention(g):
        queries = r.queries[g]
        head_of = lax.broadcasted_iota(jnp.int32, (rows, width), 1) // HD
        stacked = jnp.concatenate(
            [jnp.where(head_of == head, queries, 0).astype(jnp.bfloat16) for head in range(heads)], axis=0
        )
        scale = 1.0 / math.sqrt(HD)
        span = min(max(512 // rows, 1), ring)

        def block(first, state):
            keys = jnp.concatenate([r.kv[first + i, g, :, :width] for i in range(span)], axis=0)
            values = jnp.concatenate([r.kv[first + i, g, :, width:] for i in range(span)], axis=0)
            live = jnp.concatenate([r.masks[first + i] for i in range(span)], axis=1)
            columns = pl.ds(pl.multiple_of(first * rows, span * rows), span * rows)
            bias = r.bias[:, :, columns].reshape(heads * rows, span * rows).astype(jnp.float32)
            scores = matmul_t(stacked, keys) * scale + bias
            scores = jnp.where(live > 0, scores, FAR)
            block_max = jnp.max(scores, axis=-1, keepdims=True)
            new_maxima = block_max if state is None else jnp.maximum(state[0], block_max)
            weights = jnp.exp(scores - new_maxima)
            totals = jnp.sum(weights, axis=-1, keepdims=True)
            summed = matmul(weights.astype(jnp.bfloat16), values)
            if state is not None:
                factor = jnp.exp(state[0] - new_maxima)
                totals, summed = state[1] * factor + totals, state[2] * factor + summed
            return new_maxima, totals, summed

        state = block(0, None)
        if ring > span:
            state = lax.fori_loop(1, ring // span, lambda i, state: block(i * span, state), state)
        attended = state[2] / state[1]
        result = jnp.zeros((rows, width), jnp.float32)
        for head in range(heads):
            result = result + jnp.where(head_of == head, attended[head * rows : (head + 1) * rows], 0.0)
        gate = jax.nn.sigmoid(r.gates[g].astype(jnp.float32))
        r.gated[g] = (result * gate).astype(jnp.bfloat16)

    pending = [(transit_chains[g], step) for step in range(last - 1) for g in outer]
    pending += [(flow, step) for step in range(last - 1) for flow in small_chains]
    share = -(-len(pending) // groups)
    mask_flow.relay()
    mask_flow.complete()
    loads["bias"].wait()
    kv_flows[inner[0]].relay()
    for number, g in enumerate(inner):
        if number + 1 < groups:
            kv_flows[inner[number + 1]].relay()
        kv_flows[g].complete()
        attention(g)
        for flow, step in pending[number * share : (number + 1) * share]:
            flow.arrive(step)

    def hop(side, g, part):
        piece = pl.ds(part * half, half)
        at = (side, g, part)
        return remote(
            r.sums_out.at[g, piece], r.sums_in.at[side, g, piece], r.sum_send.at[at], r.sum_recv.at[at],
            "fsdp", me + (1 if side == 0 else -1),
        )

    def take(side, g, part):
        hop(side, g, part).wait_recv()
        piece = pl.ds(part * half, half)
        r.total[g, piece] += r.sums_in[side, g, piece].astype(jnp.float32)

    def reduce(stage, g):
        for side, here, goes in ((0, stage, g > stage), (1, last - stage, g < last - stage)):
            if goes:

                @pl.when(me == here)
                def _():
                    for part in (0, 1):
                        piece = pl.ds(part * half, half)
                        if stage > 0:
                            take(side, g, part)
                        r.sums_out[g, piece] = r.total[g, piece].astype(jnp.bfloat16)
                        hop(side, g, part).start()

    for name in ("out", "tin", "tout"):
        loads[name].wait()
    for g in outer:
        transit_chains[g].arrive(last - 1)
        full = joined(r.transit, g)
        hidden = jax.nn.silu(matmul(full, r.tin[0])) * matmul(full, r.tin[1])
        r.total[g] = matmul(r.gated[g], r.out[...]) + matmul(hidden.astype(jnp.bfloat16), r.tout[...])
        reduce(0, g)
    for flow in small_chains:
        flow.arrive(last - 1)
    for copy in swaps():
        copy.start()
    for stage in range(1, last):
        for g in outer:
            reduce(stage, g)
    for copy in swaps():
        copy.wait()
    for side, present in ((0, me > 0), (1, me < last)):

        @pl.when(present)
        def _():
            for part in (0, 1):
                take(side, me, part)

    token = (r.act[...].astype(jnp.float32) + r.total[me]).astype(jnp.bfloat16)
    r.token[...] = token
    r.rows_all[seat] = matmul(token, r.project[...].reshape(depth, -1)).astype(jnp.bfloat16)
    rows_flow.begin()
    for flow in cond_chains + attend_chains + transit_chains + small_chains:
        flow.drain()
    for shift in range(1, groups):
        slots(shift, False).wait_send()
    for halo in halos:
        halo.finish()
    for g in range(groups):
        for side, goes in ((0, g > me), (1, g < me)):

            @pl.when(goes)
            def _():
                for part in (0, 1):
                    hop(side, g, part).wait_send()

    rows_flow.relay()
    rows_flow.complete()


def token_layer(
    act, cond, mask, vectors, rim, owner, atom_part, project_part, bias, ada, attn, out, tin, tout
):
    groups, ring = lax.axis_size("fsdp"), lax.axis_size("seq")
    rows, depth = act.shape
    width = ada.shape[1]
    dma = pltpu.SemaphoreType.DMA
    vmem, far = pl.BlockSpec(memory_space=pltpu.VMEM), pl.BlockSpec(memory_space=pl.ANY)
    half_type = jnp.bfloat16
    near = dict(
        act=act, cond=cond, mask=mask, vectors=vectors, rim=rim, owner=owner,
        atom_part=atom_part, project_part=project_part,
    )
    weights = dict(ada=ada, attn=attn, bias=bias, out=out, tin=tin, tout=tout)
    outs = dict(
        token=((rows, depth), half_type),
        rows_all=((ring, rows, project_part.shape[1]), half_type),
        rim_all=(rim.shape, rim.dtype),
        owner_all=(owner.shape, owner.dtype),
        atom_all=((groups,) + atom_part.shape, half_type),
    )
    packed = (groups, groups, rows // 2, 2 * width)
    chains = 4 + 2 * groups
    hops = max(groups - 1, 1)
    length = ring // 2
    scratch = {name: pltpu.VMEM(array.shape, array.dtype) for name, array in weights.items()}
    scratch |= dict(
        conds=pltpu.VMEM((groups, rows, depth), half_type),
        act_out=pltpu.VMEM(packed[1:], half_type),
        acts=pltpu.VMEM(packed[1:], half_type),
        attend=pltpu.VMEM(packed, half_type),
        transit=pltpu.VMEM(packed, half_type),
        queries=pltpu.VMEM((groups, rows, width), half_type),
        gates=pltpu.VMEM((groups, rows, width), half_type),
        gated=pltpu.VMEM((groups, rows, width), half_type),
        kv=pltpu.VMEM((ring, groups, rows, 2 * width), half_type),
        masks=pltpu.VMEM((ring, 1, rows), jnp.int32),
        project=pltpu.VMEM((groups,) + project_part.shape, half_type),
        total=pltpu.VMEM((groups, rows, depth), jnp.float32),
        sums_out=pltpu.VMEM((groups, rows, depth), half_type),
        sums_in=pltpu.VMEM((2, groups, rows, depth), half_type),
        load=dma((len(weights),)),
        line_send=dma((chains, 2, hops)),
        line_recv=dma((chains, 2, hops)),
        act_send=dma((groups,)),
        act_recv=dma((groups,)),
        seq_send=dma((groups + 2, 2, max(length - 1, 1))),
        seq_recv=dma((groups + 2, 2, max(length - 1, 1))),
        hand_send=dma((groups + 2, 2 * length)),
        hand_recv=dma((groups + 2, 2 * length)),
        halo_send=dma((2, 2)),
        halo_recv=dma((2, 2)),
        swap_send=dma((2,)),
        swap_recv=dma((2,)),
        sum_send=dma((2, groups, 2)),
        sum_recv=dma((2, groups, 2)),
    )
    names = list(near) + [name + "_hbm" for name in weights] + list(outs) + list(scratch)
    results = pl.pallas_call(
        functools.partial(token_kernel, tuple(names), groups, ring),
        out_shape=tuple(jax.ShapeDtypeStruct(*out) for out in outs.values()),
        in_specs=[vmem] * len(near) + [far] * len(weights),
        out_specs=tuple([vmem] * len(outs)),
        scratch_shapes=list(scratch.values()),
        compiler_params=pltpu.CompilerParams(
            collective_id=1, has_side_effects=True, vmem_limit_bytes=VMEM_LIMIT
        ),
        name="token_layer",
    )(*near.values(), *weights.values())
    return results


class Halo:
    def __init__(self, axis, size, block, out, send, recv):
        self.axis, self.size, self.block, self.out = axis, size, block, out
        self.send, self.recv = send, recv
        self.index = lax.axis_index(axis)
        self.above, self.below = self.index > 0, self.index < size - 1

    def greet(self, barrier):
        for present, target in ((self.above, self.index - 1), (self.below, self.index + 1)):

            @pl.when(present)
            def _():
                pl.semaphore_signal(
                    barrier, inc=1, device_id={self.axis: target}, device_id_type=MESH
                )

        return jnp.where(self.above, 1, 0) + jnp.where(self.below, 1, 0)

    def copy(self, side):
        return pltpu.make_async_remote_copy(
            src_ref=self.block.at[side],
            dst_ref=self.out.at[1 - side],
            send_sem=self.send.at[side],
            recv_sem=self.recv.at[side],
            device_id={self.axis: self.index - 1 + 2 * side},
            device_id_type=MESH,
        )

    def begin(self):
        for side, present in ((0, self.above), (1, self.below)):

            @pl.when(present)
            def _():
                self.copy(side).start()

            @pl.when(jnp.logical_not(present))
            def _():
                self.out[side] = jnp.zeros(self.out.shape[1:], self.out.dtype)

    def steps(self):
        return 0

    def finish(self):
        for side, present in ((0, self.above), (1, self.below)):

            @pl.when(present)
            def _():
                self.copy(side).wait_send()
                self.copy(1 - side).wait_recv()


def atom_kernel(
    first_ref, bounds_ref, rows_ref, skip_ref, cond_ref, rim_ref, token_ref, weight_ref, vector_ref,
    position_ref, bias_ref, out_ref, state_ref, query_ref, gate_ref, key_ref, value_ref, held_ref,
):
    count, channels = query_ref.shape
    head_width = channels // HA
    tokens = rows_ref.shape[0]
    chunk = min(512, tokens)
    inner = pl.ds(RIM, count)
    owners = token_ref[...]
    taken = jnp.zeros((owners.shape[0], channels), jnp.float32)
    for start in range(0, tokens, chunk):
        column = lax.broadcasted_iota(jnp.int32, (owners.shape[0], chunk), 1) + start
        hit = jnp.where(owners == column, 1.0, 0.0).astype(jnp.bfloat16)
        taken = taken + matmul(hit, rows_ref[start : start + chunk, :])
    skip = jnp.concatenate([rim_ref[0, :, :channels], skip_ref[...], rim_ref[1, :, :channels]], axis=0)
    cond = jnp.concatenate([rim_ref[0, :, channels:], cond_ref[...], rim_ref[1, :, channels:]], axis=0)
    state = skip.astype(jnp.float32) + taken
    state_ref[...] = state
    normed = layer_norm(cond).astype(jnp.bfloat16)
    atom_x = (
        jax.nn.sigmoid(matmul_t(normed, weight_ref[0]) + vector_ref[0:1, :]) * layer_norm(state)
        + matmul_t(normed, weight_ref[1])
    ).astype(jnp.bfloat16)
    own_x = atom_x[RIM : RIM + count, :]
    query_ref[...] = (matmul_t(own_x, weight_ref[2]) + vector_ref[1:2, :]).astype(jnp.bfloat16)
    gate_ref[...] = matmul_t(own_x, weight_ref[5]).astype(jnp.bfloat16)
    key_ref[...] = matmul_t(atom_x, weight_ref[3]).astype(jnp.bfloat16)
    value_ref[...] = matmul_t(atom_x, weight_ref[4]).astype(jnp.bfloat16)
    head_of = lax.broadcasted_iota(jnp.int32, (WQ, channels), 1) // head_width
    lane = lax.broadcasted_iota(jnp.int32, (1, WK), 1)
    scale = 1.0 / math.sqrt(head_width)

    def windows(step, carry):
        scores = []
        bases = [pl.multiple_of(step * (BATCH * WQ) + i * WQ, WQ) for i in range(BATCH)]
        for i, base in enumerate(bases):
            queries = query_ref[pl.ds(base, WQ), :]
            stacked = jnp.concatenate(
                [jnp.where(head_of == head, queries, 0).astype(jnp.bfloat16) for head in range(HA)],
                axis=0,
            )
            score = lax.dot_general(
                stacked, key_ref[pl.ds(base, WK), :], (((1,), (1,)), ((), ())),
                preferred_element_type=jnp.float32,
            )
            bias = bias_ref[:, pl.ds(base, WQ), :].reshape(HA * WQ, WK).astype(jnp.float32)
            slot = first_ref[0] + base - RIM + lane
            index = step * BATCH + i
            inside = (slot >= bounds_ref[2 * index]) & (slot < bounds_ref[2 * index + 1])
            scores.append(jnp.where(inside, score * scale + bias, FAR))
        weights = [jnp.exp(score - jnp.max(score, axis=-1, keepdims=True)) for score in scores]
        results = []
        for base, weight in zip(bases, weights):
            attended = matmul(weight.astype(jnp.bfloat16), value_ref[pl.ds(base, WK), :])
            attended = attended / jnp.sum(weight, axis=-1, keepdims=True)
            result = jnp.zeros((WQ, channels), jnp.float32)
            for head in range(HA):
                result = result + jnp.where(
                    head_of == head, attended[head * WQ : (head + 1) * WQ], 0.0
                )
            results.append(result)
        start = pl.multiple_of(step * (BATCH * WQ), BATCH * WQ)
        held_ref[pl.ds(start, BATCH * WQ), :] = jnp.concatenate(results, axis=0)
        return carry

    lax.fori_loop(0, count // (BATCH * WQ), windows, 0)
    gated = (held_ref[...] * jax.nn.sigmoid(gate_ref[...].astype(jnp.float32))).astype(jnp.bfloat16)
    fresh = state_ref[inner, :] + matmul_t(gated, weight_ref[6])
    final = layer_norm(fresh).astype(jnp.bfloat16)
    moved = matmul_t(position_ref[...], final)
    for axis in range(out_ref.shape[0]):
        out_ref[axis] = moved[axis : axis + 1, :]


BATCH = 8


def atom_block(first, bounds, rows, skip, cond, rims, owners, weights, vectors, positions, bias):
    count, channels = bias.shape[1], skip.shape[1]
    extended = skip.shape[0] + 2 * RIM
    smem = pl.BlockSpec(memory_space=pltpu.SMEM)
    vmem = pl.BlockSpec(memory_space=pltpu.VMEM)
    return pl.pallas_call(
        atom_kernel,
        in_specs=[smem, smem] + [vmem] * 9,
        out_specs=vmem,
        out_shape=jax.ShapeDtypeStruct((positions.shape[0], 1, count), jnp.float32),
        scratch_shapes=[
            pltpu.VMEM((extended, channels), jnp.float32),
            pltpu.VMEM((count, channels), jnp.bfloat16),
            pltpu.VMEM((count, channels), jnp.bfloat16),
            pltpu.VMEM((extended, channels), jnp.bfloat16),
            pltpu.VMEM((extended, channels), jnp.bfloat16),
            pltpu.VMEM((count, channels), jnp.float32),
        ],
        compiler_params=pltpu.CompilerParams(vmem_limit_bytes=VMEM_LIMIT),
        name="atom_block",
    )(first, bounds, rows, skip, cond, rims, owners, weights, vectors, positions, bias)


def rims(array):
    return jnp.stack([array[:RIM], array[array.shape[0] - RIM :]])


def per_device(
    token_act,
    token_cond,
    pair_bias,
    token_mask,
    ada_weights,
    attention_in,
    attention_out,
    transition_in,
    transition_out,
    token_vectors,
    atom_skip,
    atom_cond,
    atom_bias,
    window_bounds,
    atom_token,
    atom_weights,
    token_to_atom,
    atom_vectors,
    position_out,
):
    groups = lax.axis_size("fsdp")
    width = attention_in.shape[2]
    channels = atom_cond.shape[1]
    atom_rims = rims(jnp.concatenate([atom_skip[0], atom_cond], axis=1))
    owner_rims = jnp.pad(rims(atom_token)[:, None, :], ((0, 0), (0, 0), (0, 2 * WK - RIM)))
    vectors = jnp.transpose(token_vectors.reshape(-1, groups, width), (1, 0, 2))
    token_result, all_rows, atom_rims, owner_rims, atom_all = token_layer(
        token_act[0],
        token_cond[0],
        token_mask[None],
        vectors,
        atom_rims,
        owner_rims,
        jnp.swapaxes(atom_weights, 1, 2).reshape(-1, channels),
        token_to_atom,
        pair_bias,
        jnp.swapaxes(ada_weights, 1, 2),
        jnp.swapaxes(attention_in, 1, 2),
        attention_out,
        transition_in,
        transition_out,
    )
    owners = jnp.concatenate([owner_rims[0, 0, :RIM], atom_token, owner_rims[1, 0, :RIM]])[:, None]
    count = atom_weights.shape[0]
    atom_full = jnp.transpose(
        atom_all.reshape(groups, count, -1, channels), (1, 0, 2, 3)
    ).reshape(count, channels, channels)
    first_atom = (lax.axis_index("seq") * atom_cond.shape[0]).astype(jnp.int32).reshape(1)
    update = atom_block(
        first_atom,
        window_bounds.reshape(-1),
        all_rows.reshape(-1, channels),
        atom_skip[0],
        atom_cond,
        atom_rims,
        owners,
        atom_full,
        atom_vectors,
        position_out,
        atom_bias,
    )
    return (token_result[None], jnp.transpose(update, (1, 0, 2)))


def solution(mesh):
    in_specs = (
        P(("sample", "fsdp"), "seq", None),
        P(("sample", "fsdp"), "seq", None),
        P("fsdp", "seq", None),
        P("seq"),
        P(None, None, "fsdp"),
        P(None, None, "fsdp"),
        P("fsdp", None),
        P(None, None, "fsdp"),
        P("fsdp", None),
        P(),
        P(("sample", "fsdp"), "seq", None),
        P("seq", None),
        P(None, "seq", None),
        P("seq", None),
        P("seq"),
        P(None, None, "fsdp"),
        P("fsdp", None),
        P(),
        P(),
    )
    out_specs = (P(("sample", "fsdp"), "seq", None), P(("sample", "fsdp"), None, "seq"))
    return jax.shard_map(
        per_device, mesh=mesh, in_specs=in_specs, out_specs=out_specs, check_vma=False
    )
```

```python
import functools
import math
import types

import jax
import jax.numpy as jnp
from jax import lax
from jax.experimental import pallas as pl
from jax.experimental.pallas import tpu as pltpu
from jax.sharding import PartitionSpec as P

HA = 4
WQ = 32
WK = 128
HD = 48
EPS = 1e-05
FAR = -1e30
RIM = (WK - WQ) // 2
ATOM_MAPS = 7
BATCH = 8
VMEM_LIMIT = 56 * 1024 * 1024
MESH = pl.DeviceIdType.MESH


def layer_norm(values):
    values = values.astype(jnp.float32)
    center = values - jnp.mean(values, axis=-1, keepdims=True)
    spread = jnp.mean(center * center, axis=-1, keepdims=True)
    return center * lax.rsqrt(spread + EPS)


def matmul(left_side, right_side):
    return jnp.dot(left_side, right_side, preferred_element_type=jnp.float32)


def matmul_t(left_side, right_side):
    return lax.dot_general(
        left_side, right_side, (((1,), (1,)), ((), ())), preferred_element_type=jnp.float32
    )


def pack(array):
    half = array.shape[-2] // 2
    return jnp.concatenate([array[..., :half, :], array[..., half:, :]], axis=-1)


def unpack(array):
    half = array.shape[-1] // 2
    return jnp.concatenate([array[..., :half], array[..., half:]], axis=-2)


def remote(source, target, send, recv, axis, peer):
    return pltpu.make_async_remote_copy(
        src_ref=source, dst_ref=target, send_sem=send, recv_sem=recv,
        device_id={axis: peer}, device_id_type=MESH,
    )


class Chain:
    def __init__(self, axis, size, view, send, recv, prefix):
        self.axis, self.size, self.view = axis, size, view
        self.send, self.recv, self.prefix = send, recv, prefix
        self.here = lax.axis_index(axis)

    def guards(self, side, step):
        here, last = self.here, self.size - 1
        if side == 0:
            return (here - step >= 0) & (here < last), here - 1 - step >= 0
        return (here + step <= last) & (here > 0), here + 1 + step <= last

    def copy(self, side, step, arriving):
        sign = 1 if side == 0 else -1
        block = self.view(self.here - sign * (step + (1 if arriving else 0)))
        at = self.prefix + (side, step)
        return remote(block, block, self.send.at[at], self.recv.at[at], self.axis, self.here + sign)

    def begin(self):
        for side in (0, 1):

            @pl.when(self.guards(side, 0)[0])
            def _():
                self.copy(side, 0, False).start()

    def arrive(self, step):
        for side in (0, 1):
            comes = self.guards(side, step)[1]

            @pl.when(comes)
            def _():
                self.copy(side, step, True).wait_recv()

            if step + 1 < self.size - 1:

                @pl.when(self.guards(side, step + 1)[0])
                def _():
                    self.copy(side, step + 1, False).start()

    def drain(self):
        for side in (0, 1):
            for step in range(self.size - 1):

                @pl.when(self.guards(side, step)[0])
                def _():
                    self.copy(side, step, False).wait_send()


class Pairs:
    def __init__(self, axis, size, view, send, recv, partner_send, partner_recv, prefix):
        self.axis, self.view, self.prefix = axis, view, prefix
        self.send, self.recv = send, recv
        self.partner_send, self.partner_recv = partner_send, partner_recv
        self.index = lax.axis_index(axis)
        self.length = size // 2
        self.position = self.index // 2
        self.parity = self.index - 2 * self.position

    def slot(self, position):
        return position * 2 + self.parity

    def partner(self):
        return self.index + 1 - 2 * self.parity

    def guards(self, side, step):
        here, last = self.position, self.length - 1
        if side == 0:
            return (here - step >= 0) & (here < last), here - 1 - step >= 0
        return (here + step <= last) & (here > 0), here + 1 + step <= last

    def copy(self, side, step, arriving):
        sign = 1 if side == 0 else -1
        block = self.view(self.slot(self.position - sign * (step + (1 if arriving else 0))))
        at = self.prefix + (side, step)
        return remote(
            block, block, self.send.at[at], self.recv.at[at], self.axis,
            self.slot(self.position + sign),
        )

    def hand(self, key, origin, arriving):
        block = self.view(origin * 2 + 1 - self.parity if arriving else self.slot(origin))
        at = self.prefix + (key,)
        return remote(
            block, block, self.partner_send.at[at], self.partner_recv.at[at], self.axis, self.partner()
        )

    def greet(self, signal):
        above, below = self.position > 0, self.position < self.length - 1

        @pl.when(above)
        def _():
            signal(self.axis, self.slot(self.position - 1))

        @pl.when(below)
        def _():
            signal(self.axis, self.slot(self.position + 1))

        signal(self.axis, self.partner())
        return jnp.where(above, 1, 0) + jnp.where(below, 1, 0) + 1

    def begin(self):
        for side in (0, 1):

            @pl.when(self.guards(side, 0)[0])
            def _():
                self.copy(side, 0, False).start()

        self.hand(0, self.position, False).start()

    def key(self, side, step):
        return 1 + side * (self.length - 1) + step

    def origin(self, side, step):
        return self.position - (step + 1) if side == 0 else self.position + step + 1

    def relay(self):
        for step in range(self.length - 1):
            for side in (0, 1):

                @pl.when(self.guards(side, step)[1])
                def _():
                    self.copy(side, step, True).wait_recv()
                    self.hand(self.key(side, step), self.origin(side, step), False).start()

                if step + 1 < self.length - 1:

                    @pl.when(self.guards(side, step + 1)[0])
                    def _():
                        self.copy(side, step + 1, False).start()

    def complete(self):
        self.hand(0, self.position, False).wait_send()
        self.hand(0, self.position, True).wait_recv()
        for step in range(self.length - 1):
            for side in (0, 1):
                goes, comes = self.guards(side, step)

                @pl.when(goes)
                def _():
                    self.copy(side, step, False).wait_send()

                @pl.when(comes)
                def _():
                    self.hand(self.key(side, step), self.origin(side, step), False).wait_send()
                    self.hand(self.key(side, step), self.origin(side, step), True).wait_recv()


class Halo:
    def __init__(self, axis, size, pieces, homes, send, recv, number):
        self.axis, self.pieces, self.homes = axis, pieces, homes
        self.send, self.recv, self.number = send, recv, number
        self.index = lax.axis_index(axis)
        self.present = self.index > 0, self.index < size - 1

    def greet(self, signal):
        for side in (0, 1):

            @pl.when(self.present[side])
            def _():
                signal(self.axis, self.index - 1 + 2 * side)

        return jnp.where(self.present[0], 1, 0) + jnp.where(self.present[1], 1, 0)

    def copy(self, side):
        at = (self.number, side)
        return remote(
            self.pieces[side], self.homes[1 - side], self.send.at[at], self.recv.at[at],
            self.axis, self.index - 1 + 2 * side,
        )

    def begin(self):
        for side in (0, 1):
            home = self.homes[side]

            @pl.when(self.present[side])
            def _():
                self.copy(side).start()

            @pl.when(jnp.logical_not(self.present[side]))
            def _():
                home[...] = jnp.zeros(home.shape, home.dtype)

    def finish(self):
        for side in (0, 1):

            @pl.when(self.present[side])
            def _():
                self.copy(side).wait_send()
                self.copy(1 - side).wait_recv()


def token_kernel(names, groups, ring, *refs):
    r = types.SimpleNamespace(**dict(zip(names, refs)))
    me, seat = lax.axis_index("fsdp"), lax.axis_index("seq")
    rows, depth = r.act.shape
    width = r.ada.shape[1]
    heads = r.bias.shape[0]
    half = rows // 2
    last = groups - 1
    barrier = pltpu.get_barrier_semaphore()

    def signal(axis, target):
        pl.semaphore_signal(barrier, inc=1, device_id={axis: target}, device_id_type=MESH)

    loads = {
        name: pltpu.make_async_copy(getattr(r, name + "_hbm"), getattr(r, name), r.load.at[number])
        for number, name in enumerate(("ada", "attn", "bias", "out", "tin", "tout", "atom_bias"))
    }
    count, channels = r.skip_hbm.shape
    inner_atoms = pl.ds(RIM, count)
    for number, name in enumerate(("skip", "atom_cond")):
        loads[name] = pltpu.make_async_copy(
            getattr(r, name + "_hbm"), getattr(r, name).at[inner_atoms], r.load.at[len(loads)]
        )

    def pairs(view, *prefix):
        return Pairs("seq", ring, view, r.seq_send, r.seq_recv, r.hand_send, r.hand_recv, prefix)

    halos = [
        Halo(
            "seq", ring, [source.at[pl.ds(start, RIM)] for start in (0, count - RIM)],
            [home.at[pl.ds(start, RIM)] for start in (0, RIM + count)], r.halo_send, r.halo_recv, number,
        )
        for number, (source, home) in enumerate(((r.skip_hbm, r.skip), (r.atom_cond_hbm, r.atom_cond)))
    ]
    halos += [
        Halo(
            "seq", ring, [r.owner_ends.at[0], r.owner_ends.at[r.owner_ends.shape[0] - 1]],
            [r.owner_rims.at[0], r.owner_rims.at[1]], r.halo_send, r.halo_recv, 2,
        )
    ]
    kv_flows = [pairs(lambda slot, g=g: r.kv.at[slot, g], g) for g in range(groups)]
    mask_flow = pairs(lambda slot: r.masks.at[slot], groups)
    rows_flow = pairs(lambda slot: r.rows_all.at[slot], groups + 1)

    for shift in range(1, groups):
        signal("fsdp", lax.rem(me + shift, groups))
    expected = last + mask_flow.greet(signal) + halos[0].greet(signal)
    for load in loads.values():
        load.start()

    def chain(number, view):
        return Chain("fsdp", groups, view, r.line_send, r.line_recv, (number,))

    cond_chains = [
        chain(part, lambda slot, part=part: r.conds.at[slot, pl.ds(part * half, half)]) for part in (0, 1)
    ]
    attend_chains = [chain(2 + g, lambda slot, g=g: r.attend.at[slot, g]) for g in range(groups)]
    transit_chains = [
        chain(2 + groups + g, lambda slot, g=g: r.transit.at[slot, g]) for g in range(groups)
    ]
    parity = seat - 2 * (seat // 2)
    atom_half, project_half = r.atom_part.shape[0] // 2, r.project_part.shape[0] // 2
    atom_rows = pl.ds(pl.multiple_of(parity * atom_half, 16), atom_half)
    project_rows = pl.ds(pl.multiple_of(parity * project_half, 16), project_half)
    small_chains = [
        chain(2 + 2 * groups, lambda slot: r.atom_all.at[slot, atom_rows]),
        chain(3 + 2 * groups, lambda slot: r.project.at[slot, project_rows]),
    ]

    def swaps():
        partner = seat + 1 - 2 * parity
        blocks = (r.atom_all.at[:, atom_rows], r.project.at[:, project_rows])
        return [
            remote(block, block, r.swap_send.at[i], r.swap_recv.at[i], "seq", partner)
            for i, block in enumerate(blocks)
        ]

    r.conds[me] = layer_norm(r.cond[...]).astype(jnp.bfloat16)
    r.masks[seat] = r.mask[...]
    r.atom_all[me, atom_rows] = r.atom_part[atom_rows, :]
    r.project[me, project_rows] = r.project_part[project_rows, :]
    pl.semaphore_wait(barrier, expected)
    for flow in cond_chains:
        flow.begin()
    act_normed = layer_norm(r.act[...]).astype(jnp.bfloat16)
    for g in range(groups):
        r.act_out[g] = pack(act_normed[:, g * width : (g + 1) * width])

    def slots(shift, arriving):
        peer = lax.rem(me + shift, groups)
        landing = lax.rem(me + groups - shift, groups) if arriving else me
        return remote(
            r.act_out.at[peer], r.acts.at[landing], r.act_send.at[shift], r.act_recv.at[shift],
            "fsdp", peer,
        )

    for shift in range(1, groups):
        slots(shift, False).start()
    mask_flow.begin()
    for halo in halos:
        halo.begin()
    offsets = r.vectors[me]

    def adaptive(sample, packed):
        rows_in = r.conds[sample]
        values = unpack(packed).astype(jnp.float32)

        def one(scale, shift, vector):
            gate = jax.nn.sigmoid(matmul_t(rows_in, r.ada[scale]) + offsets[vector : vector + 1, :])
            return pack((gate * values + matmul_t(rows_in, r.ada[shift])).astype(jnp.bfloat16))

        r.attend[me, sample] = one(0, 1, 0)
        r.transit[me, sample] = one(2, 3, 1)

    loads["ada"].wait()
    adaptive(me, r.act_out[me])
    inner = sorted(range(groups), key=lambda g: max(g, last - g))
    outer = sorted(range(groups), key=lambda g: (-max(g, last - g), g))
    for step in range(last):
        for flow in cond_chains:
            flow.arrive(step)
        for side in (0, 1):

            @pl.when(cond_chains[0].guards(side, step)[1])
            def _():
                origin = me - (step + 1) if side == 0 else me + step + 1
                slots(step + 1 if side == 0 else last - step, True).wait_recv()
                adaptive(origin, r.acts[origin])

        for g in inner:
            if max(g, last - g) == step + 1:
                attend_chains[g].begin()

    def joined(ref, g):
        return jnp.concatenate([unpack(ref[origin, g]) for origin in range(groups)], axis=1)

    def projections(g):
        full = joined(r.attend, g)
        r.queries[g] = (matmul_t(full, r.attn[0]) + offsets[2:3, :]).astype(jnp.bfloat16)
        both = r.attn[1:3].reshape(2 * width, depth)
        r.kv[seat, g] = matmul_t(full, both).astype(jnp.bfloat16)
        kv_flows[g].begin()
        r.gates[g] = matmul_t(full, r.attn[3]).astype(jnp.bfloat16)

    for step in range(last - 1):
        for g in inner:
            attend_chains[g].arrive(step)
    for g in outer:
        transit_chains[g].begin()
    loads["attn"].wait()
    for g in inner:
        attend_chains[g].arrive(last - 1)
        projections(g)
    for flow in small_chains:
        flow.begin()

    def attention(g):
        queries = r.queries[g]
        head_of = lax.broadcasted_iota(jnp.int32, (rows, width), 1) // HD
        stacked = jnp.concatenate(
            [jnp.where(head_of == head, queries, 0).astype(jnp.bfloat16) for head in range(heads)], axis=0
        )
        scale = 1.0 / math.sqrt(HD)
        span = min(max(512 // rows, 1), ring)

        def block(first, state):
            keys = jnp.concatenate([r.kv[first + i, g, :, :width] for i in range(span)], axis=0)
            values = jnp.concatenate([r.kv[first + i, g, :, width:] for i in range(span)], axis=0)
            live = jnp.concatenate([r.masks[first + i] for i in range(span)], axis=1)
            columns = pl.ds(pl.multiple_of(first * rows, span * rows), span * rows)
            bias = r.bias[:, :, columns].reshape(heads * rows, span * rows).astype(jnp.float32)
            scores = matmul_t(stacked, keys) * scale + bias
            scores = jnp.where(live > 0, scores, FAR)
            block_max = jnp.max(scores, axis=-1, keepdims=True)
            new_maxima = block_max if state is None else jnp.maximum(state[0], block_max)
            weights = jnp.exp(scores - new_maxima)
            totals = jnp.sum(weights, axis=-1, keepdims=True)
            summed = matmul(weights.astype(jnp.bfloat16), values)
            if state is not None:
                factor = jnp.exp(state[0] - new_maxima)
                totals, summed = state[1] * factor + totals, state[2] * factor + summed
            return new_maxima, totals, summed

        state = block(0, None)
        if ring > span:
            state = lax.fori_loop(1, ring // span, lambda i, state: block(i * span, state), state)
        attended = state[2] / state[1]
        result = jnp.zeros((rows, width), jnp.float32)
        for head in range(heads):
            result = result + jnp.where(head_of == head, attended[head * rows : (head + 1) * rows], 0.0)
        gate = jax.nn.sigmoid(r.gates[g].astype(jnp.float32))
        r.gated[g] = (result * gate).astype(jnp.bfloat16)

    pending = [(transit_chains[g], step) for step in range(last - 1) for g in outer]
    pending += [(flow, step) for step in range(last - 1) for flow in small_chains]
    share = -(-len(pending) // groups)
    mask_flow.relay()
    mask_flow.complete()
    loads["bias"].wait()
    kv_flows[inner[0]].relay()
    for number, g in enumerate(inner):
        if number + 1 < groups:
            kv_flows[inner[number + 1]].relay()
        kv_flows[g].complete()
        attention(g)
        for flow, step in pending[number * share : (number + 1) * share]:
            flow.arrive(step)

    def hop(side, g, part):
        piece = pl.ds(part * half, half)
        at = (side, g, part)
        return remote(
            r.sums_out.at[g, piece], r.sums_in.at[side, g, piece], r.sum_send.at[at], r.sum_recv.at[at],
            "fsdp", me + (1 if side == 0 else -1),
        )

    def take(side, g, part):
        hop(side, g, part).wait_recv()
        piece = pl.ds(part * half, half)
        r.total[g, piece] += r.sums_in[side, g, piece].astype(jnp.float32)

    def reduce(stage, g):
        for side, here, goes in ((0, stage, g > stage), (1, last - stage, g < last - stage)):
            if goes:

                @pl.when(me == here)
                def _():
                    for part in (0, 1):
                        piece = pl.ds(part * half, half)
                        if stage > 0:
                            take(side, g, part)
                        r.sums_out[g, piece] = r.total[g, piece].astype(jnp.bfloat16)
                        hop(side, g, part).start()

    heads_out = lax.broadcasted_iota(jnp.int32, (WQ, channels), 1) // (channels // HA)
    tokens = ring * rows

    def atom_weight(i):
        high = r.atom_part.shape[0] // ATOM_MAPS
        return r.atom_all[:, i * high : (i + 1) * high, :].reshape(channels, channels)

    def atom_before():
        normed = layer_norm(r.atom_cond[...]).astype(jnp.bfloat16)
        r.atom_gain[...] = jax.nn.sigmoid(matmul_t(normed, atom_weight(0)) + r.atom_vectors[0:1, :])
        r.atom_shift[...] = matmul_t(normed, atom_weight(1))
        blocks = r.owner.shape[0]

        def hit(column, start):
            span = min(512, tokens)
            for first in range(0, tokens, span):
                token = lax.broadcasted_iota(jnp.int32, (column.shape[0], span), 1) + first
                found = jnp.where(column == token.astype(jnp.float32), 1.0, 0.0).astype(jnp.bfloat16)
                r.hits[pl.ds(start, column.shape[0]), pl.ds(first, span)] = found

        owners = jnp.transpose(r.owner[...].astype(jnp.float32))
        for block in range(blocks):
            hit(owners[:, block : block + 1], RIM + block * WK)
        for side, home in ((0, 0), (1, RIM + count)):
            ends = jnp.broadcast_to(r.owner_rims[side].astype(jnp.float32), (8, WK))
            column = jnp.transpose(ends)[:, 0:1]
            hit(column[WK - RIM :] if side == 0 else column[:RIM], home)
        lane = lax.broadcasted_iota(jnp.int32, (1, WK), 1)

        def window(index, carry):
            base = pl.multiple_of(index * WQ, WQ)
            slot = seat * count + base - RIM + lane
            inside = (slot >= r.bounds[0, index]) & (slot < r.bounds[1, index])
            bias = r.atom_bias[:, pl.ds(base, WQ), :].reshape(HA * WQ, WK).astype(jnp.float32)
            r.masked[index] = jnp.where(inside, bias, FAR)
            return carry

        lax.fori_loop(0, count // WQ, window, 0)

    def atom_after():
        taken = matmul(r.hits[...], r.rows_all[...].reshape(tokens, channels))
        state = r.skip[...].astype(jnp.float32) + taken
        r.state[...] = state[RIM : RIM + count]
        atom_x = (r.atom_gain[...] * layer_norm(state) + r.atom_shift[...]).astype(jnp.bfloat16)
        own_x = atom_x[RIM : RIM + count, :]
        r.atom_query[...] = (matmul_t(own_x, atom_weight(2)) + r.atom_vectors[1:2, :]).astype(jnp.bfloat16)
        r.atom_key[...] = matmul_t(atom_x, atom_weight(3)).astype(jnp.bfloat16)
        r.atom_value[...] = matmul_t(atom_x, atom_weight(4)).astype(jnp.bfloat16)
        r.atom_gate[...] = jax.nn.sigmoid(matmul_t(own_x, atom_weight(5)).astype(jnp.bfloat16).astype(jnp.float32))
        scale = 1.0 / math.sqrt(channels // HA)

        def windows(step, carry):
            bases = [pl.multiple_of(step * (BATCH * WQ) + i * WQ, WQ) for i in range(BATCH)]
            scores = []
            for i, base in enumerate(bases):
                queries = r.atom_query[pl.ds(base, WQ), :]
                stacked = jnp.concatenate(
                    [jnp.where(heads_out == head, queries, 0).astype(jnp.bfloat16) for head in range(HA)],
                    axis=0,
                )
                score = matmul_t(stacked, r.atom_key[pl.ds(base, WK), :])
                masked = r.masked[step * BATCH + i]
                scores.append(jnp.where(masked > 0.5 * FAR, score * scale + masked, FAR))
            weights = [jnp.exp(score - jnp.max(score, axis=-1, keepdims=True)) for score in scores]
            results = []
            for base, weight in zip(bases, weights):
                attended = matmul(weight.astype(jnp.bfloat16), r.atom_value[pl.ds(base, WK), :])
                attended = attended / jnp.sum(weight, axis=-1, keepdims=True)
                result = jnp.zeros((WQ, channels), jnp.float32)
                for head in range(HA):
                    result = result + jnp.where(
                        heads_out == head, attended[head * WQ : (head + 1) * WQ], 0.0
                    )
                results.append(result)
            start = pl.multiple_of(step * (BATCH * WQ), BATCH * WQ)
            r.held[pl.ds(start, BATCH * WQ), :] = jnp.concatenate(results, axis=0)
            return carry

        lax.fori_loop(0, count // (BATCH * WQ), windows, 0)
        gated = (r.held[...] * r.atom_gate[...]).astype(jnp.bfloat16)
        fresh = r.state[...] + matmul_t(gated, atom_weight(6))
        final = layer_norm(fresh).astype(jnp.bfloat16)
        moved = matmul_t(r.position[...], final)
        for axis in range(moved.shape[0]):
            r.update[axis] = moved[axis : axis + 1, :]

    for name in ("out", "tin", "tout"):
        loads[name].wait()
    for g in outer:
        transit_chains[g].arrive(last - 1)
        full = joined(r.transit, g)
        hidden = jax.nn.silu(matmul(full, r.tin[0])) * matmul(full, r.tin[1])
        r.total[g] = matmul(r.gated[g], r.out[...]) + matmul(hidden.astype(jnp.bfloat16), r.tout[...])
        reduce(0, g)
    for flow in small_chains:
        flow.arrive(last - 1)
    for copy in swaps():
        copy.start()
    for name in ("skip", "atom_cond", "atom_bias"):
        loads[name].wait()
    for halo in halos:
        halo.finish()
    for copy in swaps():
        copy.wait()
    for stage in range(1, last):
        for g in outer:
            reduce(stage, g)
        if stage == 1:
            atom_before()
    if last == 1:
        atom_before()
    for side, present in ((0, me > 0), (1, me < last)):

        @pl.when(present)
        def _():
            for part in (0, 1):
                take(side, me, part)

    token = (r.act[...].astype(jnp.float32) + r.total[me]).astype(jnp.bfloat16)
    r.token[...] = token
    r.rows_all[seat] = matmul(token, r.project[...].reshape(depth, -1)).astype(jnp.bfloat16)
    rows_flow.begin()
    for flow in cond_chains + attend_chains + transit_chains + small_chains:
        flow.drain()
    for shift in range(1, groups):
        slots(shift, False).wait_send()
    for g in range(groups):
        for side, goes in ((0, g > me), (1, g < me)):

            @pl.when(goes)
            def _():
                for part in (0, 1):
                    hop(side, g, part).wait_send()

    rows_flow.relay()
    rows_flow.complete()
    atom_after()


def token_layer(near, weights, bounds):
    groups, ring = lax.axis_size("fsdp"), lax.axis_size("seq")
    rows, depth = near["act"].shape
    width = weights["ada"].shape[1]
    count, channels = weights["skip"].shape
    extended = count + 2 * RIM
    dma = pltpu.SemaphoreType.DMA
    vmem, far = pl.BlockSpec(memory_space=pltpu.VMEM), pl.BlockSpec(memory_space=pl.ANY)
    half_type = jnp.bfloat16
    project_part, atom_part = near["project_part"], near["atom_part"]
    outs = dict(
        token=((rows, depth), half_type),
        update=((near["position"].shape[0], 1, count), jnp.float32),
    )
    packed = (groups, groups, rows // 2, 2 * width)
    chains = 4 + 2 * groups
    hops = max(groups - 1, 1)
    length = ring // 2
    scratch = {name: pltpu.VMEM(array.shape, array.dtype) for name, array in weights.items()}
    atoms = lambda height, kind: pltpu.VMEM((height, channels), kind)
    scratch |= dict(
        skip=atoms(extended, half_type),
        atom_cond=atoms(extended, half_type),
        atom_gain=atoms(extended, jnp.float32),
        atom_shift=atoms(extended, jnp.float32),
        atom_key=atoms(extended, half_type),
        atom_value=atoms(extended, half_type),
        atom_query=atoms(count, half_type),
        atom_gate=atoms(count, jnp.float32),
        state=atoms(count, jnp.float32),
        held=atoms(count, jnp.float32),
        hits=pltpu.VMEM((extended, ring * rows), half_type),
        masked=pltpu.VMEM((count // WQ, HA * WQ, WK), jnp.float32),
        owner_rims=pltpu.VMEM((2, 1, near["owner"].shape[1]), jnp.int32),
        rows_all=pltpu.VMEM((ring, rows, channels), half_type),
        atom_all=pltpu.VMEM((groups,) + atom_part.shape, half_type),
        conds=pltpu.VMEM((groups, rows, depth), half_type),
        act_out=pltpu.VMEM(packed[1:], half_type),
        acts=pltpu.VMEM(packed[1:], half_type),
        attend=pltpu.VMEM(packed, half_type),
        transit=pltpu.VMEM(packed, half_type),
        queries=pltpu.VMEM((groups, rows, width), half_type),
        gates=pltpu.VMEM((groups, rows, width), half_type),
        gated=pltpu.VMEM((groups, rows, width), half_type),
        kv=pltpu.VMEM((ring, groups, rows, 2 * width), half_type),
        masks=pltpu.VMEM((ring, 1, rows), jnp.int32),
        project=pltpu.VMEM((groups,) + project_part.shape, half_type),
        total=pltpu.VMEM((groups, rows, depth), jnp.float32),
        sums_out=pltpu.VMEM((groups, rows, depth), half_type),
        sums_in=pltpu.VMEM((2, groups, rows, depth), half_type),
        load=dma((len(weights),)),
        line_send=dma((chains, 2, hops)),
        line_recv=dma((chains, 2, hops)),
        act_send=dma((groups,)),
        act_recv=dma((groups,)),
        seq_send=dma((groups + 2, 2, max(length - 1, 1))),
        seq_recv=dma((groups + 2, 2, max(length - 1, 1))),
        hand_send=dma((groups + 2, 2 * length)),
        hand_recv=dma((groups + 2, 2 * length)),
        halo_send=dma((3, 2)),
        halo_recv=dma((3, 2)),
        swap_send=dma((2,)),
        swap_recv=dma((2,)),
        sum_send=dma((2, groups, 2)),
        sum_recv=dma((2, groups, 2)),
    )
    names = ["bounds"] + list(near) + [name + "_hbm" for name in weights] + list(outs) + list(scratch)
    return pl.pallas_call(
        functools.partial(token_kernel, tuple(names), groups, ring),
        out_shape=tuple(jax.ShapeDtypeStruct(*out) for out in outs.values()),
        in_specs=[pl.BlockSpec(memory_space=pltpu.SMEM)] + [vmem] * len(near) + [far] * len(weights),
        out_specs=tuple([vmem] * len(outs)),
        scratch_shapes=list(scratch.values()),
        compiler_params=pltpu.CompilerParams(
            collective_id=1, has_side_effects=True, vmem_limit_bytes=VMEM_LIMIT
        ),
        name="token_layer",
    )(bounds, *near.values(), *weights.values())


def per_device(
    token_act,
    token_cond,
    pair_bias,
    token_mask,
    ada_weights,
    attention_in,
    attention_out,
    transition_in,
    transition_out,
    token_vectors,
    atom_skip,
    atom_cond,
    atom_bias,
    window_bounds,
    atom_token,
    atom_weights,
    token_to_atom,
    atom_vectors,
    position_out,
):
    groups = lax.axis_size("fsdp")
    width = attention_in.shape[2]
    channels = atom_cond.shape[1]
    near = dict(
        act=token_act[0],
        cond=token_cond[0],
        mask=token_mask[None],
        vectors=jnp.transpose(token_vectors.reshape(-1, groups, width), (1, 0, 2)),
        owner=atom_token.reshape(-1, WK),
        owner_ends=atom_token.reshape(-1, 1, WK),
        atom_part=jnp.swapaxes(atom_weights, 1, 2).reshape(-1, channels),
        project_part=token_to_atom,
        atom_vectors=atom_vectors,
        position=position_out,
    )
    weights = dict(
        ada=jnp.swapaxes(ada_weights, 1, 2),
        attn=jnp.swapaxes(attention_in, 1, 2),
        bias=pair_bias,
        out=attention_out,
        tin=transition_in,
        tout=transition_out,
        atom_bias=atom_bias,
        skip=atom_skip[0],
        atom_cond=atom_cond,
    )
    token_result, update = token_layer(near, weights, jnp.swapaxes(window_bounds, 0, 1))
    return (token_result[None], jnp.transpose(update, (1, 0, 2)))


def solution(mesh):
    in_specs = (
        P(("sample", "fsdp"), "seq", None),
        P(("sample", "fsdp"), "seq", None),
        P("fsdp", "seq", None),
        P("seq"),
        P(None, None, "fsdp"),
        P(None, None, "fsdp"),
        P("fsdp", None),
        P(None, None, "fsdp"),
        P("fsdp", None),
        P(),
        P(("sample", "fsdp"), "seq", None),
        P("seq", None),
        P(None, "seq", None),
        P("seq", None),
        P("seq"),
        P(None, None, "fsdp"),
        P("fsdp", None),
        P(),
        P(),
    )
    out_specs = (P(("sample", "fsdp"), "seq", None), P(("sample", "fsdp"), None, "seq"))
    return jax.shard_map(
        per_device, mesh=mesh, in_specs=in_specs, out_specs=out_specs, check_vma=False
    )
```

```python
import functools
import math
import types

import jax
import jax.numpy as jnp
from jax import lax
from jax.experimental import pallas as pl
from jax.experimental.pallas import tpu as pltpu
from jax.sharding import PartitionSpec as P

HA = 4
WQ = 32
WK = 128
HD = 48
EPS = 1e-05
FAR = -1e30
RIM = (WK - WQ) // 2
ATOM_MAPS = 7
BATCH = 8
VMEM_LIMIT = 56 * 1024 * 1024
MESH = pl.DeviceIdType.MESH


def layer_norm(values):
    values = values.astype(jnp.float32)
    center = values - jnp.mean(values, axis=-1, keepdims=True)
    spread = jnp.mean(center * center, axis=-1, keepdims=True)
    return center * lax.rsqrt(spread + EPS)


def matmul(left_side, right_side):
    return jnp.dot(left_side, right_side, preferred_element_type=jnp.float32)


def matmul_t(left_side, right_side):
    return lax.dot_general(
        left_side, right_side, (((1,), (1,)), ((), ())), preferred_element_type=jnp.float32
    )


def pack(array):
    half = array.shape[-2] // 2
    return jnp.concatenate([array[..., :half, :], array[..., half:, :]], axis=-1)


def unpack(array):
    half = array.shape[-1] // 2
    return jnp.concatenate([array[..., :half], array[..., half:]], axis=-2)


def remote(source, target, send, recv, axis, peer):
    return pltpu.make_async_remote_copy(
        src_ref=source, dst_ref=target, send_sem=send, recv_sem=recv,
        device_id={axis: peer}, device_id_type=MESH,
    )


class Chain:
    def __init__(self, axis, size, view, send, recv, prefix):
        self.axis, self.size, self.view = axis, size, view
        self.send, self.recv, self.prefix = send, recv, prefix
        self.here = lax.axis_index(axis)

    def guards(self, side, step):
        here, last = self.here, self.size - 1
        if side == 0:
            return (here - step >= 0) & (here < last), here - 1 - step >= 0
        return (here + step <= last) & (here > 0), here + 1 + step <= last

    def copy(self, side, step, arriving):
        sign = 1 if side == 0 else -1
        block = self.view(self.here - sign * (step + (1 if arriving else 0)))
        at = self.prefix + (side, step)
        return remote(block, block, self.send.at[at], self.recv.at[at], self.axis, self.here + sign)

    def begin(self):
        for side in (0, 1):

            @pl.when(self.guards(side, 0)[0])
            def _():
                self.copy(side, 0, False).start()

    def arrive(self, step):
        for side in (0, 1):
            comes = self.guards(side, step)[1]

            @pl.when(comes)
            def _():
                self.copy(side, step, True).wait_recv()

            if step + 1 < self.size - 1:

                @pl.when(self.guards(side, step + 1)[0])
                def _():
                    self.copy(side, step + 1, False).start()

    def drain(self):
        for side in (0, 1):
            for step in range(self.size - 1):

                @pl.when(self.guards(side, step)[0])
                def _():
                    self.copy(side, step, False).wait_send()


class Pairs:
    def __init__(self, axis, size, view, send, recv, partner_send, partner_recv, prefix):
        self.axis, self.view, self.prefix = axis, view, prefix
        self.send, self.recv = send, recv
        self.partner_send, self.partner_recv = partner_send, partner_recv
        self.index = lax.axis_index(axis)
        self.length = size // 2
        self.position = self.index // 2
        self.parity = self.index - 2 * self.position

    def slot(self, position):
        return position * 2 + self.parity

    def partner(self):
        return self.index + 1 - 2 * self.parity

    def guards(self, side, step):
        here, last = self.position, self.length - 1
        if side == 0:
            return (here - step >= 0) & (here < last), here - 1 - step >= 0
        return (here + step <= last) & (here > 0), here + 1 + step <= last

    def copy(self, side, step, arriving):
        sign = 1 if side == 0 else -1
        block = self.view(self.slot(self.position - sign * (step + (1 if arriving else 0))))
        at = self.prefix + (side, step)
        return remote(
            block, block, self.send.at[at], self.recv.at[at], self.axis,
            self.slot(self.position + sign),
        )

    def hand(self, key, origin, arriving):
        block = self.view(origin * 2 + 1 - self.parity if arriving else self.slot(origin))
        at = self.prefix + (key,)
        return remote(
            block, block, self.partner_send.at[at], self.partner_recv.at[at], self.axis, self.partner()
        )

    def begin(self):
        for side in (0, 1):

            @pl.when(self.guards(side, 0)[0])
            def _():
                self.copy(side, 0, False).start()

        self.hand(0, self.position, False).start()

    def key(self, side, step):
        return 1 + side * (self.length - 1) + step

    def origin(self, side, step):
        return self.position - (step + 1) if side == 0 else self.position + step + 1

    def relay(self):
        for step in range(self.length - 1):
            for side in (0, 1):

                @pl.when(self.guards(side, step)[1])
                def _():
                    self.copy(side, step, True).wait_recv()
                    self.hand(self.key(side, step), self.origin(side, step), False).start()

                if step + 1 < self.length - 1:

                    @pl.when(self.guards(side, step + 1)[0])
                    def _():
                        self.copy(side, step + 1, False).start()

    def complete(self):
        self.hand(0, self.position, False).wait_send()
        self.hand(0, self.position, True).wait_recv()
        for step in range(self.length - 1):
            for side in (0, 1):
                goes, comes = self.guards(side, step)

                @pl.when(goes)
                def _():
                    self.copy(side, step, False).wait_send()

                @pl.when(comes)
                def _():
                    self.hand(self.key(side, step), self.origin(side, step), False).wait_send()
                    self.hand(self.key(side, step), self.origin(side, step), True).wait_recv()


class Halo:
    def __init__(self, axis, size, pieces, homes, send, recv, number):
        self.axis, self.pieces, self.homes = axis, pieces, homes
        self.send, self.recv, self.number = send, recv, number
        self.index = lax.axis_index(axis)
        self.present = self.index > 0, self.index < size - 1

    def copy(self, side):
        at = (self.number, side)
        return remote(
            self.pieces[side], self.homes[1 - side], self.send.at[at], self.recv.at[at],
            self.axis, self.index - 1 + 2 * side,
        )

    def begin(self):
        for side in (0, 1):
            home = self.homes[side]

            @pl.when(self.present[side])
            def _():
                self.copy(side).start()

            @pl.when(jnp.logical_not(self.present[side]))
            def _():
                home[...] = jnp.zeros(home.shape, home.dtype)

    def finish(self):
        for side in (0, 1):

            @pl.when(self.present[side])
            def _():
                self.copy(side).wait_send()
                self.copy(1 - side).wait_recv()


class Spread:
    def __init__(self, axis, size, view, send, recv, number):
        self.axis, self.size, self.view = axis, size, view
        self.send, self.recv, self.number = send, recv, number
        self.here = lax.axis_index(axis)

    def copy(self, shift, arriving):
        block = self.view(lax.rem(self.here + self.size - shift, self.size) if arriving else self.here)
        at = (self.number, shift)
        peer = lax.rem(self.here + shift, self.size)
        return remote(block, block, self.send.at[at], self.recv.at[at], self.axis, peer)

    def begin(self):
        for shift in range(1, self.size):
            self.copy(shift, False).start()

    def finish(self):
        for shift in range(1, self.size):
            self.copy(shift, False).wait_send()
            self.copy(shift, True).wait_recv()


def token_kernel(names, groups, ring, *refs):
    r = types.SimpleNamespace(**dict(zip(names, refs)))
    me, seat = lax.axis_index("fsdp"), lax.axis_index("seq")
    rows, depth = r.act.shape
    width = r.ada.shape[1]
    heads = r.bias.shape[0]
    half = rows // 2
    last = groups - 1
    barrier = pltpu.get_barrier_semaphore()

    def signal(axis, target):
        pl.semaphore_signal(barrier, inc=1, device_id={axis: target}, device_id_type=MESH)

    loads = {
        name: pltpu.make_async_copy(getattr(r, name + "_hbm"), getattr(r, name), r.load.at[number])
        for number, name in enumerate(("ada", "attn", "bias", "out", "tin", "tout", "atom_bias"))
    }
    count, channels = r.skip_hbm.shape
    inner_atoms = pl.ds(RIM, count)
    for number, name in enumerate(("skip", "atom_cond")):
        loads[name] = pltpu.make_async_copy(
            getattr(r, name + "_hbm"), getattr(r, name).at[inner_atoms], r.load.at[len(loads)]
        )

    def pairs(view, *prefix):
        return Pairs("seq", ring, view, r.seq_send, r.seq_recv, r.hand_send, r.hand_recv, prefix)

    halos = [
        Halo(
            "seq", ring, [source.at[pl.ds(start, RIM)] for start in (0, count - RIM)],
            [home.at[pl.ds(start, RIM)] for start in (0, RIM + count)], r.halo_send, r.halo_recv, number,
        )
        for number, (source, home) in enumerate(((r.skip_hbm, r.skip), (r.atom_cond_hbm, r.atom_cond)))
    ]
    halos += [
        Halo(
            "seq", ring, [r.owner_ends.at[0], r.owner_ends.at[r.owner_ends.shape[0] - 1]],
            [r.owner_rims.at[0], r.owner_rims.at[1]], r.halo_send, r.halo_recv, 2,
        )
    ]
    kv_flows = [pairs(lambda slot, g=g: r.kv.at[slot, g], g) for g in range(groups)]
    mask_flow = Spread("seq", ring, lambda slot: r.masks.at[slot], r.spread_send, r.spread_recv, 0)
    rows_flow = Spread("seq", ring, lambda slot: r.rows_all.at[slot], r.spread_send, r.spread_recv, 1)

    for shift in range(1, groups):
        signal("fsdp", lax.rem(me + shift, groups))
    for shift in range(1, ring):
        signal("seq", lax.rem(seat + shift, ring))
    expected = last + ring - 1
    for load in loads.values():
        load.start()

    def chain(number, view):
        return Chain("fsdp", groups, view, r.line_send, r.line_recv, (number,))

    cond_chains = [
        chain(part, lambda slot, part=part: r.conds.at[slot, pl.ds(part * half, half)]) for part in (0, 1)
    ]
    attend_chains = [chain(2 + g, lambda slot, g=g: r.attend.at[slot, g]) for g in range(groups)]
    transit_chains = [
        chain(2 + groups + g, lambda slot, g=g: r.transit.at[slot, g]) for g in range(groups)
    ]
    parity = seat - 2 * (seat // 2)
    atom_half, project_half = r.atom_part.shape[0] // 2, r.project_part.shape[0] // 2
    atom_rows = pl.ds(pl.multiple_of(parity * atom_half, 16), atom_half)
    project_rows = pl.ds(pl.multiple_of(parity * project_half, 16), project_half)
    small_chains = [
        chain(2 + 2 * groups, lambda slot: r.atom_all.at[slot, atom_rows]),
        chain(3 + 2 * groups, lambda slot: r.project.at[slot, project_rows]),
    ]

    def swaps():
        partner = seat + 1 - 2 * parity
        blocks = (r.atom_all.at[:, atom_rows], r.project.at[:, project_rows])
        return [
            remote(block, block, r.swap_send.at[i], r.swap_recv.at[i], "seq", partner)
            for i, block in enumerate(blocks)
        ]

    r.conds[me] = layer_norm(r.cond[...]).astype(jnp.bfloat16)
    r.masks[seat] = r.mask[...]
    r.atom_all[me, atom_rows] = r.atom_part[atom_rows, :]
    r.project[me, project_rows] = r.project_part[project_rows, :]
    pl.semaphore_wait(barrier, expected)
    for flow in cond_chains:
        flow.begin()
    act_normed = layer_norm(r.act[...]).astype(jnp.bfloat16)
    for g in range(groups):
        r.act_out[g] = pack(act_normed[:, g * width : (g + 1) * width])

    def slots(shift, arriving):
        peer = lax.rem(me + shift, groups)
        landing = lax.rem(me + groups - shift, groups) if arriving else me
        return remote(
            r.act_out.at[peer], r.acts.at[landing], r.act_send.at[shift], r.act_recv.at[shift],
            "fsdp", peer,
        )

    for shift in range(1, groups):
        slots(shift, False).start()
    mask_flow.begin()
    for halo in halos:
        halo.begin()
    offsets = r.vectors[:, :width]
    for g in range(1, groups):
        offsets = jnp.where(me == g, r.vectors[:, g * width : (g + 1) * width], offsets)

    def adaptive(sample, packed):
        rows_in = r.conds[sample]
        values = unpack(packed).astype(jnp.float32)

        def one(scale, shift, vector):
            gate = jax.nn.sigmoid(matmul_t(rows_in, r.ada[scale]) + offsets[vector : vector + 1, :])
            return pack((gate * values + matmul_t(rows_in, r.ada[shift])).astype(jnp.bfloat16))

        r.attend[me, sample] = one(0, 1, 0)
        r.transit[me, sample] = one(2, 3, 1)

    loads["ada"].wait()
    adaptive(me, r.act_out[me])
    inner = sorted(range(groups), key=lambda g: max(g, last - g))
    outer = sorted(range(groups), key=lambda g: (-max(g, last - g), g))
    for step in range(last):
        for flow in cond_chains:
            flow.arrive(step)
        for side in (0, 1):

            @pl.when(cond_chains[0].guards(side, step)[1])
            def _():
                origin = me - (step + 1) if side == 0 else me + step + 1
                slots(step + 1 if side == 0 else last - step, True).wait_recv()
                adaptive(origin, r.acts[origin])

        for g in inner:
            if max(g, last - g) == step + 1:
                attend_chains[g].begin()

    def joined(ref, g):
        return jnp.concatenate([unpack(ref[origin, g]) for origin in range(groups)], axis=1)

    def projections(g):
        full = joined(r.attend, g)
        r.queries[g] = (matmul_t(full, r.attn[0]) + offsets[2:3, :]).astype(jnp.bfloat16)
        both = r.attn[1:3].reshape(2 * width, depth)
        r.kv[seat, g] = matmul_t(full, both).astype(jnp.bfloat16)
        kv_flows[g].begin()
        r.gates[g] = matmul_t(full, r.attn[3]).astype(jnp.bfloat16)

    for step in range(last - 1):
        for g in inner:
            attend_chains[g].arrive(step)
    for g in outer:
        transit_chains[g].begin()
    loads["attn"].wait()
    for g in inner:
        attend_chains[g].arrive(last - 1)
        projections(g)
    for flow in small_chains:
        flow.begin()

    def attention(g):
        queries = r.queries[g]
        head_of = lax.broadcasted_iota(jnp.int32, (rows, width), 1) // HD
        stacked = jnp.concatenate(
            [jnp.where(head_of == head, queries, 0).astype(jnp.bfloat16) for head in range(heads)], axis=0
        )
        scale = 1.0 / math.sqrt(HD)
        span = min(max(512 // rows, 1), ring)

        def block(first, state):
            keys = jnp.concatenate([r.kv[first + i, g, :, :width] for i in range(span)], axis=0)
            values = jnp.concatenate([r.kv[first + i, g, :, width:] for i in range(span)], axis=0)
            live = jnp.concatenate([r.masks[first + i] for i in range(span)], axis=1)
            columns = pl.ds(pl.multiple_of(first * rows, span * rows), span * rows)
            bias = r.bias[:, :, columns].reshape(heads * rows, span * rows).astype(jnp.float32)
            scores = matmul_t(stacked, keys) * scale + bias
            scores = jnp.where(live > 0, scores, FAR)
            block_max = jnp.max(scores, axis=-1, keepdims=True)
            new_maxima = block_max if state is None else jnp.maximum(state[0], block_max)
            weights = jnp.exp(scores - new_maxima)
            totals = jnp.sum(weights, axis=-1, keepdims=True)
            summed = matmul(weights.astype(jnp.bfloat16), values)
            if state is not None:
                factor = jnp.exp(state[0] - new_maxima)
                totals, summed = state[1] * factor + totals, state[2] * factor + summed
            return new_maxima, totals, summed

        state = block(0, None)
        if ring > span:
            state = lax.fori_loop(1, ring // span, lambda i, state: block(i * span, state), state)
        attended = state[2] * (1.0 / state[1])
        result = jnp.zeros((rows, width), jnp.float32)
        for head in range(heads):
            result = result + jnp.where(head_of == head, attended[head * rows : (head + 1) * rows], 0.0)
        gate = jax.nn.sigmoid(r.gates[g].astype(jnp.float32))
        r.gated[g] = (result * gate).astype(jnp.bfloat16)

    pending = [(transit_chains[g], step) for step in range(last - 1) for g in outer]
    pending += [(flow, step) for step in range(last - 1) for flow in small_chains]
    share = -(-len(pending) // groups)
    mask_flow.finish()
    loads["bias"].wait()
    kv_flows[inner[0]].relay()
    for number, g in enumerate(inner):
        if number + 1 < groups:
            kv_flows[inner[number + 1]].relay()
        kv_flows[g].complete()
        attention(g)
        for flow, step in pending[number * share : (number + 1) * share]:
            flow.arrive(step)

    def hop(side, g, part):
        piece = pl.ds(part * half, half)
        at = (side, g, part)
        return remote(
            r.sums_out.at[g, piece], r.sums_in.at[side, g, piece], r.sum_send.at[at], r.sum_recv.at[at],
            "fsdp", me + (1 if side == 0 else -1),
        )

    def take(side, g, part):
        hop(side, g, part).wait_recv()
        piece = pl.ds(part * half, half)
        r.total[g, piece] += r.sums_in[side, g, piece].astype(jnp.float32)

    def reduce(stage, g):
        for side, here, goes in ((0, stage, g > stage), (1, last - stage, g < last - stage)):
            if goes:

                @pl.when(me == here)
                def _():
                    for part in (0, 1):
                        piece = pl.ds(part * half, half)
                        if stage > 0:
                            take(side, g, part)
                        r.sums_out[g, piece] = r.total[g, piece].astype(jnp.bfloat16)
                        hop(side, g, part).start()

    heads_out = lax.broadcasted_iota(jnp.int32, (WQ, channels), 1) // (channels // HA)
    tokens = ring * rows

    def atom_weight(i):
        high = r.atom_part.shape[0] // ATOM_MAPS
        return r.atom_all[:, i * high : (i + 1) * high, :].reshape(channels, channels)

    def atom_before():
        normed = layer_norm(r.atom_cond[...]).astype(jnp.bfloat16)
        r.atom_gain[...] = jax.nn.sigmoid(matmul_t(normed, atom_weight(0)) + r.atom_vectors[0:1, :])
        r.atom_shift[...] = matmul_t(normed, atom_weight(1))
        blocks = r.owner.shape[0]

        def hit(column, start):
            span = min(512, tokens)
            for first in range(0, tokens, span):
                token = lax.broadcasted_iota(jnp.int32, (column.shape[0], span), 1) + first
                found = jnp.where(column == token.astype(jnp.float32), 1.0, 0.0).astype(jnp.bfloat16)
                r.hits[pl.ds(start, column.shape[0]), pl.ds(first, span)] = found

        owners = jnp.transpose(r.owner[...].astype(jnp.float32))
        for block in range(blocks):
            hit(owners[:, block : block + 1], RIM + block * WK)
        for side, home in ((0, 0), (1, RIM + count)):
            ends = jnp.broadcast_to(r.owner_rims[side].astype(jnp.float32), (8, WK))
            column = jnp.transpose(ends)[:, 0:1]
            hit(column[WK - RIM :] if side == 0 else column[:RIM], home)
        lane = lax.broadcasted_iota(jnp.int32, (1, WK), 1)

        def window(index, carry):
            base = pl.multiple_of(index * WQ, WQ)
            slot = seat * count + base - RIM + lane
            inside = (slot >= r.bounds[0, index]) & (slot < r.bounds[1, index])
            bias = r.atom_bias[:, pl.ds(base, WQ), :].reshape(HA * WQ, WK).astype(jnp.float32)
            r.masked[index] = jnp.where(inside, bias, FAR)
            return carry

        lax.fori_loop(0, count // WQ, window, 0)

    def atom_after():
        taken = matmul(r.hits[...], r.rows_all[...].reshape(tokens, channels))
        state = r.skip[...].astype(jnp.float32) + taken
        r.state[...] = state[RIM : RIM + count]
        atom_x = (r.atom_gain[...] * layer_norm(state) + r.atom_shift[...]).astype(jnp.bfloat16)
        own_x = atom_x[RIM : RIM + count, :]
        r.atom_query[...] = (matmul_t(own_x, atom_weight(2)) + r.atom_vectors[1:2, :]).astype(jnp.bfloat16)
        r.atom_key[...] = matmul_t(atom_x, atom_weight(3)).astype(jnp.bfloat16)
        r.atom_value[...] = matmul_t(atom_x, atom_weight(4)).astype(jnp.bfloat16)
        r.atom_gate[...] = jax.nn.sigmoid(matmul_t(own_x, atom_weight(5)).astype(jnp.bfloat16).astype(jnp.float32))
        scale = 1.0 / math.sqrt(channels // HA)

        def windows(step, carry):
            bases = [pl.multiple_of(step * (BATCH * WQ) + i * WQ, WQ) for i in range(BATCH)]
            scores = []
            for i, base in enumerate(bases):
                queries = r.atom_query[pl.ds(base, WQ), :]
                stacked = jnp.concatenate(
                    [jnp.where(heads_out == head, queries, 0).astype(jnp.bfloat16) for head in range(HA)],
                    axis=0,
                )
                score = matmul_t(stacked, r.atom_key[pl.ds(base, WK), :])
                scores.append(score * scale + r.masked[step * BATCH + i])
            weights = [jnp.exp(score - jnp.max(score, axis=-1, keepdims=True)) for score in scores]
            results = []
            for base, weight in zip(bases, weights):
                attended = matmul(weight.astype(jnp.bfloat16), r.atom_value[pl.ds(base, WK), :])
                attended = attended * (1.0 / jnp.sum(weight, axis=-1, keepdims=True))
                result = jnp.zeros((WQ, channels), jnp.float32)
                for head in range(HA):
                    result = result + jnp.where(
                        heads_out == head, attended[head * WQ : (head + 1) * WQ], 0.0
                    )
                results.append(result)
            start = pl.multiple_of(step * (BATCH * WQ), BATCH * WQ)
            r.held[pl.ds(start, BATCH * WQ), :] = jnp.concatenate(results, axis=0)
            return carry

        lax.fori_loop(0, count // (BATCH * WQ), windows, 0)
        gated = (r.held[...] * r.atom_gate[...]).astype(jnp.bfloat16)
        fresh = r.state[...] + matmul_t(gated, atom_weight(6))
        final = layer_norm(fresh).astype(jnp.bfloat16)
        moved = matmul_t(r.position[...], final)
        for axis in range(moved.shape[0]):
            r.update[axis] = moved[axis : axis + 1, :]

    for name in ("out", "tin", "tout"):
        loads[name].wait()
    for g in outer:
        transit_chains[g].arrive(last - 1)
        full = joined(r.transit, g)
        hidden = jax.nn.silu(matmul(full, r.tin[0])) * matmul(full, r.tin[1])
        r.total[g] = matmul(r.gated[g], r.out[...]) + matmul(hidden.astype(jnp.bfloat16), r.tout[...])
        reduce(0, g)
    for flow in small_chains:
        flow.arrive(last - 1)
    for copy in swaps():
        copy.start()
    for name in ("skip", "atom_cond", "atom_bias"):
        loads[name].wait()
    for halo in halos:
        halo.finish()
    for copy in swaps():
        copy.wait()
    for stage in range(1, last):
        for g in outer:
            reduce(stage, g)
        if stage == 1:
            atom_before()
    if last == 1:
        atom_before()
    for side, present in ((0, me > 0), (1, me < last)):

        @pl.when(present)
        def _():
            for part in (0, 1):
                take(side, me, part)

    token = (r.act[...].astype(jnp.float32) + r.total[me]).astype(jnp.bfloat16)
    r.token[...] = token
    r.rows_all[seat] = matmul(token, r.project[...].reshape(depth, -1)).astype(jnp.bfloat16)
    rows_flow.begin()
    for flow in cond_chains + attend_chains + transit_chains + small_chains:
        flow.drain()
    for shift in range(1, groups):
        slots(shift, False).wait_send()
    for g in range(groups):
        for side, goes in ((0, g > me), (1, g < me)):

            @pl.when(goes)
            def _():
                for part in (0, 1):
                    hop(side, g, part).wait_send()

    rows_flow.finish()
    atom_after()


def token_layer(near, weights, bounds):
    groups, ring = lax.axis_size("fsdp"), lax.axis_size("seq")
    rows, depth = near["act"].shape
    width = weights["ada"].shape[1]
    count, channels = weights["skip"].shape
    extended = count + 2 * RIM
    dma = pltpu.SemaphoreType.DMA
    vmem, far = pl.BlockSpec(memory_space=pltpu.VMEM), pl.BlockSpec(memory_space=pl.ANY)
    half_type = jnp.bfloat16
    project_part, atom_part = near["project_part"], near["atom_part"]
    outs = dict(
        token=((rows, depth), half_type),
        update=((near["position"].shape[0], 1, count), jnp.float32),
    )
    packed = (groups, groups, rows // 2, 2 * width)
    chains = 4 + 2 * groups
    hops = max(groups - 1, 1)
    length = ring // 2
    scratch = {name: pltpu.VMEM(array.shape, array.dtype) for name, array in weights.items()}
    atoms = lambda height, kind: pltpu.VMEM((height, channels), kind)
    scratch |= dict(
        skip=atoms(extended, half_type),
        atom_cond=atoms(extended, half_type),
        atom_gain=atoms(extended, jnp.float32),
        atom_shift=atoms(extended, jnp.float32),
        atom_key=atoms(extended, half_type),
        atom_value=atoms(extended, half_type),
        atom_query=atoms(count, half_type),
        atom_gate=atoms(count, jnp.float32),
        state=atoms(count, jnp.float32),
        held=atoms(count, jnp.float32),
        hits=pltpu.VMEM((extended, ring * rows), half_type),
        masked=pltpu.VMEM((count // WQ, HA * WQ, WK), jnp.float32),
        owner_rims=pltpu.VMEM((2, 1, near["owner"].shape[1]), jnp.int32),
        rows_all=pltpu.VMEM((ring, rows, channels), half_type),
        atom_all=pltpu.VMEM((groups,) + atom_part.shape, half_type),
        conds=pltpu.VMEM((groups, rows, depth), half_type),
        act_out=pltpu.VMEM(packed[1:], half_type),
        acts=pltpu.VMEM(packed[1:], half_type),
        attend=pltpu.VMEM(packed, half_type),
        transit=pltpu.VMEM(packed, half_type),
        queries=pltpu.VMEM((groups, rows, width), half_type),
        gates=pltpu.VMEM((groups, rows, width), half_type),
        gated=pltpu.VMEM((groups, rows, width), half_type),
        kv=pltpu.VMEM((ring, groups, rows, 2 * width), half_type),
        masks=pltpu.VMEM((ring, 1, rows), jnp.int32),
        project=pltpu.VMEM((groups,) + project_part.shape, half_type),
        total=pltpu.VMEM((groups, rows, depth), jnp.float32),
        sums_out=pltpu.VMEM((groups, rows, depth), half_type),
        sums_in=pltpu.VMEM((2, groups, rows, depth), half_type),
        load=dma((len(weights),)),
        line_send=dma((chains, 2, hops)),
        line_recv=dma((chains, 2, hops)),
        act_send=dma((groups,)),
        act_recv=dma((groups,)),
        seq_send=dma((groups, 2, max(length - 1, 1))),
        seq_recv=dma((groups, 2, max(length - 1, 1))),
        hand_send=dma((groups, 2 * length)),
        hand_recv=dma((groups, 2 * length)),
        spread_send=dma((2, ring)),
        spread_recv=dma((2, ring)),
        halo_send=dma((3, 2)),
        halo_recv=dma((3, 2)),
        swap_send=dma((2,)),
        swap_recv=dma((2,)),
        sum_send=dma((2, groups, 2)),
        sum_recv=dma((2, groups, 2)),
    )
    names = ["bounds"] + list(near) + [name + "_hbm" for name in weights] + list(outs) + list(scratch)
    return pl.pallas_call(
        functools.partial(token_kernel, tuple(names), groups, ring),
        out_shape=tuple(jax.ShapeDtypeStruct(*out) for out in outs.values()),
        in_specs=[pl.BlockSpec(memory_space=pltpu.SMEM)] + [vmem] * len(near) + [far] * len(weights),
        out_specs=tuple([vmem] * len(outs)),
        scratch_shapes=list(scratch.values()),
        compiler_params=pltpu.CompilerParams(
            collective_id=1, has_side_effects=True, vmem_limit_bytes=VMEM_LIMIT
        ),
        name="token_layer",
    )(bounds, *near.values(), *weights.values())


def settle_kernel(token_ref, update_ref, token_out, update_out):
    token_out[...] = token_ref[...]
    update_out[...] = update_ref[...]


def settle(token, update):
    vmem = pl.BlockSpec(memory_space=pltpu.VMEM)
    return pl.pallas_call(
        settle_kernel,
        out_shape=tuple(jax.ShapeDtypeStruct(array.shape, array.dtype) for array in (token, update)),
        in_specs=[vmem] * 2,
        out_specs=(vmem, vmem),
        compiler_params=pltpu.CompilerParams(vmem_limit_bytes=VMEM_LIMIT),
        name="settle",
    )(token, update)


def per_device(
    token_act,
    token_cond,
    pair_bias,
    token_mask,
    ada_weights,
    attention_in,
    attention_out,
    transition_in,
    transition_out,
    token_vectors,
    atom_skip,
    atom_cond,
    atom_bias,
    window_bounds,
    atom_token,
    atom_weights,
    token_to_atom,
    atom_vectors,
    position_out,
):
    channels = atom_cond.shape[1]
    near = dict(
        act=token_act[0],
        cond=token_cond[0],
        mask=token_mask[None],
        vectors=token_vectors,
        owner=atom_token.reshape(-1, WK),
        owner_ends=atom_token.reshape(-1, 1, WK),
        atom_part=jnp.swapaxes(atom_weights, 1, 2).reshape(-1, channels),
        project_part=token_to_atom,
        atom_vectors=atom_vectors,
        position=position_out,
    )
    weights = dict(
        ada=jnp.swapaxes(ada_weights, 1, 2),
        attn=jnp.swapaxes(attention_in, 1, 2),
        bias=pair_bias,
        out=attention_out,
        tin=transition_in,
        tout=transition_out,
        atom_bias=atom_bias,
        skip=atom_skip[0],
        atom_cond=atom_cond,
    )
    token_result, update = settle(*token_layer(near, weights, jnp.swapaxes(window_bounds, 0, 1)))
    return (token_result[None], jnp.transpose(update, (1, 0, 2)))


def solution(mesh):
    in_specs = (
        P(("sample", "fsdp"), "seq", None),
        P(("sample", "fsdp"), "seq", None),
        P("fsdp", "seq", None),
        P("seq"),
        P(None, None, "fsdp"),
        P(None, None, "fsdp"),
        P("fsdp", None),
        P(None, None, "fsdp"),
        P("fsdp", None),
        P(),
        P(("sample", "fsdp"), "seq", None),
        P("seq", None),
        P(None, "seq", None),
        P("seq", None),
        P("seq"),
        P(None, None, "fsdp"),
        P("fsdp", None),
        P(),
        P(),
    )
    out_specs = (P(("sample", "fsdp"), "seq", None), P(("sample", "fsdp"), None, "seq"))
    return jax.shard_map(
        per_device, mesh=mesh, in_specs=in_specs, out_specs=out_specs, check_vma=False
    )
```

```python
import functools
import math
import types

import jax
import jax.numpy as jnp
from jax import lax
from jax.experimental import pallas as pl
from jax.experimental.pallas import tpu as pltpu
from jax.sharding import PartitionSpec as P

HA = 4
WQ = 32
WK = 128
HD = 48
EPS = 1e-05
FAR = -1e30
RIM = (WK - WQ) // 2
ATOM_MAPS = 7
SQUARE = 4
PARTS = 4
BATCH = 8
VMEM_LIMIT = 56 * 1024 * 1024
MESH = pl.DeviceIdType.MESH


def layer_norm(values):
    values = values.astype(jnp.float32)
    center = values - jnp.mean(values, axis=-1, keepdims=True)
    spread = jnp.mean(center * center, axis=-1, keepdims=True)
    return center * lax.rsqrt(spread + EPS)


def matmul(left_side, right_side):
    return jnp.dot(left_side, right_side, preferred_element_type=jnp.float32)


def matmul_t(left_side, right_side):
    return lax.dot_general(
        left_side, right_side, (((1,), (1,)), ((), ())), preferred_element_type=jnp.float32
    )


def remote(source, target, send, recv, axis, peer):
    return pltpu.make_async_remote_copy(
        src_ref=source, dst_ref=target, send_sem=send, recv_sem=recv,
        device_id={axis: peer}, device_id_type=MESH,
    )


class Chain:
    def __init__(self, axis, size, view, send, recv, prefix):
        self.axis, self.size, self.view = axis, size, view
        self.send, self.recv, self.prefix = send, recv, prefix
        self.here = lax.axis_index(axis)

    def guards(self, side, step):
        here, last = self.here, self.size - 1
        if side == 0:
            return (here - step >= 0) & (here < last), here - 1 - step >= 0
        return (here + step <= last) & (here > 0), here + 1 + step <= last

    def copy(self, side, step, arriving):
        sign = 1 if side == 0 else -1
        block = self.view(self.here - sign * (step + (1 if arriving else 0)))
        at = self.prefix + (side, step)
        return remote(block, block, self.send.at[at], self.recv.at[at], self.axis, self.here + sign)

    def begin(self):
        for side in (0, 1):

            @pl.when(self.guards(side, 0)[0])
            def _():
                self.copy(side, 0, False).start()

    def arrive(self, step):
        for side in (0, 1):
            comes = self.guards(side, step)[1]

            @pl.when(comes)
            def _():
                self.copy(side, step, True).wait_recv()

            if step + 1 < self.size - 1:

                @pl.when(self.guards(side, step + 1)[0])
                def _():
                    self.copy(side, step + 1, False).start()

    def drain(self):
        for side in (0, 1):
            for step in range(self.size - 1):

                @pl.when(self.guards(side, step)[0])
                def _():
                    self.copy(side, step, False).wait_send()


class Pairs:
    def __init__(self, axis, size, view, send, recv, partner_send, partner_recv, prefix):
        self.axis, self.view, self.prefix = axis, view, prefix
        self.send, self.recv = send, recv
        self.partner_send, self.partner_recv = partner_send, partner_recv
        self.index = lax.axis_index(axis)
        self.length = size // 2
        self.position = self.index // 2
        self.parity = self.index - 2 * self.position

    def slot(self, position):
        return position * 2 + self.parity

    def partner(self):
        return self.index + 1 - 2 * self.parity

    def guards(self, side, step):
        here, last = self.position, self.length - 1
        if side == 0:
            return (here - step >= 0) & (here < last), here - 1 - step >= 0
        return (here + step <= last) & (here > 0), here + 1 + step <= last

    def copy(self, side, step, arriving):
        sign = 1 if side == 0 else -1
        block = self.view(self.slot(self.position - sign * (step + (1 if arriving else 0))))
        at = self.prefix + (side, step)
        return remote(
            block, block, self.send.at[at], self.recv.at[at], self.axis,
            self.slot(self.position + sign),
        )

    def hand(self, key, origin, arriving):
        block = self.view(origin * 2 + 1 - self.parity if arriving else self.slot(origin))
        at = self.prefix + (key,)
        return remote(
            block, block, self.partner_send.at[at], self.partner_recv.at[at], self.axis, self.partner()
        )

    def begin(self):
        for side in (0, 1):

            @pl.when(self.guards(side, 0)[0])
            def _():
                self.copy(side, 0, False).start()

        self.hand(0, self.position, False).start()

    def key(self, side, step):
        return 1 + side * (self.length - 1) + step

    def origin(self, side, step):
        return self.position - (step + 1) if side == 0 else self.position + step + 1

    def relay(self):
        for step in range(self.length - 1):
            for side in (0, 1):

                @pl.when(self.guards(side, step)[1])
                def _():
                    self.copy(side, step, True).wait_recv()
                    self.hand(self.key(side, step), self.origin(side, step), False).start()

                if step + 1 < self.length - 1:

                    @pl.when(self.guards(side, step + 1)[0])
                    def _():
                        self.copy(side, step + 1, False).start()

    def complete(self):
        self.hand(0, self.position, False).wait_send()
        self.hand(0, self.position, True).wait_recv()
        for step in range(self.length - 1):
            for side in (0, 1):
                goes, comes = self.guards(side, step)

                @pl.when(goes)
                def _():
                    self.copy(side, step, False).wait_send()

                @pl.when(comes)
                def _():
                    self.hand(self.key(side, step), self.origin(side, step), False).wait_send()
                    self.hand(self.key(side, step), self.origin(side, step), True).wait_recv()


class Halo:
    def __init__(self, axis, size, pieces, homes, send, recv, number):
        self.axis, self.pieces, self.homes = axis, pieces, homes
        self.send, self.recv, self.number = send, recv, number
        self.index = lax.axis_index(axis)
        self.present = self.index > 0, self.index < size - 1

    def copy(self, side):
        at = (self.number, side)
        return remote(
            self.pieces[side], self.homes[1 - side], self.send.at[at], self.recv.at[at],
            self.axis, self.index - 1 + 2 * side,
        )

    def begin(self):
        for side in (0, 1):
            home = self.homes[side]

            @pl.when(self.present[side])
            def _():
                self.copy(side).start()

            @pl.when(jnp.logical_not(self.present[side]))
            def _():
                home[...] = jnp.zeros(home.shape, home.dtype)

    def finish(self):
        for side in (0, 1):

            @pl.when(self.present[side])
            def _():
                self.copy(side).wait_send()
                self.copy(1 - side).wait_recv()


class Plane:
    def __init__(self, chain, home, send, recv, number):
        self.chain, self.home, self.send, self.recv, self.number = chain, home, send, recv, number
        seat = lax.axis_index("seq")
        self.base = SQUARE * (seat // SQUARE)
        inside = seat - self.base
        self.across = lax.axis_index("sample")
        self.chip, self.core = inside // 2, inside - 2 * (inside // 2)

    def index(self, across, chip, core):
        return across * SQUARE + chip * 2 + core

    def piece(self, origin, message, across, chip, core):
        if message in (3, 4):
            chip = 1 - chip
        if message in (5, 6):
            across = 1 - across
        if message in (7, 8):
            across, chip = 1 - across, 1 - chip
        block = self.home.at[origin, self.index(across, chip, core)]
        half = self.home.shape[-1] // 2
        if message in (3, 7):
            block = block.at[:, pl.ds(0, half)]
        if message in (5, 8):
            block = block.at[:, pl.ds(half, half)]
        return block

    def copy(self, step, side, message, arriving):
        origin = self.chain.here - (step + 1) if side == 0 else self.chain.here + step + 1
        across, chip, core = self.across, self.chip, self.core
        if message in (2, 3):
            axis, peer, sender = "sample", 1 - across, (1 - across, chip, core)
        elif message in (1, 5):
            axis, peer = "seq", self.base + 2 * (1 - chip) + core
            sender = (across, 1 - chip, core)
        else:
            axis, peer = "seq", self.base + 2 * chip + 1 - core
            sender = (across, chip, 1 - core)
        block = self.piece(origin, message, *(sender if arriving else (across, chip, core)))
        at = (self.number, 2 * step + side, message)
        return remote(block, block, self.send.at[at], self.recv.at[at], axis, peer)

    def each(self, step, actions):
        for side in (0, 1):

            @pl.when(self.chain.guards(side, step)[1])
            def _():
                for action, messages in actions:
                    for message in messages:
                        if action == "start":
                            self.copy(step, side, message, False).start()
                        elif action == "recv":
                            self.copy(step, side, message, True).wait_recv()
                        else:
                            self.copy(step, side, message, False).wait_send()

    def first(self, step):
        self.each(step, [("start", (1, 2, 0))])

    def second(self, step):
        self.each(step, [("recv", (1,)), ("start", (3, 4)), ("recv", (2,)), ("start", (5, 6))])

    def third(self, step):
        self.each(step, [("recv", (3,)), ("start", (7,)), ("recv", (5,)), ("start", (8,))])

    def done(self):
        for step in range(self.chain.size - 1):
            self.each(step, [("recv", (0, 4, 6, 7, 8))])

    def drain(self):
        for step in range(self.chain.size - 1):
            self.each(step, [("send", tuple(range(9)))])


class Spread:
    def __init__(self, axis, size, view, send, recv, number):
        self.axis, self.size, self.view = axis, size, view
        self.send, self.recv, self.number = send, recv, number
        self.here = lax.axis_index(axis)

    def copy(self, shift, arriving):
        block = self.view(lax.rem(self.here + self.size - shift, self.size) if arriving else self.here)
        at = (self.number, shift)
        peer = lax.rem(self.here + shift, self.size)
        return remote(block, block, self.send.at[at], self.recv.at[at], self.axis, peer)

    def begin(self):
        for shift in range(1, self.size):
            self.copy(shift, False).start()

    def finish(self):
        for shift in range(1, self.size):
            self.copy(shift, False).wait_send()
            self.copy(shift, True).wait_recv()


def token_kernel(names, groups, ring, *refs):
    r = types.SimpleNamespace(**dict(zip(names, refs)))
    me, seat = lax.axis_index("fsdp"), lax.axis_index("seq")
    rows, depth = r.act.shape
    width = r.attn.shape[1]
    heads = r.bias.shape[0]
    last = groups - 1
    barrier = pltpu.get_barrier_semaphore()

    def signal(axis, target):
        pl.semaphore_signal(barrier, inc=1, device_id={axis: target}, device_id_type=MESH)

    loads = {
        name: pltpu.make_async_copy(getattr(r, name + "_hbm"), getattr(r, name), r.load.at[number])
        for number, name in enumerate(("attn", "bias", "out", "tin", "tout", "atom_bias"))
    }
    count, channels = r.skip_hbm.shape
    inner_atoms = pl.ds(RIM, count)
    for number, name in enumerate(("skip", "atom_cond")):
        loads[name] = pltpu.make_async_copy(
            getattr(r, name + "_hbm"), getattr(r, name).at[inner_atoms], r.load.at[len(loads)]
        )
    for kind in (0, 1):
        loads[kind] = pltpu.make_async_copy(
            r.ada_hbm.at[kind], r.ada.at[kind, me], r.load.at[len(loads)]
        )

    def pairs(view, *prefix):
        return Pairs("seq", ring, view, r.seq_send, r.seq_recv, r.hand_send, r.hand_recv, prefix)

    halos = [
        Halo(
            "seq", ring, [source.at[pl.ds(start, RIM)] for start in (0, count - RIM)],
            [home.at[pl.ds(start, RIM)] for start in (0, RIM + count)], r.halo_send, r.halo_recv, number,
        )
        for number, (source, home) in enumerate(((r.skip_hbm, r.skip), (r.atom_cond_hbm, r.atom_cond)))
    ]
    halos += [
        Halo(
            "seq", ring, [r.owner_ends.at[0], r.owner_ends.at[r.owner_ends.shape[0] - 1]],
            [r.owner_rims.at[0], r.owner_rims.at[1]], r.halo_send, r.halo_recv, 2,
        )
    ]
    kv_flows = [pairs(lambda slot, g=g: r.kv.at[slot, g], g) for g in range(groups)]
    mask_flow = Spread("seq", ring, lambda slot: r.masks.at[slot], r.spread_send, r.spread_recv, 0)
    rows_flow = Spread("seq", ring, lambda slot: r.rows_all.at[slot], r.spread_send, r.spread_recv, 1)

    for shift in range(1, groups):
        signal("fsdp", lax.rem(me + shift, groups))
    for shift in range(1, ring):
        signal("seq", lax.rem(seat + shift, ring))
    across = lax.axis_index("sample")
    signal("sample", 1 - across)
    expected = last + ring
    for load in [loads[0], loads[1]] + [loads[name] for name in loads if name not in (0, 1)]:
        load.start()

    def chain(number, view):
        return Chain("fsdp", groups, view, r.line_send, r.line_recv, (number,))

    inside = seat - SQUARE * (seat // SQUARE)
    piece = across * SQUARE + inside
    ada_chains = [chain(kind, lambda slot, kind=kind: r.ada.at[kind, slot, piece]) for kind in (0, 1)]
    planes = [
        Plane(flow, r.ada.at[kind], r.plane_send, r.plane_recv, kind)
        for kind, flow in enumerate(ada_chains)
    ]
    part_rows = rows // PARTS

    def row_chains(ref, first):
        return [
            chain(first + part, lambda slot, part=part: ref.at[slot, pl.ds(part * part_rows, part_rows)])
            for part in range(PARTS)
        ]

    attend_chains = row_chains(r.attend, 2)
    transit_chains = row_chains(r.transit, 2 + PARTS)
    parity = seat - 2 * (seat // 2)
    atom_half, project_half = r.atom_part.shape[0] // 2, r.project_part.shape[0] // 2
    atom_rows = pl.ds(pl.multiple_of(parity * atom_half, 16), atom_half)
    project_rows = pl.ds(pl.multiple_of(parity * project_half, 16), project_half)
    small_chains = [
        chain(2 + 2 * PARTS, lambda slot: r.atom_all.at[slot, atom_rows]),
        chain(3 + 2 * PARTS, lambda slot: r.project.at[slot, project_rows]),
    ]

    def swaps():
        partner = seat + 1 - 2 * parity
        blocks = (r.atom_all.at[:, atom_rows], r.project.at[:, project_rows])
        return [
            remote(block, block, r.swap_send.at[i], r.swap_recv.at[i], "seq", partner)
            for i, block in enumerate(blocks)
        ]

    order, found = [me] + [0] * last, 1
    for distance in range(1, groups):
        for sample in (me - distance, me + distance):
            valid = (sample >= 0) & (sample <= last)
            for n in range(1, groups):
                order[n] = jnp.where(valid & (found == n), sample, order[n])
            found = found + jnp.where(valid, 1, 0)

    pl.semaphore_wait(barrier, expected)
    loads[0].wait()
    ada_chains[0].begin()
    r.masks[seat] = r.mask[...]
    r.cond_normed[...] = layer_norm(r.cond[...]).astype(jnp.bfloat16)
    r.act_normed[...] = layer_norm(r.act[...])
    r.atom_all[me, atom_rows] = r.atom_part[atom_rows, :]
    r.project[me, project_rows] = r.project_part[project_rows, :]
    for step in range(last):
        ada_chains[0].arrive(step)
        planes[0].first(step)
        if step > 0:
            planes[0].second(step - 1)
    loads[1].wait()
    ada_chains[1].begin()
    planes[0].second(last - 1)
    for step in range(last):
        planes[0].third(step)
        if step < last - 1:
            ada_chains[1].arrive(step)
            planes[1].first(step)
    planes[0].done()

    def adaptive(kind, target):
        pieces = []
        for g in range(groups):
            columns = slice(g * width, (g + 1) * width)
            maps = r.ada[kind, g].reshape(2 * width, depth)
            both = matmul_t(r.cond_normed[...], maps)
            gate = jax.nn.sigmoid(both[:, :width] + r.vectors[kind : kind + 1, columns])
            pieces.append((gate * r.act_normed[:, columns] + both[:, width:]).astype(jnp.bfloat16))
        target[me] = jnp.concatenate(pieces, axis=1)

    adaptive(0, r.attend)
    for flow in attend_chains:
        flow.begin()
    ada_chains[1].arrive(last - 1)
    planes[1].first(last - 1)
    mask_flow.begin()
    for halo in halos:
        halo.begin()
    for step in range(last - 1):
        planes[1].second(step)
    query_bias = r.vectors[2:3, :width]
    for g in range(1, groups):
        query_bias = jnp.where(me == g, r.vectors[2:3, g * width : (g + 1) * width], query_bias)

    def projections(n):
        full = r.attend[order[n]]
        both = r.attn[1:3].reshape(2 * width, depth)
        r.kv[seat, n] = matmul_t(full, both).astype(jnp.bfloat16)
        kv_flows[n].begin()
        r.queries[n] = (matmul_t(full, r.attn[0]) + query_bias).astype(jnp.bfloat16)
        r.gates[n] = matmul_t(full, r.attn[3]).astype(jnp.bfloat16)

    def attention(g):
        queries = r.queries[g]
        head_of = lax.broadcasted_iota(jnp.int32, (rows, width), 1) // HD
        stacked = jnp.concatenate(
            [jnp.where(head_of == head, queries, 0).astype(jnp.bfloat16) for head in range(heads)], axis=0
        )
        scale = 1.0 / math.sqrt(HD)
        span = min(max(512 // rows, 1), ring)

        def block(first, state):
            keys = jnp.concatenate([r.kv[first + i, g, :, :width] for i in range(span)], axis=0)
            values = jnp.concatenate([r.kv[first + i, g, :, width:] for i in range(span)], axis=0)
            live = jnp.concatenate([r.masks[first + i] for i in range(span)], axis=1)
            columns = pl.ds(pl.multiple_of(first * rows, span * rows), span * rows)
            bias = r.bias[:, :, columns].reshape(heads * rows, span * rows).astype(jnp.float32)
            scores = matmul_t(stacked, keys) * scale + bias
            scores = jnp.where(live > 0, scores, FAR)
            block_max = jnp.max(scores, axis=-1, keepdims=True)
            new_maxima = block_max if state is None else jnp.maximum(state[0], block_max)
            weights = jnp.exp(scores - new_maxima)
            totals = jnp.sum(weights, axis=-1, keepdims=True)
            summed = matmul(weights.astype(jnp.bfloat16), values)
            if state is not None:
                factor = jnp.exp(state[0] - new_maxima)
                totals, summed = state[1] * factor + totals, state[2] * factor + summed
            return new_maxima, totals, summed

        state = block(0, None)
        if ring > span:
            state = lax.fori_loop(1, ring // span, lambda i, state: block(i * span, state), state)
        attended = state[2] * (1.0 / state[1])
        result = jnp.zeros((rows, width), jnp.float32)
        for head in range(heads):
            result = result + jnp.where(head_of == head, attended[head * rows : (head + 1) * rows], 0.0)
        gate = jax.nn.sigmoid(r.gates[g].astype(jnp.float32))
        r.gated[g] = (result * gate).astype(jnp.bfloat16)

    def attend_group(n):
        kv_flows[n].relay()
        kv_flows[n].complete()
        attention(n)

    for flow in attend_chains:
        flow.arrive(0)
    planes[1].second(last - 1)
    for step in range(last):
        planes[1].third(step)
    planes[1].done()
    adaptive(1, r.transit)
    loads["attn"].wait()
    projections(0)
    projections(1)
    for step in range(1, last - 1):
        for flow in attend_chains:
            flow.arrive(step)
        projections(step + 1)
    for flow in transit_chains:
        flow.begin()
    mask_flow.finish()
    loads["bias"].wait()
    attend_group(0)
    if last > 1:
        for flow in attend_chains:
            flow.arrive(last - 1)
        projections(last)
    attend_group(1)
    for flow in small_chains:
        flow.begin()

    def hop(side, g, part):
        piece = pl.ds(part * part_rows, part_rows)
        at = (side, g, part)
        return remote(
            r.sums_out.at[g, piece], r.sums_in.at[side, g, piece], r.sum_send.at[at], r.sum_recv.at[at],
            "fsdp", me + (1 if side == 0 else -1),
        )

    def take(side, g, part):
        hop(side, g, part).wait_recv()
        piece = pl.ds(part * part_rows, part_rows)
        r.total[g, piece] += r.sums_in[side, g, piece].astype(jnp.float32)

    def send(side, g, part):
        piece = pl.ds(part * part_rows, part_rows)
        r.sums_out[g, piece] = r.total[g, piece].astype(jnp.bfloat16)
        hop(side, g, part).start()

    def transition(n):
        g = order[n]
        full = r.transit[g]
        hidden = jax.nn.silu(matmul(full, r.tin[0])) * matmul(full, r.tin[1])
        r.total[g] = matmul(r.gated[n], r.out[...]) + matmul(hidden.astype(jnp.bfloat16), r.tout[...])
        for side, goes in ((0, (me == 0) & (g > 0)), (1, (me == last) & (g < last))):

            @pl.when(goes)
            def _():
                for part in range(PARTS):
                    send(side, g, part)

    def reduce(stage):
        for side, here in ((0, stage), (1, last - stage)):

            @pl.when(me == here)
            def _():
                for g in range(here + 1, groups) if side == 0 else range(here - 1, -1, -1):
                    for part in range(PARTS):
                        take(side, g, part)
                        send(side, g, part)

    heads_out = lax.broadcasted_iota(jnp.int32, (WQ, channels), 1) // (channels // HA)
    tokens = ring * rows

    def atom_weight(i):
        high = r.atom_part.shape[0] // ATOM_MAPS
        return r.atom_all[:, i * high : (i + 1) * high, :].reshape(channels, channels)

    def atom_before():
        normed = layer_norm(r.atom_cond[...]).astype(jnp.bfloat16)
        r.atom_gain[...] = jax.nn.sigmoid(matmul_t(normed, atom_weight(0)) + r.atom_vectors[0:1, :])
        r.atom_shift[...] = matmul_t(normed, atom_weight(1))
        blocks = r.owner.shape[0]

        def hit(column, start):
            span = min(512, tokens)
            for first in range(0, tokens, span):
                token = lax.broadcasted_iota(jnp.int32, (column.shape[0], span), 1) + first
                found = jnp.where(column == token.astype(jnp.float32), 1.0, 0.0).astype(jnp.bfloat16)
                r.hits[pl.ds(start, column.shape[0]), pl.ds(first, span)] = found

        owners = jnp.transpose(r.owner[...].astype(jnp.float32))
        for block in range(blocks):
            hit(owners[:, block : block + 1], RIM + block * WK)
        for side, home in ((0, 0), (1, RIM + count)):
            ends = jnp.broadcast_to(r.owner_rims[side].astype(jnp.float32), (8, WK))
            column = jnp.transpose(ends)[:, 0:1]
            hit(column[WK - RIM :] if side == 0 else column[:RIM], home)
        lane = lax.broadcasted_iota(jnp.int32, (1, WK), 1)

        def window(index, carry):
            base = pl.multiple_of(index * WQ, WQ)
            slot = seat * count + base - RIM + lane
            inside = (slot >= r.bounds[0, index]) & (slot < r.bounds[1, index])
            bias = r.atom_bias[:, pl.ds(base, WQ), :].reshape(HA * WQ, WK).astype(jnp.float32)
            r.masked[index] = jnp.where(inside, bias, FAR)
            return carry

        lax.fori_loop(0, count // WQ, window, 0)

    def atom_after():
        taken = matmul(r.hits[...], r.rows_all[...].reshape(tokens, channels))
        state = r.skip[...].astype(jnp.float32) + taken
        r.state[...] = state[RIM : RIM + count]
        atom_x = (r.atom_gain[...] * layer_norm(state) + r.atom_shift[...]).astype(jnp.bfloat16)
        own_x = atom_x[RIM : RIM + count, :]
        r.atom_query[...] = (matmul_t(own_x, atom_weight(2)) + r.atom_vectors[1:2, :]).astype(jnp.bfloat16)
        r.atom_key[...] = matmul_t(atom_x, atom_weight(3)).astype(jnp.bfloat16)
        r.atom_value[...] = matmul_t(atom_x, atom_weight(4)).astype(jnp.bfloat16)
        r.atom_gate[...] = jax.nn.sigmoid(matmul_t(own_x, atom_weight(5)).astype(jnp.bfloat16).astype(jnp.float32))
        scale = 1.0 / math.sqrt(channels // HA)

        def windows(step, carry):
            bases = [pl.multiple_of(step * (BATCH * WQ) + i * WQ, WQ) for i in range(BATCH)]
            scores = []
            for i, base in enumerate(bases):
                queries = r.atom_query[pl.ds(base, WQ), :]
                stacked = jnp.concatenate(
                    [jnp.where(heads_out == head, queries, 0).astype(jnp.bfloat16) for head in range(HA)],
                    axis=0,
                )
                score = matmul_t(stacked, r.atom_key[pl.ds(base, WK), :])
                scores.append(score * scale + r.masked[step * BATCH + i])
            weights = [jnp.exp(score - jnp.max(score, axis=-1, keepdims=True)) for score in scores]
            results = []
            for base, weight in zip(bases, weights):
                attended = matmul(weight.astype(jnp.bfloat16), r.atom_value[pl.ds(base, WK), :])
                attended = attended * (1.0 / jnp.sum(weight, axis=-1, keepdims=True))
                result = jnp.zeros((WQ, channels), jnp.float32)
                for head in range(HA):
                    result = result + jnp.where(
                        heads_out == head, attended[head * WQ : (head + 1) * WQ], 0.0
                    )
                results.append(result)
            start = pl.multiple_of(step * (BATCH * WQ), BATCH * WQ)
            r.held[pl.ds(start, BATCH * WQ), :] = jnp.concatenate(results, axis=0)
            return carry

        lax.fori_loop(0, count // (BATCH * WQ), windows, 0)
        gated = (r.held[...] * r.atom_gate[...]).astype(jnp.bfloat16)
        fresh = r.state[...] + matmul_t(gated, atom_weight(6))
        final = layer_norm(fresh).astype(jnp.bfloat16)
        moved = matmul_t(r.position[...], final)
        for axis in range(moved.shape[0]):
            r.update[axis] = moved[axis : axis + 1, :]

    for name in ("out", "tin", "tout"):
        loads[name].wait()
    transition(0)
    for step in range(last):
        for flow in transit_chains + small_chains:
            flow.arrive(step)
        if step + 2 < groups:
            attend_group(step + 2)
        transition(step + 1)
    for copy in swaps():
        copy.start()
    for name in ("skip", "atom_cond", "atom_bias"):
        loads[name].wait()
    for halo in halos:
        halo.finish()
    for copy in swaps():
        copy.wait()
    for stage in range(1, last):
        reduce(stage)
        if stage == 1:
            atom_before()
    if last == 1:
        atom_before()
    for side, present in ((0, me > 0), (1, me < last)):

        @pl.when(present)
        def _():
            for part in range(PARTS):
                take(side, me, part)

    token = (r.act[...].astype(jnp.float32) + r.total[me]).astype(jnp.bfloat16)
    r.token[...] = token
    r.rows_all[seat] = matmul(token, r.project[...].reshape(depth, -1)).astype(jnp.bfloat16)
    rows_flow.begin()
    for flow in ada_chains + planes + attend_chains + transit_chains + small_chains:
        flow.drain()
    for g in range(groups):
        for side, goes in ((0, g > me), (1, g < me)):

            @pl.when(goes)
            def _():
                for part in range(PARTS):
                    hop(side, g, part).wait_send()

    rows_flow.finish()
    atom_after()


def token_layer(near, weights, bounds):
    groups, ring = lax.axis_size("fsdp"), lax.axis_size("seq")
    rows, depth = near["act"].shape
    width = weights["attn"].shape[1]
    count, channels = weights["skip"].shape
    extended = count + 2 * RIM
    dma = pltpu.SemaphoreType.DMA
    vmem, far = pl.BlockSpec(memory_space=pltpu.VMEM), pl.BlockSpec(memory_space=pl.ANY)
    half_type = jnp.bfloat16
    project_part, atom_part = near["project_part"], near["atom_part"]
    outs = dict(
        token=((rows, depth), half_type),
        update=((near["position"].shape[0], 1, count), jnp.float32),
    )
    chains = 4 + 2 * PARTS
    hops = max(groups - 1, 1)
    length = ring // 2
    scratch = {name: pltpu.VMEM(array.shape, array.dtype) for name, array in weights.items()}
    atoms = lambda height, kind: pltpu.VMEM((height, channels), kind)
    scratch |= dict(
        skip=atoms(extended, half_type),
        atom_cond=atoms(extended, half_type),
        atom_gain=atoms(extended, jnp.float32),
        atom_shift=atoms(extended, jnp.float32),
        atom_key=atoms(extended, half_type),
        atom_value=atoms(extended, half_type),
        atom_query=atoms(count, half_type),
        atom_gate=atoms(count, jnp.float32),
        state=atoms(count, jnp.float32),
        held=atoms(count, jnp.float32),
        hits=pltpu.VMEM((extended, ring * rows), half_type),
        masked=pltpu.VMEM((count // WQ, HA * WQ, WK), jnp.float32),
        owner_rims=pltpu.VMEM((2, 1, near["owner"].shape[1]), jnp.int32),
        rows_all=pltpu.VMEM((ring, rows, channels), half_type),
        atom_all=pltpu.VMEM((groups,) + atom_part.shape, half_type),
        ada=pltpu.VMEM((2, groups) + weights["ada"].shape[1:], half_type),
        cond_normed=pltpu.VMEM((rows, depth), half_type),
        act_normed=pltpu.VMEM((rows, depth), jnp.float32),
        attend=pltpu.VMEM((groups, rows, depth), half_type),
        transit=pltpu.VMEM((groups, rows, depth), half_type),
        queries=pltpu.VMEM((groups, rows, width), half_type),
        gates=pltpu.VMEM((groups, rows, width), half_type),
        gated=pltpu.VMEM((groups, rows, width), half_type),
        kv=pltpu.VMEM((ring, groups, rows, 2 * width), half_type),
        masks=pltpu.VMEM((ring, 1, rows), jnp.int32),
        project=pltpu.VMEM((groups,) + project_part.shape, half_type),
        total=pltpu.VMEM((groups, rows, depth), jnp.float32),
        sums_out=pltpu.VMEM((groups, rows, depth), half_type),
        sums_in=pltpu.VMEM((2, groups, rows, depth), half_type),
        load=dma((len(weights) + 1,)),
        line_send=dma((chains, 2, hops)),
        line_recv=dma((chains, 2, hops)),
        plane_send=dma((2, 2 * hops, 9)),
        plane_recv=dma((2, 2 * hops, 9)),
        seq_send=dma((groups, 2, max(length - 1, 1))),
        seq_recv=dma((groups, 2, max(length - 1, 1))),
        hand_send=dma((groups, 2 * length)),
        hand_recv=dma((groups, 2 * length)),
        spread_send=dma((2, ring)),
        spread_recv=dma((2, ring)),
        halo_send=dma((3, 2)),
        halo_recv=dma((3, 2)),
        swap_send=dma((2,)),
        swap_recv=dma((2,)),
        sum_send=dma((2, groups, PARTS)),
        sum_recv=dma((2, groups, PARTS)),
    )
    names = ["bounds"] + list(near) + [name + "_hbm" for name in weights] + list(outs) + list(scratch)
    return pl.pallas_call(
        functools.partial(token_kernel, tuple(names), groups, ring),
        out_shape=tuple(jax.ShapeDtypeStruct(*out) for out in outs.values()),
        in_specs=[pl.BlockSpec(memory_space=pltpu.SMEM)] + [vmem] * len(near) + [far] * len(weights),
        out_specs=tuple([vmem] * len(outs)),
        scratch_shapes=list(scratch.values()),
        compiler_params=pltpu.CompilerParams(
            collective_id=1, has_side_effects=True, vmem_limit_bytes=VMEM_LIMIT
        ),
        name="token_layer",
    )(bounds, *near.values(), *weights.values())


def settle_kernel(token_ref, update_ref, token_out, update_out):
    token_out[...] = token_ref[...]
    update_out[...] = update_ref[...]


def settle(token, update):
    vmem = pl.BlockSpec(memory_space=pltpu.VMEM)
    return pl.pallas_call(
        settle_kernel,
        out_shape=tuple(jax.ShapeDtypeStruct(array.shape, array.dtype) for array in (token, update)),
        in_specs=[vmem] * 2,
        out_specs=(vmem, vmem),
        compiler_params=pltpu.CompilerParams(vmem_limit_bytes=VMEM_LIMIT),
        name="settle",
    )(token, update)


def per_device(
    token_act,
    token_cond,
    pair_bias,
    token_mask,
    ada_weights,
    attention_in,
    attention_out,
    transition_in,
    transition_out,
    token_vectors,
    atom_skip,
    atom_cond,
    atom_bias,
    window_bounds,
    atom_token,
    atom_weights,
    token_to_atom,
    atom_vectors,
    position_out,
):
    channels = atom_cond.shape[1]
    helpers = SQUARE * lax.axis_size("sample")
    near = dict(
        act=token_act[0],
        cond=token_cond[0],
        mask=token_mask[None],
        vectors=token_vectors,
        owner=atom_token.reshape(-1, WK),
        owner_ends=atom_token.reshape(-1, 1, WK),
        atom_part=jnp.swapaxes(atom_weights, 1, 2).reshape(-1, channels),
        project_part=token_to_atom,
        atom_vectors=atom_vectors,
        position=position_out,
    )
    weights = dict(
        ada=jnp.swapaxes(ada_weights, 1, 2).reshape(2, helpers, -1, ada_weights.shape[1]),
        attn=jnp.swapaxes(attention_in, 1, 2),
        bias=pair_bias,
        out=attention_out,
        tin=transition_in,
        tout=transition_out,
        atom_bias=atom_bias,
        skip=atom_skip[0],
        atom_cond=atom_cond,
    )
    token_result, update = settle(*token_layer(near, weights, jnp.swapaxes(window_bounds, 0, 1)))
    return (token_result[None], jnp.transpose(update, (1, 0, 2)))


def solution(mesh):
    in_specs = (
        P(("sample", "fsdp"), "seq", None),
        P(("sample", "fsdp"), "seq", None),
        P("fsdp", "seq", None),
        P("seq"),
        P(None, None, "fsdp"),
        P(None, None, "fsdp"),
        P("fsdp", None),
        P(None, None, "fsdp"),
        P("fsdp", None),
        P(),
        P(("sample", "fsdp"), "seq", None),
        P("seq", None),
        P(None, "seq", None),
        P("seq", None),
        P("seq"),
        P(None, None, "fsdp"),
        P("fsdp", None),
        P(),
        P(),
    )
    out_specs = (P(("sample", "fsdp"), "seq", None), P(("sample", "fsdp"), None, "seq"))
    return jax.shard_map(
        per_device, mesh=mesh, in_specs=in_specs, out_specs=out_specs, check_vma=False
    )
```

```python
import functools
import math
import types

import jax
import jax.numpy as jnp
from jax import lax
from jax.experimental import pallas as pl
from jax.experimental.pallas import tpu as pltpu
from jax.sharding import PartitionSpec as P

HA = 4
WQ = 32
WK = 128
HD = 48
EPS = 1e-05
FAR = -1e30
RIM = (WK - WQ) // 2
ATOM_MAPS = 7
SQUARE = 4
PARTS = 4
BATCH = 8
VMEM_LIMIT = 56 * 1024 * 1024
MESH = pl.DeviceIdType.MESH


def layer_norm(values):
    values = values.astype(jnp.float32)
    center = values - jnp.mean(values, axis=-1, keepdims=True)
    spread = jnp.mean(center * center, axis=-1, keepdims=True)
    return center * lax.rsqrt(spread + EPS)


def matmul(left_side, right_side):
    return jnp.dot(left_side, right_side, preferred_element_type=jnp.float32)


def matmul_t(left_side, right_side):
    return lax.dot_general(
        left_side, right_side, (((1,), (1,)), ((), ())), preferred_element_type=jnp.float32
    )


def remote(source, target, send, recv, axis, peer):
    return pltpu.make_async_remote_copy(
        src_ref=source, dst_ref=target, send_sem=send, recv_sem=recv,
        device_id={axis: peer}, device_id_type=MESH,
    )


class Chain:
    def __init__(self, axis, size, view, send, recv, prefix):
        self.axis, self.size, self.view = axis, size, view
        self.send, self.recv, self.prefix = send, recv, prefix
        self.here = lax.axis_index(axis)

    def guards(self, side, step):
        here, last = self.here, self.size - 1
        if side == 0:
            return (here - step >= 0) & (here < last), here - 1 - step >= 0
        return (here + step <= last) & (here > 0), here + 1 + step <= last

    def copy(self, side, step, arriving):
        sign = 1 if side == 0 else -1
        block = self.view(self.here - sign * (step + (1 if arriving else 0)))
        at = self.prefix + (side, step)
        return remote(block, block, self.send.at[at], self.recv.at[at], self.axis, self.here + sign)

    def begin(self):
        for side in (0, 1):

            @pl.when(self.guards(side, 0)[0])
            def _():
                self.copy(side, 0, False).start()

    def arrive(self, step):
        for side in (0, 1):
            comes = self.guards(side, step)[1]

            @pl.when(comes)
            def _():
                self.copy(side, step, True).wait_recv()

            if step + 1 < self.size - 1:

                @pl.when(self.guards(side, step + 1)[0])
                def _():
                    self.copy(side, step + 1, False).start()

    def drain(self):
        for side in (0, 1):
            for step in range(self.size - 1):

                @pl.when(self.guards(side, step)[0])
                def _():
                    self.copy(side, step, False).wait_send()


class Pairs:
    def __init__(self, axis, size, view, send, recv, partner_send, partner_recv, prefix):
        self.axis, self.view, self.prefix = axis, view, prefix
        self.send, self.recv = send, recv
        self.partner_send, self.partner_recv = partner_send, partner_recv
        self.index = lax.axis_index(axis)
        self.length = size // 2
        self.position = self.index // 2
        self.parity = self.index - 2 * self.position

    def slot(self, position):
        return position * 2 + self.parity

    def partner(self):
        return self.index + 1 - 2 * self.parity

    def guards(self, side, step):
        here, last = self.position, self.length - 1
        if side == 0:
            return (here - step >= 0) & (here < last), here - 1 - step >= 0
        return (here + step <= last) & (here > 0), here + 1 + step <= last

    def copy(self, side, step, arriving):
        sign = 1 if side == 0 else -1
        block = self.view(self.slot(self.position - sign * (step + (1 if arriving else 0))))
        at = self.prefix + (side, step)
        return remote(
            block, block, self.send.at[at], self.recv.at[at], self.axis,
            self.slot(self.position + sign),
        )

    def hand(self, key, origin, arriving):
        block = self.view(origin * 2 + 1 - self.parity if arriving else self.slot(origin))
        at = self.prefix + (key,)
        return remote(
            block, block, self.partner_send.at[at], self.partner_recv.at[at], self.axis, self.partner()
        )

    def begin(self):
        for side in (0, 1):

            @pl.when(self.guards(side, 0)[0])
            def _():
                self.copy(side, 0, False).start()

        self.hand(0, self.position, False).start()

    def key(self, side, step):
        return 1 + side * (self.length - 1) + step

    def origin(self, side, step):
        return self.position - (step + 1) if side == 0 else self.position + step + 1

    def relay(self):
        for step in range(self.length - 1):
            for side in (0, 1):

                @pl.when(self.guards(side, step)[1])
                def _():
                    self.copy(side, step, True).wait_recv()
                    self.hand(self.key(side, step), self.origin(side, step), False).start()

                if step + 1 < self.length - 1:

                    @pl.when(self.guards(side, step + 1)[0])
                    def _():
                        self.copy(side, step + 1, False).start()

    def complete(self):
        self.hand(0, self.position, False).wait_send()
        self.hand(0, self.position, True).wait_recv()
        for step in range(self.length - 1):
            for side in (0, 1):
                goes, comes = self.guards(side, step)

                @pl.when(goes)
                def _():
                    self.copy(side, step, False).wait_send()

                @pl.when(comes)
                def _():
                    self.hand(self.key(side, step), self.origin(side, step), False).wait_send()
                    self.hand(self.key(side, step), self.origin(side, step), True).wait_recv()


class Halo:
    def __init__(self, axis, size, pieces, homes, send, recv, number):
        self.axis, self.pieces, self.homes = axis, pieces, homes
        self.send, self.recv, self.number = send, recv, number
        self.index = lax.axis_index(axis)
        self.present = self.index > 0, self.index < size - 1

    def copy(self, side):
        at = (self.number, side)
        return remote(
            self.pieces[side], self.homes[1 - side], self.send.at[at], self.recv.at[at],
            self.axis, self.index - 1 + 2 * side,
        )

    def begin(self):
        for side in (0, 1):
            home = self.homes[side]

            @pl.when(self.present[side])
            def _():
                self.copy(side).start()

            @pl.when(jnp.logical_not(self.present[side]))
            def _():
                home[...] = jnp.zeros(home.shape, home.dtype)

    def finish(self):
        for side in (0, 1):

            @pl.when(self.present[side])
            def _():
                self.copy(side).wait_send()
                self.copy(1 - side).wait_recv()


class Plane:
    def __init__(self, chain, home, send, recv, number):
        self.chain, self.home, self.send, self.recv, self.number = chain, home, send, recv, number
        seat = lax.axis_index("seq")
        self.base = SQUARE * (seat // SQUARE)
        inside = seat - self.base
        self.across = lax.axis_index("sample")
        self.chip, self.core = inside // 2, inside - 2 * (inside // 2)

    def index(self, across, chip, core):
        return across * SQUARE + chip * 2 + core

    def piece(self, origin, message, across, chip, core):
        if message in (3, 4):
            chip = 1 - chip
        if message in (5, 6):
            across = 1 - across
        if message in (7, 8):
            across, chip = 1 - across, 1 - chip
        block = self.home.at[origin, self.index(across, chip, core)]
        half = self.home.shape[-1] // 2
        if message in (3, 7):
            block = block.at[:, pl.ds(0, half)]
        if message in (5, 8):
            block = block.at[:, pl.ds(half, half)]
        return block

    def copy(self, step, side, message, arriving):
        origin = self.chain.here - (step + 1) if side == 0 else self.chain.here + step + 1
        across, chip, core = self.across, self.chip, self.core
        if message in (2, 3):
            axis, peer, sender = "sample", 1 - across, (1 - across, chip, core)
        elif message in (1, 5):
            axis, peer = "seq", self.base + 2 * (1 - chip) + core
            sender = (across, 1 - chip, core)
        else:
            axis, peer = "seq", self.base + 2 * chip + 1 - core
            sender = (across, chip, 1 - core)
        block = self.piece(origin, message, *(sender if arriving else (across, chip, core)))
        at = (self.number, 2 * step + side, message)
        return remote(block, block, self.send.at[at], self.recv.at[at], axis, peer)

    def each(self, step, actions):
        for side in (0, 1):

            @pl.when(self.chain.guards(side, step)[1])
            def _():
                for action, messages in actions:
                    for message in messages:
                        if action == "start":
                            self.copy(step, side, message, False).start()
                        elif action == "recv":
                            self.copy(step, side, message, True).wait_recv()
                        else:
                            self.copy(step, side, message, False).wait_send()

    def first(self, step):
        self.each(step, [("start", (1, 2, 0))])

    def second(self, step):
        self.each(step, [("recv", (1,)), ("start", (3, 4)), ("recv", (2,)), ("start", (5, 6))])

    def third(self, step):
        self.each(step, [("recv", (3,)), ("start", (7,)), ("recv", (5,)), ("start", (8,))])

    def done(self):
        for step in range(self.chain.size - 1):
            self.each(step, [("recv", (0, 4, 6, 7, 8))])

    def drain(self):
        for step in range(self.chain.size - 1):
            self.each(step, [("send", tuple(range(9)))])


class Spread:
    def __init__(self, axis, size, view, send, recv, number):
        self.axis, self.size, self.view = axis, size, view
        self.send, self.recv, self.number = send, recv, number
        self.here = lax.axis_index(axis)

    def copy(self, shift, arriving):
        block = self.view(lax.rem(self.here + self.size - shift, self.size) if arriving else self.here)
        at = (self.number, shift)
        peer = lax.rem(self.here + shift, self.size)
        return remote(block, block, self.send.at[at], self.recv.at[at], self.axis, peer)

    def begin(self):
        for shift in range(1, self.size):
            self.copy(shift, False).start()

    def finish(self):
        for shift in range(1, self.size):
            self.copy(shift, False).wait_send()
            self.copy(shift, True).wait_recv()


def token_kernel(names, groups, ring, *refs):
    r = types.SimpleNamespace(**dict(zip(names, refs)))
    me, seat = lax.axis_index("fsdp"), lax.axis_index("seq")
    rows, depth = r.act.shape
    width = r.attn.shape[1]
    heads = r.bias.shape[0]
    last = groups - 1
    barrier = pltpu.get_barrier_semaphore()

    def signal(axis, target):
        pl.semaphore_signal(barrier, inc=1, device_id={axis: target}, device_id_type=MESH)

    loads = {
        name: pltpu.make_async_copy(getattr(r, name + "_hbm"), getattr(r, name), r.load.at[number])
        for number, name in enumerate(("attn", "bias", "out", "tin", "tout", "atom_bias"))
    }
    count, channels = r.skip_hbm.shape
    inner_atoms = pl.ds(RIM, count)
    for number, name in enumerate(("skip", "atom_cond")):
        loads[name] = pltpu.make_async_copy(
            getattr(r, name + "_hbm"), getattr(r, name).at[inner_atoms], r.load.at[len(loads)]
        )
    for kind in (0, 1):
        loads[kind] = pltpu.make_async_copy(
            r.ada_hbm.at[kind], r.ada.at[kind, me], r.load.at[len(loads)]
        )

    def pairs(view, *prefix):
        return Pairs("seq", ring, view, r.seq_send, r.seq_recv, r.hand_send, r.hand_recv, prefix)

    halos = [
        Halo(
            "seq", ring, [source.at[pl.ds(start, RIM)] for start in (0, count - RIM)],
            [home.at[pl.ds(start, RIM)] for start in (0, RIM + count)], r.halo_send, r.halo_recv, number,
        )
        for number, (source, home) in enumerate(((r.skip_hbm, r.skip), (r.atom_cond_hbm, r.atom_cond)))
    ]
    halos += [
        Halo(
            "seq", ring, [r.owner_ends.at[0], r.owner_ends.at[r.owner_ends.shape[0] - 1]],
            [r.owner_rims.at[0], r.owner_rims.at[1]], r.halo_send, r.halo_recv, 2,
        )
    ]
    kv_flows = [pairs(lambda slot, g=g: r.kv.at[slot, g], g) for g in range(groups)]
    mask_flow = Spread("seq", ring, lambda slot: r.masks.at[slot], r.spread_send, r.spread_recv, 0)
    rows_flow = Spread("seq", ring, lambda slot: r.rows_all.at[slot], r.spread_send, r.spread_recv, 1)

    for shift in range(1, groups):
        signal("fsdp", lax.rem(me + shift, groups))
    for shift in range(1, ring):
        signal("seq", lax.rem(seat + shift, ring))
    across = lax.axis_index("sample")
    signal("sample", 1 - across)
    expected = last + ring
    for load in [loads[0], loads[1]] + [loads[name] for name in loads if name not in (0, 1)]:
        load.start()

    def chain(number, view):
        return Chain("fsdp", groups, view, r.line_send, r.line_recv, (number,))

    inside = seat - SQUARE * (seat // SQUARE)
    piece = across * SQUARE + inside
    cut = depth // 2
    ada_chains = [
        [
            chain(
                2 * kind + side,
                lambda slot, kind=kind, side=side: r.ada.at[kind, slot, piece, :, pl.ds(side * cut, cut)],
            )
            for side in (0, 1)
        ]
        for kind in (0, 1)
    ]
    planes = [
        Plane(flow[0], r.ada.at[kind], r.plane_send, r.plane_recv, kind)
        for kind, flow in enumerate(ada_chains)
    ]
    part_rows = rows // PARTS

    def row_chains(ref, first):
        return [
            chain(first + part, lambda slot, part=part: ref.at[slot, pl.ds(part * part_rows, part_rows)])
            for part in range(PARTS)
        ]

    attend_chains = row_chains(r.attend, 4)
    transit_chains = row_chains(r.transit, 4 + PARTS)
    parity = seat - 2 * (seat // 2)
    atom_half, project_half = r.atom_part.shape[0] // 2, r.project_part.shape[0] // 2
    atom_rows = pl.ds(pl.multiple_of(parity * atom_half, 16), atom_half)
    project_rows = pl.ds(pl.multiple_of(parity * project_half, 16), project_half)
    small_chains = [
        chain(4 + 2 * PARTS, lambda slot: r.atom_all.at[slot, atom_rows]),
        chain(5 + 2 * PARTS, lambda slot: r.project.at[slot, project_rows]),
    ]

    def swaps():
        partner = seat + 1 - 2 * parity
        blocks = (r.atom_all.at[:, atom_rows], r.project.at[:, project_rows])
        return [
            remote(block, block, r.swap_send.at[i], r.swap_recv.at[i], "seq", partner)
            for i, block in enumerate(blocks)
        ]

    order, found = [me] + [0] * last, 1
    for distance in range(1, groups):
        for sample in (me - distance, me + distance):
            valid = (sample >= 0) & (sample <= last)
            for n in range(1, groups):
                order[n] = jnp.where(valid & (found == n), sample, order[n])
            found = found + jnp.where(valid, 1, 0)

    pl.semaphore_wait(barrier, expected)
    loads[0].wait()
    for flow in ada_chains[0]:
        flow.begin()
    r.masks[seat] = r.mask[...]
    r.cond_normed[...] = layer_norm(r.cond[...]).astype(jnp.bfloat16)
    r.act_normed[...] = layer_norm(r.act[...])
    r.atom_all[me, atom_rows] = r.atom_part[atom_rows, :]
    r.project[me, project_rows] = r.project_part[project_rows, :]
    for step in range(last):
        for flow in ada_chains[0]:
            flow.arrive(step)
        planes[0].first(step)
        if step > 0:
            planes[0].second(step - 1)
    loads[1].wait()
    for flow in ada_chains[1]:
        flow.begin()
    planes[0].second(last - 1)
    for step in range(last):
        planes[0].third(step)
        if step < last - 1:
            for flow in ada_chains[1]:
                flow.arrive(step)
            planes[1].first(step)
    planes[0].done()

    def adaptive(kind, target):
        pieces = []
        for g in range(groups):
            columns = slice(g * width, (g + 1) * width)
            maps = r.ada[kind, g].reshape(2 * width, depth)
            both = matmul_t(r.cond_normed[...], maps)
            gate = jax.nn.sigmoid(both[:, :width] + r.vectors[kind : kind + 1, columns])
            pieces.append((gate * r.act_normed[:, columns] + both[:, width:]).astype(jnp.bfloat16))
        target[me] = jnp.concatenate(pieces, axis=1)

    adaptive(0, r.attend)
    for flow in attend_chains:
        flow.begin()
    for flow in ada_chains[1]:
        flow.arrive(last - 1)
    planes[1].first(last - 1)
    planes[1].second(0)
    mask_flow.begin()
    for halo in halos:
        halo.begin()
    query_bias = r.vectors[2:3, :width]
    for g in range(1, groups):
        query_bias = jnp.where(me == g, r.vectors[2:3, g * width : (g + 1) * width], query_bias)

    def projections(n):
        full = r.attend[order[n]]
        both = r.attn[1:3].reshape(2 * width, depth)
        r.kv[seat, n] = matmul_t(full, both).astype(jnp.bfloat16)
        kv_flows[n].begin()
        r.queries[n] = (matmul_t(full, r.attn[0]) + query_bias).astype(jnp.bfloat16)
        r.gates[n] = matmul_t(full, r.attn[3]).astype(jnp.bfloat16)

    def attention(g):
        queries = r.queries[g]
        head_of = lax.broadcasted_iota(jnp.int32, (rows, width), 1) // HD
        stacked = jnp.concatenate(
            [jnp.where(head_of == head, queries, 0).astype(jnp.bfloat16) for head in range(heads)], axis=0
        )
        scale = 1.0 / math.sqrt(HD)
        span = min(max(512 // rows, 1), ring)

        def block(first, state):
            keys = jnp.concatenate([r.kv[first + i, g, :, :width] for i in range(span)], axis=0)
            values = jnp.concatenate([r.kv[first + i, g, :, width:] for i in range(span)], axis=0)
            live = jnp.concatenate([r.masks[first + i] for i in range(span)], axis=1)
            columns = pl.ds(pl.multiple_of(first * rows, span * rows), span * rows)
            bias = r.bias[:, :, columns].reshape(heads * rows, span * rows).astype(jnp.float32)
            scores = matmul_t(stacked, keys) * scale + bias
            scores = jnp.where(live > 0, scores, FAR)
            block_max = jnp.max(scores, axis=-1, keepdims=True)
            new_maxima = block_max if state is None else jnp.maximum(state[0], block_max)
            weights = jnp.exp(scores - new_maxima)
            totals = jnp.sum(weights, axis=-1, keepdims=True)
            summed = matmul(weights.astype(jnp.bfloat16), values)
            if state is not None:
                factor = jnp.exp(state[0] - new_maxima)
                totals, summed = state[1] * factor + totals, state[2] * factor + summed
            return new_maxima, totals, summed

        state = block(0, None)
        if ring > span:
            state = lax.fori_loop(1, ring // span, lambda i, state: block(i * span, state), state)
        attended = state[2] * (1.0 / state[1])
        result = jnp.zeros((rows, width), jnp.float32)
        for head in range(heads):
            result = result + jnp.where(head_of == head, attended[head * rows : (head + 1) * rows], 0.0)
        gate = jax.nn.sigmoid(r.gates[g].astype(jnp.float32))
        r.gated[g] = (result * gate).astype(jnp.bfloat16)

    def attend_group(n):
        kv_flows[n].relay()
        kv_flows[n].complete()
        attention(n)

    for flow in attend_chains:
        flow.arrive(0)
    for step in range(1, last):
        planes[1].second(step)
    for step in range(last - 1):
        planes[1].third(step)
    for step in range(1, last - 1):
        for flow in attend_chains:
            flow.arrive(step)
    planes[1].third(last - 1)
    planes[1].done()
    adaptive(1, r.transit)
    for flow in transit_chains:
        flow.begin()
    loads["attn"].wait()
    for n in range(last):
        projections(n)
    if last > 1:
        for flow in attend_chains:
            flow.arrive(last - 1)
    projections(last)
    mask_flow.finish()
    loads["bias"].wait()
    attend_group(0)
    attend_group(1)
    for flow in small_chains:
        flow.begin()

    def hop(side, g, part):
        piece = pl.ds(part * part_rows, part_rows)
        at = (side, g, part)
        return remote(
            r.sums_out.at[g, piece], r.sums_in.at[side, g, piece], r.sum_send.at[at], r.sum_recv.at[at],
            "fsdp", me + (1 if side == 0 else -1),
        )

    def take(side, g, part):
        hop(side, g, part).wait_recv()
        piece = pl.ds(part * part_rows, part_rows)
        r.total[g, piece] += r.sums_in[side, g, piece].astype(jnp.float32)

    def send(side, g, part):
        piece = pl.ds(part * part_rows, part_rows)
        r.sums_out[g, piece] = r.total[g, piece].astype(jnp.bfloat16)
        hop(side, g, part).start()

    def far(number, size):
        piece = pl.ds(number * size, size)
        return remote(
            r.sums_out.at[last - me, piece], r.sums_far.at[piece], r.far_send.at[number],
            r.far_recv.at[number], "fsdp", last - me,
        )

    half = rows // 2

    def transition(n, number, size):
        g = order[n]
        piece = pl.ds(number * size, size)
        parts = range(number * size // part_rows, (number + 1) * size // part_rows)
        full = r.transit[g, piece]
        hidden = jax.nn.silu(matmul(full, r.tin[0])) * matmul(full, r.tin[1])
        sums = matmul(r.gated[n, piece], r.out[...])
        r.total[g, piece] = sums + matmul(hidden.astype(jnp.bfloat16), r.tout[...])
        ends = ((0, 0, last, 1), (1, last, 0, last - 1))
        for side, end, other, next_to_end in ends:
            beyond = g > me if side == 0 else g < me
            begins = (me == end) & beyond & (g != other)
            if last > 1:
                begins = begins | ((me == next_to_end) & (g == other))

            @pl.when(begins)
            def _():
                for part in parts:
                    send(side, g, part)

        if n == last:

            @pl.when(((me == 0) & (g == last)) | ((me == last) & (g == 0)))
            def _():
                r.sums_out[g, piece] = r.total[g, piece].astype(jnp.bfloat16)
                far(number, size).start()

    def reduce(stage):
        for side, here, other in ((0, stage, last), (1, last - stage, 0)):

            @pl.when(me == here)
            def _():
                for g in range(here + 1, groups) if side == 0 else range(here - 1, -1, -1):
                    if stage > 1 or g != other:
                        for part in range(PARTS):
                            take(side, g, part)
                            send(side, g, part)

    heads_out = lax.broadcasted_iota(jnp.int32, (WQ, channels), 1) // (channels // HA)
    tokens = ring * rows

    def atom_weight(i):
        high = r.atom_part.shape[0] // ATOM_MAPS
        return r.atom_all[:, i * high : (i + 1) * high, :].reshape(channels, channels)

    def atom_before():
        normed = layer_norm(r.atom_cond[...]).astype(jnp.bfloat16)
        r.atom_gain[...] = jax.nn.sigmoid(matmul_t(normed, atom_weight(0)) + r.atom_vectors[0:1, :])
        r.atom_shift[...] = matmul_t(normed, atom_weight(1))
        blocks = r.owner.shape[0]

        def hit(column, start):
            span = min(512, tokens)
            for first in range(0, tokens, span):
                token = lax.broadcasted_iota(jnp.int32, (column.shape[0], span), 1) + first
                found = jnp.where(column == token.astype(jnp.float32), 1.0, 0.0).astype(jnp.bfloat16)
                r.hits[pl.ds(start, column.shape[0]), pl.ds(first, span)] = found

        owners = jnp.transpose(r.owner[...].astype(jnp.float32))
        for block in range(blocks):
            hit(owners[:, block : block + 1], RIM + block * WK)
        for side, home in ((0, 0), (1, RIM + count)):
            ends = jnp.broadcast_to(r.owner_rims[side].astype(jnp.float32), (8, WK))
            column = jnp.transpose(ends)[:, 0:1]
            hit(column[WK - RIM :] if side == 0 else column[:RIM], home)
        lane = lax.broadcasted_iota(jnp.int32, (1, WK), 1)

        def window(index, carry):
            base = pl.multiple_of(index * WQ, WQ)
            slot = seat * count + base - RIM + lane
            inside = (slot >= r.bounds[0, index]) & (slot < r.bounds[1, index])
            bias = r.atom_bias[:, pl.ds(base, WQ), :].reshape(HA * WQ, WK).astype(jnp.float32)
            r.masked[index] = jnp.where(inside, bias, FAR)
            return carry

        lax.fori_loop(0, count // WQ, window, 0)

    def atom_after():
        taken = matmul(r.hits[...], r.rows_all[...].reshape(tokens, channels))
        state = r.skip[...].astype(jnp.float32) + taken
        r.state[...] = state[RIM : RIM + count]
        atom_x = (r.atom_gain[...] * layer_norm(state) + r.atom_shift[...]).astype(jnp.bfloat16)
        own_x = atom_x[RIM : RIM + count, :]
        r.atom_query[...] = (matmul_t(own_x, atom_weight(2)) + r.atom_vectors[1:2, :]).astype(jnp.bfloat16)
        r.atom_key[...] = matmul_t(atom_x, atom_weight(3)).astype(jnp.bfloat16)
        r.atom_value[...] = matmul_t(atom_x, atom_weight(4)).astype(jnp.bfloat16)
        r.atom_gate[...] = jax.nn.sigmoid(matmul_t(own_x, atom_weight(5)).astype(jnp.bfloat16).astype(jnp.float32))
        scale = 1.0 / math.sqrt(channels // HA)

        def windows(step, carry):
            bases = [pl.multiple_of(step * (BATCH * WQ) + i * WQ, WQ) for i in range(BATCH)]
            scores = []
            for i, base in enumerate(bases):
                queries = r.atom_query[pl.ds(base, WQ), :]
                stacked = jnp.concatenate(
                    [jnp.where(heads_out == head, queries, 0).astype(jnp.bfloat16) for head in range(HA)],
                    axis=0,
                )
                score = matmul_t(stacked, r.atom_key[pl.ds(base, WK), :])
                scores.append(score * scale + r.masked[step * BATCH + i])
            weights = [jnp.exp(score - jnp.max(score, axis=-1, keepdims=True)) for score in scores]
            results = []
            for base, weight in zip(bases, weights):
                attended = matmul(weight.astype(jnp.bfloat16), r.atom_value[pl.ds(base, WK), :])
                attended = attended * (1.0 / jnp.sum(weight, axis=-1, keepdims=True))
                result = jnp.zeros((WQ, channels), jnp.float32)
                for head in range(HA):
                    result = result + jnp.where(
                        heads_out == head, attended[head * WQ : (head + 1) * WQ], 0.0
                    )
                results.append(result)
            start = pl.multiple_of(step * (BATCH * WQ), BATCH * WQ)
            r.held[pl.ds(start, BATCH * WQ), :] = jnp.concatenate(results, axis=0)
            return carry

        lax.fori_loop(0, count // (BATCH * WQ), windows, 0)
        gated = (r.held[...] * r.atom_gate[...]).astype(jnp.bfloat16)
        fresh = r.state[...] + matmul_t(gated, atom_weight(6))
        final = layer_norm(fresh).astype(jnp.bfloat16)
        moved = matmul_t(r.position[...], final)
        for axis in range(moved.shape[0]):
            r.update[axis] = moved[axis : axis + 1, :]

    for name in ("out", "tin", "tout"):
        loads[name].wait()
    transition(0, 0, rows)
    for step in range(last - 1):
        for flow in transit_chains + small_chains:
            flow.arrive(step)
        attend_group(step + 2)
        transition(step + 1, 0, rows)
    for number in (0, 1):
        for flow in transit_chains[number * PARTS // 2 : (number + 1) * PARTS // 2]:
            flow.arrive(last - 1)
        transition(last, number, half)
    for flow in small_chains:
        flow.arrive(last - 1)
    for copy in swaps():
        copy.start()
    for stage in range(1, last):
        reduce(stage)
    for name in ("skip", "atom_cond", "atom_bias"):
        loads[name].wait()
    for halo in halos:
        halo.finish()
    for copy in swaps():
        copy.wait()
    atom_before()
    if last > 1:
        for side, present in ((0, me > 0), (1, me < last)):

            @pl.when(present)
            def _():
                for part in range(PARTS):
                    take(side, me, part)

    @pl.when((me == 0) | (me == last))
    def _():
        for number in (0, 1):
            far(number, half).wait_recv()
        r.total[me] += r.sums_far[...].astype(jnp.float32)

    token = (r.act[...].astype(jnp.float32) + r.total[me]).astype(jnp.bfloat16)
    r.token[...] = token
    r.rows_all[seat] = matmul(token, r.project[...].reshape(depth, -1)).astype(jnp.bfloat16)
    rows_flow.begin()

    @pl.when((me == 0) | (me == last))
    def _():
        for number in (0, 1):
            far(number, half).wait_send()

    for flow in ada_chains[0] + ada_chains[1] + planes + attend_chains + transit_chains + small_chains:
        flow.drain()
    for g in range(groups):
        for side, goes in ((0, (g > me) & (g - me < last)), (1, (g < me) & (me - g < last))):

            @pl.when(goes)
            def _():
                for part in range(PARTS):
                    hop(side, g, part).wait_send()

    rows_flow.finish()
    atom_after()


def token_layer(near, weights, bounds):
    groups, ring = lax.axis_size("fsdp"), lax.axis_size("seq")
    rows, depth = near["act"].shape
    width = weights["attn"].shape[1]
    count, channels = weights["skip"].shape
    extended = count + 2 * RIM
    dma = pltpu.SemaphoreType.DMA
    vmem, far = pl.BlockSpec(memory_space=pltpu.VMEM), pl.BlockSpec(memory_space=pl.ANY)
    half_type = jnp.bfloat16
    project_part, atom_part = near["project_part"], near["atom_part"]
    outs = dict(
        token=((rows, depth), half_type),
        update=((near["position"].shape[0], 1, count), jnp.float32),
    )
    chains = 6 + 2 * PARTS
    hops = max(groups - 1, 1)
    length = ring // 2
    scratch = {name: pltpu.VMEM(array.shape, array.dtype) for name, array in weights.items()}
    atoms = lambda height, kind: pltpu.VMEM((height, channels), kind)
    scratch |= dict(
        skip=atoms(extended, half_type),
        atom_cond=atoms(extended, half_type),
        atom_gain=atoms(extended, jnp.float32),
        atom_shift=atoms(extended, jnp.float32),
        atom_key=atoms(extended, half_type),
        atom_value=atoms(extended, half_type),
        atom_query=atoms(count, half_type),
        atom_gate=atoms(count, jnp.float32),
        state=atoms(count, jnp.float32),
        held=atoms(count, jnp.float32),
        hits=pltpu.VMEM((extended, ring * rows), half_type),
        masked=pltpu.VMEM((count // WQ, HA * WQ, WK), jnp.float32),
        owner_rims=pltpu.VMEM((2, 1, near["owner"].shape[1]), jnp.int32),
        rows_all=pltpu.VMEM((ring, rows, channels), half_type),
        atom_all=pltpu.VMEM((groups,) + atom_part.shape, half_type),
        ada=pltpu.VMEM((2, groups) + weights["ada"].shape[1:], half_type),
        cond_normed=pltpu.VMEM((rows, depth), half_type),
        act_normed=pltpu.VMEM((rows, depth), jnp.float32),
        attend=pltpu.VMEM((groups, rows, depth), half_type),
        transit=pltpu.VMEM((groups, rows, depth), half_type),
        queries=pltpu.VMEM((groups, rows, width), half_type),
        gates=pltpu.VMEM((groups, rows, width), half_type),
        gated=pltpu.VMEM((groups, rows, width), half_type),
        kv=pltpu.VMEM((ring, groups, rows, 2 * width), half_type),
        masks=pltpu.VMEM((ring, 1, rows), jnp.int32),
        project=pltpu.VMEM((groups,) + project_part.shape, half_type),
        total=pltpu.VMEM((groups, rows, depth), jnp.float32),
        sums_out=pltpu.VMEM((groups, rows, depth), half_type),
        sums_in=pltpu.VMEM((2, groups, rows, depth), half_type),
        load=dma((len(weights) + 1,)),
        line_send=dma((chains, 2, hops)),
        line_recv=dma((chains, 2, hops)),
        plane_send=dma((2, 2 * hops, 9)),
        plane_recv=dma((2, 2 * hops, 9)),
        seq_send=dma((groups, 2, max(length - 1, 1))),
        seq_recv=dma((groups, 2, max(length - 1, 1))),
        hand_send=dma((groups, 2 * length)),
        hand_recv=dma((groups, 2 * length)),
        spread_send=dma((2, ring)),
        spread_recv=dma((2, ring)),
        halo_send=dma((3, 2)),
        halo_recv=dma((3, 2)),
        swap_send=dma((2,)),
        swap_recv=dma((2,)),
        sums_far=pltpu.VMEM((rows, depth), half_type),
        far_send=dma((2,)),
        far_recv=dma((2,)),
        sum_send=dma((2, groups, PARTS)),
        sum_recv=dma((2, groups, PARTS)),
    )
    names = ["bounds"] + list(near) + [name + "_hbm" for name in weights] + list(outs) + list(scratch)
    return pl.pallas_call(
        functools.partial(token_kernel, tuple(names), groups, ring),
        out_shape=tuple(jax.ShapeDtypeStruct(*out) for out in outs.values()),
        in_specs=[pl.BlockSpec(memory_space=pltpu.SMEM)] + [vmem] * len(near) + [far] * len(weights),
        out_specs=tuple([vmem] * len(outs)),
        scratch_shapes=list(scratch.values()),
        compiler_params=pltpu.CompilerParams(
            collective_id=1, has_side_effects=True, vmem_limit_bytes=VMEM_LIMIT
        ),
        name="token_layer",
    )(bounds, *near.values(), *weights.values())


def settle_kernel(token_ref, update_ref, token_out, update_out):
    token_out[...] = token_ref[...]
    update_out[...] = update_ref[...]


def settle(token, update):
    vmem = pl.BlockSpec(memory_space=pltpu.VMEM)
    return pl.pallas_call(
        settle_kernel,
        out_shape=tuple(jax.ShapeDtypeStruct(array.shape, array.dtype) for array in (token, update)),
        in_specs=[vmem] * 2,
        out_specs=(vmem, vmem),
        compiler_params=pltpu.CompilerParams(vmem_limit_bytes=VMEM_LIMIT),
        name="settle",
    )(token, update)


def per_device(
    token_act,
    token_cond,
    pair_bias,
    token_mask,
    ada_weights,
    attention_in,
    attention_out,
    transition_in,
    transition_out,
    token_vectors,
    atom_skip,
    atom_cond,
    atom_bias,
    window_bounds,
    atom_token,
    atom_weights,
    token_to_atom,
    atom_vectors,
    position_out,
):
    channels = atom_cond.shape[1]
    helpers = SQUARE * lax.axis_size("sample")
    near = dict(
        act=token_act[0],
        cond=token_cond[0],
        mask=token_mask[None],
        vectors=token_vectors,
        owner=atom_token.reshape(-1, WK),
        owner_ends=atom_token.reshape(-1, 1, WK),
        atom_part=jnp.swapaxes(atom_weights, 1, 2).reshape(-1, channels),
        project_part=token_to_atom,
        atom_vectors=atom_vectors,
        position=position_out,
    )
    weights = dict(
        ada=jnp.swapaxes(ada_weights, 1, 2).reshape(2, helpers, -1, ada_weights.shape[1]),
        attn=jnp.swapaxes(attention_in, 1, 2),
        bias=pair_bias,
        out=attention_out,
        tin=transition_in,
        tout=transition_out,
        atom_bias=atom_bias,
        skip=atom_skip[0],
        atom_cond=atom_cond,
    )
    token_result, update = settle(*token_layer(near, weights, jnp.swapaxes(window_bounds, 0, 1)))
    return (token_result[None], jnp.transpose(update, (1, 0, 2)))


def solution(mesh):
    in_specs = (
        P(("sample", "fsdp"), "seq", None),
        P(("sample", "fsdp"), "seq", None),
        P("fsdp", "seq", None),
        P("seq"),
        P(None, None, "fsdp"),
        P(None, None, "fsdp"),
        P("fsdp", None),
        P(None, None, "fsdp"),
        P("fsdp", None),
        P(),
        P(("sample", "fsdp"), "seq", None),
        P("seq", None),
        P(None, "seq", None),
        P("seq", None),
        P("seq"),
        P(None, None, "fsdp"),
        P("fsdp", None),
        P(),
        P(),
    )
    out_specs = (P(("sample", "fsdp"), "seq", None), P(("sample", "fsdp"), None, "seq"))
    return jax.shard_map(
        per_device, mesh=mesh, in_specs=in_specs, out_specs=out_specs, check_vma=False
    )
```

```python
import functools
import math
import types

import jax
import jax.numpy as jnp
from jax import lax
from jax.experimental import pallas as pl
from jax.experimental.pallas import tpu as pltpu
from jax.sharding import PartitionSpec as P

HA = 4
WQ = 32
WK = 128
HD = 48
EPS = 1e-05
FAR = -1e30
RIM = (WK - WQ) // 2
ATOM_MAPS = 7
SQUARE = 4
PARTS = 4
BATCH = 8
VMEM_LIMIT = 56 * 1024 * 1024
MESH = pl.DeviceIdType.MESH


def layer_norm(values):
    values = values.astype(jnp.float32)
    center = values - jnp.mean(values, axis=-1, keepdims=True)
    spread = jnp.mean(center * center, axis=-1, keepdims=True)
    return center * lax.rsqrt(spread + EPS)


def matmul(left_side, right_side):
    return jnp.dot(left_side, right_side, preferred_element_type=jnp.float32)


def matmul_t(left_side, right_side):
    return lax.dot_general(
        left_side, right_side, (((1,), (1,)), ((), ())), preferred_element_type=jnp.float32
    )


def pack(array):
    half = array.shape[-2] // 2
    return jnp.concatenate([array[..., :half, :], array[..., half:, :]], axis=-1)


def unpack(array):
    half = array.shape[-1] // 2
    return jnp.concatenate([array[..., :half], array[..., half:]], axis=-2)


def remote(source, target, send, recv, axis, peer):
    return pltpu.make_async_remote_copy(
        src_ref=source, dst_ref=target, send_sem=send, recv_sem=recv,
        device_id={axis: peer}, device_id_type=MESH,
    )


class Chain:
    def __init__(self, axis, size, view, send, recv, prefix):
        self.axis, self.size, self.view = axis, size, view
        self.send, self.recv, self.prefix = send, recv, prefix
        self.here = lax.axis_index(axis)

    def guards(self, side, step):
        here, last = self.here, self.size - 1
        if side == 0:
            return (here - step >= 0) & (here < last), here - 1 - step >= 0
        return (here + step <= last) & (here > 0), here + 1 + step <= last

    def copy(self, side, step, arriving):
        sign = 1 if side == 0 else -1
        block = self.view(self.here - sign * (step + (1 if arriving else 0)))
        at = self.prefix + (side, step)
        return remote(block, block, self.send.at[at], self.recv.at[at], self.axis, self.here + sign)

    def begin(self):
        for side in (0, 1):

            @pl.when(self.guards(side, 0)[0])
            def _():
                self.copy(side, 0, False).start()

    def arrive(self, step):
        for side in (0, 1):
            comes = self.guards(side, step)[1]

            @pl.when(comes)
            def _():
                self.copy(side, step, True).wait_recv()

            if step + 1 < self.size - 1:

                @pl.when(self.guards(side, step + 1)[0])
                def _():
                    self.copy(side, step + 1, False).start()

    def drain(self):
        for side in (0, 1):
            for step in range(self.size - 1):

                @pl.when(self.guards(side, step)[0])
                def _():
                    self.copy(side, step, False).wait_send()


class Pairs:
    def __init__(self, axis, size, view, send, recv, partner_send, partner_recv, prefix):
        self.axis, self.view, self.prefix = axis, view, prefix
        self.send, self.recv = send, recv
        self.partner_send, self.partner_recv = partner_send, partner_recv
        self.index = lax.axis_index(axis)
        self.length = size // 2
        self.position = self.index // 2
        self.parity = self.index - 2 * self.position

    def slot(self, position):
        return position * 2 + self.parity

    def partner(self):
        return self.index + 1 - 2 * self.parity

    def guards(self, side, step):
        here, last = self.position, self.length - 1
        if side == 0:
            return (here - step >= 0) & (here < last), here - 1 - step >= 0
        return (here + step <= last) & (here > 0), here + 1 + step <= last

    def copy(self, side, step, arriving):
        sign = 1 if side == 0 else -1
        block = self.view(self.slot(self.position - sign * (step + (1 if arriving else 0))))
        at = self.prefix + (side, step)
        return remote(
            block, block, self.send.at[at], self.recv.at[at], self.axis,
            self.slot(self.position + sign),
        )

    def hand(self, key, origin, arriving):
        block = self.view(origin * 2 + 1 - self.parity if arriving else self.slot(origin))
        at = self.prefix + (key,)
        return remote(
            block, block, self.partner_send.at[at], self.partner_recv.at[at], self.axis, self.partner()
        )

    def begin(self):
        for side in (0, 1):

            @pl.when(self.guards(side, 0)[0])
            def _():
                self.copy(side, 0, False).start()

        self.hand(0, self.position, False).start()

    def key(self, side, step):
        return 1 + side * (self.length - 1) + step

    def origin(self, side, step):
        return self.position - (step + 1) if side == 0 else self.position + step + 1

    def relay(self):
        for step in range(self.length - 1):
            for side in (0, 1):

                @pl.when(self.guards(side, step)[1])
                def _():
                    self.copy(side, step, True).wait_recv()
                    self.hand(self.key(side, step), self.origin(side, step), False).start()

                if step + 1 < self.length - 1:

                    @pl.when(self.guards(side, step + 1)[0])
                    def _():
                        self.copy(side, step + 1, False).start()

    def complete(self):
        self.hand(0, self.position, False).wait_send()
        self.hand(0, self.position, True).wait_recv()
        for step in range(self.length - 1):
            for side in (0, 1):
                goes, comes = self.guards(side, step)

                @pl.when(goes)
                def _():
                    self.copy(side, step, False).wait_send()

                @pl.when(comes)
                def _():
                    self.hand(self.key(side, step), self.origin(side, step), False).wait_send()
                    self.hand(self.key(side, step), self.origin(side, step), True).wait_recv()


class Halo:
    def __init__(self, axis, size, pieces, homes, send, recv, number):
        self.axis, self.pieces, self.homes = axis, pieces, homes
        self.send, self.recv, self.number = send, recv, number
        self.index = lax.axis_index(axis)
        self.present = self.index > 0, self.index < size - 1

    def copy(self, side):
        at = (self.number, side)
        return remote(
            self.pieces[side], self.homes[1 - side], self.send.at[at], self.recv.at[at],
            self.axis, self.index - 1 + 2 * side,
        )

    def begin(self):
        for side in (0, 1):
            home = self.homes[side]

            @pl.when(self.present[side])
            def _():
                self.copy(side).start()

            @pl.when(jnp.logical_not(self.present[side]))
            def _():
                home[...] = jnp.zeros(home.shape, home.dtype)

    def finish(self):
        for side in (0, 1):

            @pl.when(self.present[side])
            def _():
                self.copy(side).wait_send()
                self.copy(1 - side).wait_recv()


class Spread:
    def __init__(self, axis, size, view, send, recv, number):
        self.axis, self.size, self.view = axis, size, view
        self.send, self.recv, self.number = send, recv, number
        self.here = lax.axis_index(axis)

    def copy(self, shift, arriving):
        block = self.view(lax.rem(self.here + self.size - shift, self.size) if arriving else self.here)
        at = (self.number, shift)
        peer = lax.rem(self.here + shift, self.size)
        return remote(block, block, self.send.at[at], self.recv.at[at], self.axis, peer)

    def begin(self):
        for shift in range(1, self.size):
            self.copy(shift, False).start()

    def finish(self):
        for shift in range(1, self.size):
            self.copy(shift, False).wait_send()
            self.copy(shift, True).wait_recv()


def token_kernel(names, groups, ring, *refs):
    r = types.SimpleNamespace(**dict(zip(names, refs)))
    me, seat = lax.axis_index("fsdp"), lax.axis_index("seq")
    rows, depth = r.act.shape
    width = r.ada.shape[1]
    heads = r.bias.shape[0]
    half = rows // 2
    part_rows = rows // PARTS
    last = groups - 1
    barrier = pltpu.get_barrier_semaphore()

    def signal(axis, target):
        pl.semaphore_signal(barrier, inc=1, device_id={axis: target}, device_id_type=MESH)

    loads = {
        name: pltpu.make_async_copy(getattr(r, name + "_hbm"), getattr(r, name), r.load.at[number])
        for number, name in enumerate(("ada", "attn", "bias", "out", "tin", "tout", "atom_bias"))
    }
    count, channels = r.skip_hbm.shape
    inner_atoms = pl.ds(RIM, count)
    for number, name in enumerate(("skip", "atom_cond")):
        loads[name] = pltpu.make_async_copy(
            getattr(r, name + "_hbm"), getattr(r, name).at[inner_atoms], r.load.at[len(loads)]
        )

    def pairs(view, *prefix):
        return Pairs("seq", ring, view, r.seq_send, r.seq_recv, r.hand_send, r.hand_recv, prefix)

    halos = [
        Halo(
            "seq", ring, [source.at[pl.ds(start, RIM)] for start in (0, count - RIM)],
            [home.at[pl.ds(start, RIM)] for start in (0, RIM + count)], r.halo_send, r.halo_recv, number,
        )
        for number, (source, home) in enumerate(((r.skip_hbm, r.skip), (r.atom_cond_hbm, r.atom_cond)))
    ]
    halos += [
        Halo(
            "seq", ring, [r.owner_ends.at[0], r.owner_ends.at[r.owner_ends.shape[0] - 1]],
            [r.owner_rims.at[0], r.owner_rims.at[1]], r.halo_send, r.halo_recv, 2,
        )
    ]
    kv_flows = [pairs(lambda slot, g=g: r.kv.at[slot, g], g) for g in range(groups)]
    mask_flow = Spread("seq", ring, lambda slot: r.masks.at[slot], r.spread_send, r.spread_recv, 0)
    rows_flow = Spread("seq", ring, lambda slot: r.rows_all.at[slot], r.spread_send, r.spread_recv, 1)

    for shift in range(1, groups):
        signal("fsdp", lax.rem(me + shift, groups))
    for shift in range(1, ring):
        signal("seq", lax.rem(seat + shift, ring))
    expected = last + ring - 1
    for load in loads.values():
        load.start()

    def chain(number, view):
        return Chain("fsdp", groups, view, r.line_send, r.line_recv, (number,))

    cond_chains = [
        chain(part, lambda slot, part=part: r.conds.at[slot, pl.ds(part * half, half)]) for part in (0, 1)
    ]
    attend_chains = [chain(2 + g, lambda slot, g=g: r.attend.at[slot, g]) for g in range(groups)]
    transit_chains = [
        chain(2 + groups + g, lambda slot, g=g: r.transit.at[slot, g]) for g in range(groups)
    ]
    base = SQUARE * (seat // SQUARE)
    inside = seat - base
    atom_quarter, project_quarter = r.atom_pad.shape[0] // SQUARE, r.project_part.shape[0] // SQUARE

    def quarters(number):
        return (
            pl.ds(pl.multiple_of(number * atom_quarter, 16), atom_quarter),
            pl.ds(pl.multiple_of(number * project_quarter, 16), project_quarter),
        )

    atom_rows, project_rows = quarters(inside)
    small_chains = [
        chain(2 + 2 * groups, lambda slot: r.atom_all.at[slot, atom_rows]),
        chain(3 + 2 * groups, lambda slot: r.project.at[slot, project_rows]),
    ]

    def swaps(shift, arriving):
        peer = base + lax.rem(inside + shift, SQUARE)
        ones, others = quarters(lax.rem(inside + SQUARE - shift, SQUARE) if arriving else inside)
        blocks = (r.atom_all.at[:, ones], r.project.at[:, others])
        return [
            remote(block, block, r.swap_send.at[i, shift], r.swap_recv.at[i, shift], "seq", peer)
            for i, block in enumerate(blocks)
        ]

    r.conds[me] = layer_norm(r.cond[...]).astype(jnp.bfloat16)
    r.masks[seat] = r.mask[...]
    height = r.atom_part.shape[0]
    r.atom_pad[0:height] = r.atom_part[...]
    r.atom_pad[height:] = jnp.zeros((r.atom_pad.shape[0] - height, channels), jnp.bfloat16)
    r.atom_all[me, atom_rows] = r.atom_pad[atom_rows, :]
    r.project[me, project_rows] = r.project_part[project_rows, :]
    pl.semaphore_wait(barrier, expected)
    for flow in cond_chains:
        flow.begin()
    act_normed = layer_norm(r.act[...]).astype(jnp.bfloat16)
    for g in range(groups):
        r.act_out[g] = pack(act_normed[:, g * width : (g + 1) * width])

    def slots(shift, arriving):
        peer = lax.rem(me + shift, groups)
        landing = lax.rem(me + groups - shift, groups) if arriving else me
        return remote(
            r.act_out.at[peer], r.acts.at[landing], r.act_send.at[shift], r.act_recv.at[shift],
            "fsdp", peer,
        )

    for shift in range(1, groups):
        slots(shift, False).start()
    mask_flow.begin()
    for halo in halos:
        halo.begin()
    offsets = r.vectors[:, :width]
    for g in range(1, groups):
        offsets = jnp.where(me == g, r.vectors[:, g * width : (g + 1) * width], offsets)

    def adaptive(sample, packed):
        rows_in = r.conds[sample]
        values = unpack(packed).astype(jnp.float32)

        def one(scale, shift, vector):
            gate = jax.nn.sigmoid(matmul_t(rows_in, r.ada[scale]) + offsets[vector : vector + 1, :])
            return pack((gate * values + matmul_t(rows_in, r.ada[shift])).astype(jnp.bfloat16))

        r.attend[me, sample] = one(0, 1, 0)
        r.transit[me, sample] = one(2, 3, 1)

    loads["ada"].wait()
    adaptive(me, r.act_out[me])
    inner = sorted(range(groups), key=lambda g: max(g, last - g))
    outer = sorted(range(groups), key=lambda g: (-max(g, last - g), g))
    for step in range(last):
        for flow in cond_chains:
            flow.arrive(step)
        for side in (0, 1):

            @pl.when(cond_chains[0].guards(side, step)[1])
            def _():
                origin = me - (step + 1) if side == 0 else me + step + 1
                slots(step + 1 if side == 0 else last - step, True).wait_recv()
                adaptive(origin, r.acts[origin])

        for g in inner:
            if max(g, last - g) == step + 1:
                attend_chains[g].begin()

    def joined(ref, g):
        return jnp.concatenate([unpack(ref[origin, g]) for origin in range(groups)], axis=1)

    def projections(g):
        full = joined(r.attend, g)
        r.queries[g] = (matmul_t(full, r.attn[0]) + offsets[2:3, :]).astype(jnp.bfloat16)
        both = r.attn[1:3].reshape(2 * width, depth)
        r.kv[seat, g] = matmul_t(full, both).astype(jnp.bfloat16)
        kv_flows[g].begin()
        r.gates[g] = matmul_t(full, r.attn[3]).astype(jnp.bfloat16)

    for step in range(last - 1):
        for g in inner:
            attend_chains[g].arrive(step)
    for g in outer:
        transit_chains[g].begin()
    loads["attn"].wait()
    for g in inner:
        attend_chains[g].arrive(last - 1)
        projections(g)
    for flow in small_chains:
        flow.begin()

    def attention(g):
        queries = r.queries[g]
        head_of = lax.broadcasted_iota(jnp.int32, (rows, width), 1) // HD
        stacked = jnp.concatenate(
            [jnp.where(head_of == head, queries, 0).astype(jnp.bfloat16) for head in range(heads)], axis=0
        )
        scale = 1.0 / math.sqrt(HD)
        span = min(max(512 // rows, 1), ring)

        def block(first, state):
            keys = jnp.concatenate([r.kv[first + i, g, :, :width] for i in range(span)], axis=0)
            values = jnp.concatenate([r.kv[first + i, g, :, width:] for i in range(span)], axis=0)
            live = jnp.concatenate([r.masks[first + i] for i in range(span)], axis=1)
            columns = pl.ds(pl.multiple_of(first * rows, span * rows), span * rows)
            bias = r.bias[:, :, columns].reshape(heads * rows, span * rows).astype(jnp.float32)
            scores = matmul_t(stacked, keys) * scale + bias
            scores = jnp.where(live > 0, scores, FAR)
            block_max = jnp.max(scores, axis=-1, keepdims=True)
            new_maxima = block_max if state is None else jnp.maximum(state[0], block_max)
            weights = jnp.exp(scores - new_maxima)
            totals = jnp.sum(weights, axis=-1, keepdims=True)
            summed = matmul(weights.astype(jnp.bfloat16), values)
            if state is not None:
                factor = jnp.exp(state[0] - new_maxima)
                totals, summed = state[1] * factor + totals, state[2] * factor + summed
            return new_maxima, totals, summed

        state = block(0, None)
        if ring > span:
            state = lax.fori_loop(1, ring // span, lambda i, state: block(i * span, state), state)
        attended = state[2] * (1.0 / state[1])
        result = jnp.zeros((rows, width), jnp.float32)
        for head in range(heads):
            result = result + jnp.where(head_of == head, attended[head * rows : (head + 1) * rows], 0.0)
        gate = jax.nn.sigmoid(r.gates[g].astype(jnp.float32))
        r.gated[g] = (result * gate).astype(jnp.bfloat16)

    pending = [(transit_chains[g], step) for step in range(last - 1) for g in outer]
    pending += [(flow, step) for step in range(last - 1) for flow in small_chains]
    share = -(-len(pending) // groups)
    mask_flow.finish()
    loads["bias"].wait()
    kv_flows[inner[0]].relay()
    for number, g in enumerate(inner):
        if number + 1 < groups:
            kv_flows[inner[number + 1]].relay()
        kv_flows[g].complete()
        attention(g)
        for flow, step in pending[number * share : (number + 1) * share]:
            flow.arrive(step)

    def hop(side, g, part):
        piece = pl.ds(part * part_rows, part_rows)
        at = (side, g, part)
        return remote(
            r.sums_out.at[g, piece], r.sums_in.at[side, g, piece], r.sum_send.at[at], r.sum_recv.at[at],
            "fsdp", me + (1 if side == 0 else -1),
        )

    def take(side, g, part):
        hop(side, g, part).wait_recv()
        piece = pl.ds(part * part_rows, part_rows)
        r.total[g, piece] += r.sums_in[side, g, piece].astype(jnp.float32)

    def reduce(stage, g):
        for side, here, goes in ((0, stage, g > stage), (1, last - stage, g < last - stage)):
            if goes:

                @pl.when(me == here)
                def _():
                    for part in range(PARTS):
                        piece = pl.ds(part * part_rows, part_rows)
                        if stage > 0:
                            take(side, g, part)
                        r.sums_out[g, piece] = r.total[g, piece].astype(jnp.bfloat16)
                        hop(side, g, part).start()

    heads_out = lax.broadcasted_iota(jnp.int32, (WQ, channels), 1) // (channels // HA)
    tokens = ring * rows

    def atom_weight(i):
        high = r.atom_part.shape[0] // ATOM_MAPS
        return r.atom_all[:, i * high : (i + 1) * high, :].reshape(channels, channels)

    def atom_before():
        normed = layer_norm(r.atom_cond[...]).astype(jnp.bfloat16)
        r.atom_gain[...] = jax.nn.sigmoid(matmul_t(normed, atom_weight(0)) + r.atom_vectors[0:1, :])
        r.atom_shift[...] = matmul_t(normed, atom_weight(1))
        blocks = r.owner.shape[0]

        def hit(column, start):
            span = min(512, tokens)
            for first in range(0, tokens, span):
                token = lax.broadcasted_iota(jnp.int32, (column.shape[0], span), 1) + first
                found = jnp.where(column == token.astype(jnp.float32), 1.0, 0.0).astype(jnp.bfloat16)
                r.hits[pl.ds(start, column.shape[0]), pl.ds(first, span)] = found

        owners = jnp.transpose(r.owner[...].astype(jnp.float32))
        for block in range(blocks):
            hit(owners[:, block : block + 1], RIM + block * WK)
        for side, home in ((0, 0), (1, RIM + count)):
            ends = jnp.broadcast_to(r.owner_rims[side].astype(jnp.float32), (8, WK))
            column = jnp.transpose(ends)[:, 0:1]
            hit(column[WK - RIM :] if side == 0 else column[:RIM], home)
        lane = lax.broadcasted_iota(jnp.int32, (1, WK), 1)

        def window(index, carry):
            base = pl.multiple_of(index * WQ, WQ)
            slot = seat * count + base - RIM + lane
            inside = (slot >= r.bounds[0, index]) & (slot < r.bounds[1, index])
            bias = r.atom_bias[:, pl.ds(base, WQ), :].reshape(HA * WQ, WK).astype(jnp.float32)
            r.masked[index] = jnp.where(inside, bias, FAR)
            return carry

        lax.fori_loop(0, count // WQ, window, 0)

    def atom_after():
        taken = matmul(r.hits[...], r.rows_all[...].reshape(tokens, channels))
        state = r.skip[...].astype(jnp.float32) + taken
        r.state[...] = state[RIM : RIM + count]
        atom_x = (r.atom_gain[...] * layer_norm(state) + r.atom_shift[...]).astype(jnp.bfloat16)
        own_x = atom_x[RIM : RIM + count, :]
        r.atom_query[...] = (matmul_t(own_x, atom_weight(2)) + r.atom_vectors[1:2, :]).astype(jnp.bfloat16)
        r.atom_key[...] = matmul_t(atom_x, atom_weight(3)).astype(jnp.bfloat16)
        r.atom_value[...] = matmul_t(atom_x, atom_weight(4)).astype(jnp.bfloat16)
        r.atom_gate[...] = jax.nn.sigmoid(matmul_t(own_x, atom_weight(5)).astype(jnp.bfloat16).astype(jnp.float32))
        scale = 1.0 / math.sqrt(channels // HA)

        def windows(step, carry):
            bases = [pl.multiple_of(step * (BATCH * WQ) + i * WQ, WQ) for i in range(BATCH)]
            scores = []
            for i, base in enumerate(bases):
                queries = r.atom_query[pl.ds(base, WQ), :]
                stacked = jnp.concatenate(
                    [jnp.where(heads_out == head, queries, 0).astype(jnp.bfloat16) for head in range(HA)],
                    axis=0,
                )
                score = matmul_t(stacked, r.atom_key[pl.ds(base, WK), :])
                scores.append(score * scale + r.masked[step * BATCH + i])
            weights = [jnp.exp(score - jnp.max(score, axis=-1, keepdims=True)) for score in scores]
            results = []
            for base, weight in zip(bases, weights):
                attended = matmul(weight.astype(jnp.bfloat16), r.atom_value[pl.ds(base, WK), :])
                attended = attended * (1.0 / jnp.sum(weight, axis=-1, keepdims=True))
                result = jnp.zeros((WQ, channels), jnp.float32)
                for head in range(HA):
                    result = result + jnp.where(
                        heads_out == head, attended[head * WQ : (head + 1) * WQ], 0.0
                    )
                results.append(result)
            start = pl.multiple_of(step * (BATCH * WQ), BATCH * WQ)
            r.held[pl.ds(start, BATCH * WQ), :] = jnp.concatenate(results, axis=0)
            return carry

        lax.fori_loop(0, count // (BATCH * WQ), windows, 0)
        gated = (r.held[...] * r.atom_gate[...]).astype(jnp.bfloat16)
        fresh = r.state[...] + matmul_t(gated, atom_weight(6))
        final = layer_norm(fresh).astype(jnp.bfloat16)
        moved = matmul_t(r.position[...], final)
        for axis in range(moved.shape[0]):
            r.update[axis] = moved[axis : axis + 1, :]

    for name in ("out", "tin", "tout"):
        loads[name].wait()
    for g in outer:
        transit_chains[g].arrive(last - 1)
        full = joined(r.transit, g)
        hidden = jax.nn.silu(matmul(full, r.tin[0])) * matmul(full, r.tin[1])
        r.total[g] = matmul(r.gated[g], r.out[...]) + matmul(hidden.astype(jnp.bfloat16), r.tout[...])
        reduce(0, g)
    for flow in small_chains:
        flow.arrive(last - 1)
    for shift in range(1, SQUARE):
        for copy in swaps(shift, False):
            copy.start()
    for stage in range(1, last):
        for g in outer:
            reduce(stage, g)
    for name in ("skip", "atom_cond", "atom_bias"):
        loads[name].wait()
    for halo in halos:
        halo.finish()
    for shift in range(1, SQUARE):
        for copy in swaps(shift, False):
            copy.wait_send()
        for copy in swaps(shift, True):
            copy.wait_recv()
    atom_before()
    for side, present in ((0, me > 0), (1, me < last)):

        @pl.when(present)
        def _():
            for part in range(PARTS):
                take(side, me, part)

    token = (r.act[...].astype(jnp.float32) + r.total[me]).astype(jnp.bfloat16)
    r.token[...] = token
    r.rows_all[seat] = matmul(token, r.project[...].reshape(depth, -1)).astype(jnp.bfloat16)
    rows_flow.begin()
    for flow in cond_chains + attend_chains + transit_chains + small_chains:
        flow.drain()
    for shift in range(1, groups):
        slots(shift, False).wait_send()
    for g in range(groups):
        for side, goes in ((0, g > me), (1, g < me)):

            @pl.when(goes)
            def _():
                for part in range(PARTS):
                    hop(side, g, part).wait_send()

    rows_flow.finish()
    atom_after()


def token_layer(near, weights, bounds):
    groups, ring = lax.axis_size("fsdp"), lax.axis_size("seq")
    rows, depth = near["act"].shape
    width = weights["ada"].shape[1]
    count, channels = weights["skip"].shape
    extended = count + 2 * RIM
    dma = pltpu.SemaphoreType.DMA
    vmem, far = pl.BlockSpec(memory_space=pltpu.VMEM), pl.BlockSpec(memory_space=pl.ANY)
    half_type = jnp.bfloat16
    project_part, atom_part = near["project_part"], near["atom_part"]
    outs = dict(
        token=((rows, depth), half_type),
        update=((near["position"].shape[0], 1, count), jnp.float32),
    )
    packed = (groups, groups, rows // 2, 2 * width)
    chains = 4 + 2 * groups
    high = atom_part.shape[0] // ATOM_MAPS
    padded = high * SQUARE * -(-ATOM_MAPS // SQUARE)
    hops = max(groups - 1, 1)
    length = ring // 2
    scratch = {name: pltpu.VMEM(array.shape, array.dtype) for name, array in weights.items()}
    atoms = lambda height, kind: pltpu.VMEM((height, channels), kind)
    scratch |= dict(
        skip=atoms(extended, half_type),
        atom_cond=atoms(extended, half_type),
        atom_gain=atoms(extended, jnp.float32),
        atom_shift=atoms(extended, jnp.float32),
        atom_key=atoms(extended, half_type),
        atom_value=atoms(extended, half_type),
        atom_query=atoms(count, half_type),
        atom_gate=atoms(count, jnp.float32),
        state=atoms(count, jnp.float32),
        held=atoms(count, jnp.float32),
        hits=pltpu.VMEM((extended, ring * rows), half_type),
        masked=pltpu.VMEM((count // WQ, HA * WQ, WK), jnp.float32),
        owner_rims=pltpu.VMEM((2, 1, near["owner"].shape[1]), jnp.int32),
        rows_all=pltpu.VMEM((ring, rows, channels), half_type),
        atom_pad=pltpu.VMEM((padded, channels), half_type),
        atom_all=pltpu.VMEM((groups, padded, channels), half_type),
        conds=pltpu.VMEM((groups, rows, depth), half_type),
        act_out=pltpu.VMEM(packed[1:], half_type),
        acts=pltpu.VMEM(packed[1:], half_type),
        attend=pltpu.VMEM(packed, half_type),
        transit=pltpu.VMEM(packed, half_type),
        queries=pltpu.VMEM((groups, rows, width), half_type),
        gates=pltpu.VMEM((groups, rows, width), half_type),
        gated=pltpu.VMEM((groups, rows, width), half_type),
        kv=pltpu.VMEM((ring, groups, rows, 2 * width), half_type),
        masks=pltpu.VMEM((ring, 1, rows), jnp.int32),
        project=pltpu.VMEM((groups,) + project_part.shape, half_type),
        total=pltpu.VMEM((groups, rows, depth), jnp.float32),
        sums_out=pltpu.VMEM((groups, rows, depth), half_type),
        sums_in=pltpu.VMEM((2, groups, rows, depth), half_type),
        load=dma((len(weights),)),
        line_send=dma((chains, 2, hops)),
        line_recv=dma((chains, 2, hops)),
        act_send=dma((groups,)),
        act_recv=dma((groups,)),
        seq_send=dma((groups, 2, max(length - 1, 1))),
        seq_recv=dma((groups, 2, max(length - 1, 1))),
        hand_send=dma((groups, 2 * length)),
        hand_recv=dma((groups, 2 * length)),
        spread_send=dma((2, ring)),
        spread_recv=dma((2, ring)),
        halo_send=dma((3, 2)),
        halo_recv=dma((3, 2)),
        swap_send=dma((2, SQUARE)),
        swap_recv=dma((2, SQUARE)),
        sum_send=dma((2, groups, PARTS)),
        sum_recv=dma((2, groups, PARTS)),
    )
    names = ["bounds"] + list(near) + [name + "_hbm" for name in weights] + list(outs) + list(scratch)
    return pl.pallas_call(
        functools.partial(token_kernel, tuple(names), groups, ring),
        out_shape=tuple(jax.ShapeDtypeStruct(*out) for out in outs.values()),
        in_specs=[pl.BlockSpec(memory_space=pltpu.SMEM)] + [vmem] * len(near) + [far] * len(weights),
        out_specs=tuple([vmem] * len(outs)),
        scratch_shapes=list(scratch.values()),
        compiler_params=pltpu.CompilerParams(
            collective_id=1, has_side_effects=True, vmem_limit_bytes=VMEM_LIMIT
        ),
        name="token_layer",
    )(bounds, *near.values(), *weights.values())


def settle_kernel(token_ref, update_ref, token_out, update_out):
    token_out[...] = token_ref[...]
    update_out[...] = update_ref[...]


def settle(token, update):
    vmem = pl.BlockSpec(memory_space=pltpu.VMEM)
    return pl.pallas_call(
        settle_kernel,
        out_shape=tuple(jax.ShapeDtypeStruct(array.shape, array.dtype) for array in (token, update)),
        in_specs=[vmem] * 2,
        out_specs=(vmem, vmem),
        compiler_params=pltpu.CompilerParams(vmem_limit_bytes=VMEM_LIMIT),
        name="settle",
    )(token, update)


def per_device(
    token_act,
    token_cond,
    pair_bias,
    token_mask,
    ada_weights,
    attention_in,
    attention_out,
    transition_in,
    transition_out,
    token_vectors,
    atom_skip,
    atom_cond,
    atom_bias,
    window_bounds,
    atom_token,
    atom_weights,
    token_to_atom,
    atom_vectors,
    position_out,
):
    channels = atom_cond.shape[1]
    near = dict(
        act=token_act[0],
        cond=token_cond[0],
        mask=token_mask[None],
        vectors=token_vectors,
        owner=atom_token.reshape(-1, WK),
        owner_ends=atom_token.reshape(-1, 1, WK),
        atom_part=jnp.swapaxes(atom_weights, 1, 2).reshape(-1, channels),
        project_part=token_to_atom,
        atom_vectors=atom_vectors,
        position=position_out,
    )
    weights = dict(
        ada=jnp.swapaxes(ada_weights, 1, 2),
        attn=jnp.swapaxes(attention_in, 1, 2),
        bias=pair_bias,
        out=attention_out,
        tin=transition_in,
        tout=transition_out,
        atom_bias=atom_bias,
        skip=atom_skip[0],
        atom_cond=atom_cond,
    )
    token_result, update = settle(*token_layer(near, weights, jnp.swapaxes(window_bounds, 0, 1)))
    return (token_result[None], jnp.transpose(update, (1, 0, 2)))


def solution(mesh):
    in_specs = (
        P(("sample", "fsdp"), "seq", None),
        P(("sample", "fsdp"), "seq", None),
        P("fsdp", "seq", None),
        P("seq"),
        P(None, None, "fsdp"),
        P(None, None, "fsdp"),
        P("fsdp", None),
        P(None, None, "fsdp"),
        P("fsdp", None),
        P(),
        P(("sample", "fsdp"), "seq", None),
        P("seq", None),
        P(None, "seq", None),
        P("seq", None),
        P("seq"),
        P(None, None, "fsdp"),
        P("fsdp", None),
        P(),
        P(),
    )
    out_specs = (P(("sample", "fsdp"), "seq", None), P(("sample", "fsdp"), None, "seq"))
    return jax.shard_map(
        per_device, mesh=mesh, in_specs=in_specs, out_specs=out_specs, check_vma=False
    )
```

```python
import functools
import math
import types

import jax
import jax.numpy as jnp
from jax import lax
from jax.experimental import pallas as pl
from jax.experimental.pallas import tpu as pltpu
from jax.sharding import PartitionSpec as P

HA = 4
WQ = 32
WK = 128
HD = 48
EPS = 1e-05
FAR = -1e30
RIM = (WK - WQ) // 2
ATOM_MAPS = 7
SQUARE = 4
PARTS = 4
BATCH = 8
VMEM_LIMIT = 56 * 1024 * 1024
MESH = pl.DeviceIdType.MESH


def layer_norm(values):
    values = values.astype(jnp.float32)
    center = values - jnp.mean(values, axis=-1, keepdims=True)
    spread = jnp.mean(center * center, axis=-1, keepdims=True)
    return center * lax.rsqrt(spread + EPS)


def matmul(left_side, right_side):
    return jnp.dot(left_side, right_side, preferred_element_type=jnp.float32)


def matmul_t(left_side, right_side):
    return lax.dot_general(
        left_side, right_side, (((1,), (1,)), ((), ())), preferred_element_type=jnp.float32
    )


def pack(array):
    half = array.shape[-2] // 2
    return jnp.concatenate([array[..., :half, :], array[..., half:, :]], axis=-1)


def unpack(array):
    half = array.shape[-1] // 2
    return jnp.concatenate([array[..., :half], array[..., half:]], axis=-2)


def remote(source, target, send, recv, axis, peer):
    return pltpu.make_async_remote_copy(
        src_ref=source, dst_ref=target, send_sem=send, recv_sem=recv,
        device_id={axis: peer}, device_id_type=MESH,
    )


class Chain:
    def __init__(self, axis, size, view, send, recv, prefix):
        self.axis, self.size, self.view = axis, size, view
        self.send, self.recv, self.prefix = send, recv, prefix
        self.here = lax.axis_index(axis)

    def guards(self, side, step):
        here, last = self.here, self.size - 1
        if side == 0:
            return (here - step >= 0) & (here < last), here - 1 - step >= 0
        return (here + step <= last) & (here > 0), here + 1 + step <= last

    def copy(self, side, step, arriving):
        sign = 1 if side == 0 else -1
        block = self.view(self.here - sign * (step + (1 if arriving else 0)))
        at = self.prefix + (side, step)
        return remote(block, block, self.send.at[at], self.recv.at[at], self.axis, self.here + sign)

    def begin(self):
        for side in (0, 1):

            @pl.when(self.guards(side, 0)[0])
            def _():
                self.copy(side, 0, False).start()

    def arrive(self, step):
        for side in (0, 1):
            comes = self.guards(side, step)[1]

            @pl.when(comes)
            def _():
                self.copy(side, step, True).wait_recv()

            if step + 1 < self.size - 1:

                @pl.when(self.guards(side, step + 1)[0])
                def _():
                    self.copy(side, step + 1, False).start()

    def drain(self):
        for side in (0, 1):
            for step in range(self.size - 1):

                @pl.when(self.guards(side, step)[0])
                def _():
                    self.copy(side, step, False).wait_send()


class Pairs:
    def __init__(self, axis, size, view, send, recv, partner_send, partner_recv, prefix):
        self.axis, self.view, self.prefix = axis, view, prefix
        self.send, self.recv = send, recv
        self.partner_send, self.partner_recv = partner_send, partner_recv
        self.index = lax.axis_index(axis)
        self.length = size // 2
        self.position = self.index // 2
        self.parity = self.index - 2 * self.position

    def slot(self, position):
        return position * 2 + self.parity

    def partner(self):
        return self.index + 1 - 2 * self.parity

    def guards(self, side, step):
        here, last = self.position, self.length - 1
        if side == 0:
            return (here - step >= 0) & (here < last), here - 1 - step >= 0
        return (here + step <= last) & (here > 0), here + 1 + step <= last

    def copy(self, side, step, arriving):
        sign = 1 if side == 0 else -1
        block = self.view(self.slot(self.position - sign * (step + (1 if arriving else 0))))
        at = self.prefix + (side, step)
        return remote(
            block, block, self.send.at[at], self.recv.at[at], self.axis,
            self.slot(self.position + sign),
        )

    def hand(self, key, origin, arriving):
        block = self.view(origin * 2 + 1 - self.parity if arriving else self.slot(origin))
        at = self.prefix + (key,)
        return remote(
            block, block, self.partner_send.at[at], self.partner_recv.at[at], self.axis, self.partner()
        )

    def begin(self):
        for side in (0, 1):

            @pl.when(self.guards(side, 0)[0])
            def _():
                self.copy(side, 0, False).start()

        self.hand(0, self.position, False).start()

    def key(self, side, step):
        return 1 + side * (self.length - 1) + step

    def origin(self, side, step):
        return self.position - (step + 1) if side == 0 else self.position + step + 1

    def relay(self):
        for step in range(self.length - 1):
            for side in (0, 1):

                @pl.when(self.guards(side, step)[1])
                def _():
                    self.copy(side, step, True).wait_recv()
                    self.hand(self.key(side, step), self.origin(side, step), False).start()

                if step + 1 < self.length - 1:

                    @pl.when(self.guards(side, step + 1)[0])
                    def _():
                        self.copy(side, step + 1, False).start()

    def complete(self):
        self.hand(0, self.position, False).wait_send()
        self.hand(0, self.position, True).wait_recv()
        for step in range(self.length - 1):
            for side in (0, 1):
                goes, comes = self.guards(side, step)

                @pl.when(goes)
                def _():
                    self.copy(side, step, False).wait_send()

                @pl.when(comes)
                def _():
                    self.hand(self.key(side, step), self.origin(side, step), False).wait_send()
                    self.hand(self.key(side, step), self.origin(side, step), True).wait_recv()


class Halo:
    def __init__(self, axis, size, pieces, homes, send, recv, number):
        self.axis, self.pieces, self.homes = axis, pieces, homes
        self.send, self.recv, self.number = send, recv, number
        self.index = lax.axis_index(axis)
        self.present = self.index > 0, self.index < size - 1

    def copy(self, side):
        at = (self.number, side)
        return remote(
            self.pieces[side], self.homes[1 - side], self.send.at[at], self.recv.at[at],
            self.axis, self.index - 1 + 2 * side,
        )

    def begin(self):
        for side in (0, 1):
            home = self.homes[side]

            @pl.when(self.present[side])
            def _():
                self.copy(side).start()

            @pl.when(jnp.logical_not(self.present[side]))
            def _():
                home[...] = jnp.zeros(home.shape, home.dtype)

    def finish(self):
        for side in (0, 1):

            @pl.when(self.present[side])
            def _():
                self.copy(side).wait_send()
                self.copy(1 - side).wait_recv()


class Spread:
    def __init__(self, axis, size, view, send, recv, number):
        self.axis, self.size, self.view = axis, size, view
        self.send, self.recv, self.number = send, recv, number
        self.here = lax.axis_index(axis)

    def copy(self, shift, arriving):
        block = self.view(lax.rem(self.here + self.size - shift, self.size) if arriving else self.here)
        at = (self.number, shift)
        peer = lax.rem(self.here + shift, self.size)
        return remote(block, block, self.send.at[at], self.recv.at[at], self.axis, peer)

    def begin(self):
        for shift in range(1, self.size):
            self.copy(shift, False).start()

    def finish(self):
        for shift in range(1, self.size):
            self.copy(shift, False).wait_send()
            self.copy(shift, True).wait_recv()


def token_kernel(names, groups, ring, *refs):
    r = types.SimpleNamespace(**dict(zip(names, refs)))
    me, seat = lax.axis_index("fsdp"), lax.axis_index("seq")
    rows, depth = r.act.shape
    width = r.ada.shape[1]
    heads = r.bias.shape[0]
    half = rows // 2
    part_rows = rows // PARTS
    last = groups - 1
    barrier = pltpu.get_barrier_semaphore()

    def signal(axis, target):
        pl.semaphore_signal(barrier, inc=1, device_id={axis: target}, device_id_type=MESH)

    loads = {
        name: pltpu.make_async_copy(getattr(r, name + "_hbm"), getattr(r, name), r.load.at[number])
        for number, name in enumerate(("ada", "attn", "bias", "out", "tin", "tout", "atom_bias"))
    }
    count, channels = r.skip_hbm.shape
    inner_atoms = pl.ds(RIM, count)
    for number, name in enumerate(("skip", "atom_cond")):
        loads[name] = pltpu.make_async_copy(
            getattr(r, name + "_hbm"), getattr(r, name).at[inner_atoms], r.load.at[len(loads)]
        )

    def pairs(view, *prefix):
        return Pairs("seq", ring, view, r.seq_send, r.seq_recv, r.hand_send, r.hand_recv, prefix)

    halos = [
        Halo(
            "seq", ring, [source.at[pl.ds(start, RIM)] for start in (0, count - RIM)],
            [home.at[pl.ds(start, RIM)] for start in (0, RIM + count)], r.halo_send, r.halo_recv, number,
        )
        for number, (source, home) in enumerate(((r.skip_hbm, r.skip), (r.atom_cond_hbm, r.atom_cond)))
    ]
    halos += [
        Halo(
            "seq", ring, [r.owner_ends.at[0], r.owner_ends.at[r.owner_ends.shape[0] - 1]],
            [r.owner_rims.at[0], r.owner_rims.at[1]], r.halo_send, r.halo_recv, 2,
        )
    ]
    kv_flows = [pairs(lambda slot, g=g: r.kv.at[slot, g], g) for g in range(groups)]
    mask_flow = Spread("seq", ring, lambda slot: r.masks.at[slot], r.spread_send, r.spread_recv, 0)
    rows_flow = Spread("seq", ring, lambda slot: r.rows_all.at[slot], r.spread_send, r.spread_recv, 1)

    for shift in range(1, groups):
        signal("fsdp", lax.rem(me + shift, groups))
    for shift in range(1, ring):
        signal("seq", lax.rem(seat + shift, ring))
    expected = last + ring - 1
    for load in loads.values():
        load.start()

    def chain(number, view):
        return Chain("fsdp", groups, view, r.line_send, r.line_recv, (number,))

    cond_chains = [
        chain(part, lambda slot, part=part: r.conds.at[slot, pl.ds(part * half, half)]) for part in (0, 1)
    ]
    attend_chains = [chain(2 + g, lambda slot, g=g: r.attend.at[slot, g]) for g in range(groups)]
    transit_chains = [
        chain(2 + groups + g, lambda slot, g=g: r.transit.at[slot, g]) for g in range(groups)
    ]
    base = SQUARE * (seat // SQUARE)
    inside = seat - base
    atom_quarter, project_quarter = r.atom_pad.shape[0] // SQUARE, r.project_part.shape[0] // SQUARE

    def quarters(number):
        return (
            pl.ds(pl.multiple_of(number * atom_quarter, 16), atom_quarter),
            pl.ds(pl.multiple_of(number * project_quarter, 16), project_quarter),
        )

    atom_rows, project_rows = quarters(inside)
    small_chains = [
        chain(2 + 2 * groups, lambda slot: r.atom_all.at[slot, atom_rows]),
        chain(3 + 2 * groups, lambda slot: r.project.at[slot, project_rows]),
    ]

    def swaps(shift, arriving):
        peer = base + lax.rem(inside + shift, SQUARE)
        ones, others = quarters(lax.rem(inside + SQUARE - shift, SQUARE) if arriving else inside)
        blocks = (r.atom_all.at[:, ones], r.project.at[:, others])
        return [
            remote(block, block, r.swap_send.at[i, shift], r.swap_recv.at[i, shift], "seq", peer)
            for i, block in enumerate(blocks)
        ]

    r.conds[me] = layer_norm(r.cond[...]).astype(jnp.bfloat16)
    r.masks[seat] = r.mask[...]
    height = r.atom_part.shape[0]
    r.atom_pad[0:height] = r.atom_part[...]
    r.atom_pad[height:] = jnp.zeros((r.atom_pad.shape[0] - height, channels), jnp.bfloat16)
    r.atom_all[me, atom_rows] = r.atom_pad[atom_rows, :]
    r.project[me, project_rows] = r.project_part[project_rows, :]
    pl.semaphore_wait(barrier, expected)
    for flow in cond_chains:
        flow.begin()
    act_normed = layer_norm(r.act[...]).astype(jnp.bfloat16)
    for g in range(groups):
        r.act_out[g] = pack(act_normed[:, g * width : (g + 1) * width])

    def slots(shift, arriving):
        peer = lax.rem(me + shift, groups)
        landing = lax.rem(me + groups - shift, groups) if arriving else me
        return remote(
            r.act_out.at[peer], r.acts.at[landing], r.act_send.at[shift], r.act_recv.at[shift],
            "fsdp", peer,
        )

    for shift in range(1, groups):
        slots(shift, False).start()
    mask_flow.begin()
    for halo in halos:
        halo.begin()
    offsets = r.vectors[:, :width]
    for g in range(1, groups):
        offsets = jnp.where(me == g, r.vectors[:, g * width : (g + 1) * width], offsets)

    def adaptive(sample, packed):
        rows_in = r.conds[sample]
        values = unpack(packed).astype(jnp.float32)

        def one(scale, shift, vector):
            gate = jax.nn.sigmoid(matmul_t(rows_in, r.ada[scale]) + offsets[vector : vector + 1, :])
            return pack((gate * values + matmul_t(rows_in, r.ada[shift])).astype(jnp.bfloat16))

        r.attend[me, sample] = one(0, 1, 0)
        r.transit[me, sample] = one(2, 3, 1)

    loads["ada"].wait()
    adaptive(me, r.act_out[me])
    inner = sorted(range(groups), key=lambda g: max(g, last - g))
    outer = sorted(range(groups), key=lambda g: (-max(g, last - g), g))
    for step in range(last):
        for flow in cond_chains:
            flow.arrive(step)
        for side in (0, 1):

            @pl.when(cond_chains[0].guards(side, step)[1])
            def _():
                origin = me - (step + 1) if side == 0 else me + step + 1
                slots(step + 1 if side == 0 else last - step, True).wait_recv()
                adaptive(origin, r.acts[origin])

        for g in inner:
            if max(g, last - g) == step + 1:
                attend_chains[g].begin()

    def joined(ref, g):
        return jnp.concatenate([unpack(ref[origin, g]) for origin in range(groups)], axis=1)

    def projections(g):
        full = joined(r.attend, g)
        r.queries[g] = (matmul_t(full, r.attn[0]) + offsets[2:3, :]).astype(jnp.bfloat16)
        both = r.attn[1:3].reshape(2 * width, depth)
        r.kv[seat, g] = matmul_t(full, both).astype(jnp.bfloat16)
        kv_flows[g].begin()
        r.gates[g] = matmul_t(full, r.attn[3]).astype(jnp.bfloat16)

    for step in range(last - 1):
        for g in inner:
            attend_chains[g].arrive(step)
    for g in outer[:2]:
        transit_chains[g].begin()
    loads["attn"].wait()
    for g in inner:
        attend_chains[g].arrive(last - 1)
        projections(g)
    for flow in small_chains:
        flow.begin()

    def attention(g):
        queries = r.queries[g]
        head_of = lax.broadcasted_iota(jnp.int32, (rows, width), 1) // HD
        stacked = jnp.concatenate(
            [jnp.where(head_of == head, queries, 0).astype(jnp.bfloat16) for head in range(heads)], axis=0
        )
        scale = 1.0 / math.sqrt(HD)
        span = min(max(512 // rows, 1), ring)

        def block(first, state):
            keys = jnp.concatenate([r.kv[first + i, g, :, :width] for i in range(span)], axis=0)
            values = jnp.concatenate([r.kv[first + i, g, :, width:] for i in range(span)], axis=0)
            live = jnp.concatenate([r.masks[first + i] for i in range(span)], axis=1)
            columns = pl.ds(pl.multiple_of(first * rows, span * rows), span * rows)
            bias = r.bias[:, :, columns].reshape(heads * rows, span * rows).astype(jnp.float32)
            scores = matmul_t(stacked, keys) * scale + bias
            scores = jnp.where(live > 0, scores, FAR)
            block_max = jnp.max(scores, axis=-1, keepdims=True)
            new_maxima = block_max if state is None else jnp.maximum(state[0], block_max)
            weights = jnp.exp(scores - new_maxima)
            totals = jnp.sum(weights, axis=-1, keepdims=True)
            summed = matmul(weights.astype(jnp.bfloat16), values)
            if state is not None:
                factor = jnp.exp(state[0] - new_maxima)
                totals, summed = state[1] * factor + totals, state[2] * factor + summed
            return new_maxima, totals, summed

        state = block(0, None)
        if ring > span:
            state = lax.fori_loop(1, ring // span, lambda i, state: block(i * span, state), state)
        attended = state[2] * (1.0 / state[1])
        result = jnp.zeros((rows, width), jnp.float32)
        for head in range(heads):
            result = result + jnp.where(head_of == head, attended[head * rows : (head + 1) * rows], 0.0)
        gate = jax.nn.sigmoid(r.gates[g].astype(jnp.float32))
        r.gated[g] = (result * gate).astype(jnp.bfloat16)

    mask_flow.finish()
    loads["bias"].wait()
    def hop(side, g, part):
        piece = pl.ds(part * part_rows, part_rows)
        at = (side, g, part)
        return remote(
            r.sums_out.at[g, piece], r.sums_in.at[side, g, piece], r.sum_send.at[at], r.sum_recv.at[at],
            "fsdp", me + (1 if side == 0 else -1),
        )

    def take(side, g, part):
        hop(side, g, part).wait_recv()
        piece = pl.ds(part * part_rows, part_rows)
        r.total[g, piece] += r.sums_in[side, g, piece].astype(jnp.float32)

    def reduce(stage, g):
        for side, here, goes in ((0, stage, g > stage), (1, last - stage, g < last - stage)):
            if goes:

                @pl.when(me == here)
                def _():
                    for part in range(PARTS):
                        piece = pl.ds(part * part_rows, part_rows)
                        if stage > 0:
                            take(side, g, part)
                        r.sums_out[g, piece] = r.total[g, piece].astype(jnp.bfloat16)
                        hop(side, g, part).start()

    heads_out = lax.broadcasted_iota(jnp.int32, (WQ, channels), 1) // (channels // HA)
    tokens = ring * rows

    def atom_weight(i):
        high = r.atom_part.shape[0] // ATOM_MAPS
        return r.atom_all[:, i * high : (i + 1) * high, :].reshape(channels, channels)

    def atom_before():
        normed = layer_norm(r.atom_cond[...]).astype(jnp.bfloat16)
        r.atom_gain[...] = jax.nn.sigmoid(matmul_t(normed, atom_weight(0)) + r.atom_vectors[0:1, :])
        r.atom_shift[...] = matmul_t(normed, atom_weight(1))
        blocks = r.owner.shape[0]

        def hit(column, start):
            span = min(512, tokens)
            for first in range(0, tokens, span):
                token = lax.broadcasted_iota(jnp.int32, (column.shape[0], span), 1) + first
                found = jnp.where(column == token.astype(jnp.float32), 1.0, 0.0).astype(jnp.bfloat16)
                r.hits[pl.ds(start, column.shape[0]), pl.ds(first, span)] = found

        owners = jnp.transpose(r.owner[...].astype(jnp.float32))
        for block in range(blocks):
            hit(owners[:, block : block + 1], RIM + block * WK)
        for side, home in ((0, 0), (1, RIM + count)):
            ends = jnp.broadcast_to(r.owner_rims[side].astype(jnp.float32), (8, WK))
            column = jnp.transpose(ends)[:, 0:1]
            hit(column[WK - RIM :] if side == 0 else column[:RIM], home)
        lane = lax.broadcasted_iota(jnp.int32, (1, WK), 1)

        def window(index, carry):
            base = pl.multiple_of(index * WQ, WQ)
            slot = seat * count + base - RIM + lane
            inside = (slot >= r.bounds[0, index]) & (slot < r.bounds[1, index])
            bias = r.atom_bias[:, pl.ds(base, WQ), :].reshape(HA * WQ, WK).astype(jnp.float32)
            r.masked[index] = jnp.where(inside, bias, FAR)
            return carry

        lax.fori_loop(0, count // WQ, window, 0)

    def atom_after():
        taken = matmul(r.hits[...], r.rows_all[...].reshape(tokens, channels))
        state = r.skip[...].astype(jnp.float32) + taken
        r.state[...] = state[RIM : RIM + count]
        atom_x = (r.atom_gain[...] * layer_norm(state) + r.atom_shift[...]).astype(jnp.bfloat16)
        own_x = atom_x[RIM : RIM + count, :]
        r.atom_query[...] = (matmul_t(own_x, atom_weight(2)) + r.atom_vectors[1:2, :]).astype(jnp.bfloat16)
        r.atom_key[...] = matmul_t(atom_x, atom_weight(3)).astype(jnp.bfloat16)
        r.atom_value[...] = matmul_t(atom_x, atom_weight(4)).astype(jnp.bfloat16)
        r.atom_gate[...] = jax.nn.sigmoid(matmul_t(own_x, atom_weight(5)).astype(jnp.bfloat16).astype(jnp.float32))
        scale = 1.0 / math.sqrt(channels // HA)

        def windows(step, carry):
            bases = [pl.multiple_of(step * (BATCH * WQ) + i * WQ, WQ) for i in range(BATCH)]
            scores = []
            for i, base in enumerate(bases):
                queries = r.atom_query[pl.ds(base, WQ), :]
                stacked = jnp.concatenate(
                    [jnp.where(heads_out == head, queries, 0).astype(jnp.bfloat16) for head in range(HA)],
                    axis=0,
                )
                score = matmul_t(stacked, r.atom_key[pl.ds(base, WK), :])
                scores.append(score * scale + r.masked[step * BATCH + i])
            weights = [jnp.exp(score - jnp.max(score, axis=-1, keepdims=True)) for score in scores]
            results = []
            for base, weight in zip(bases, weights):
                attended = matmul(weight.astype(jnp.bfloat16), r.atom_value[pl.ds(base, WK), :])
                attended = attended * (1.0 / jnp.sum(weight, axis=-1, keepdims=True))
                result = jnp.zeros((WQ, channels), jnp.float32)
                for head in range(HA):
                    result = result + jnp.where(
                        heads_out == head, attended[head * WQ : (head + 1) * WQ], 0.0
                    )
                results.append(result)
            start = pl.multiple_of(step * (BATCH * WQ), BATCH * WQ)
            r.held[pl.ds(start, BATCH * WQ), :] = jnp.concatenate(results, axis=0)
            return carry

        lax.fori_loop(0, count // (BATCH * WQ), windows, 0)
        gated = (r.held[...] * r.atom_gate[...]).astype(jnp.bfloat16)
        fresh = r.state[...] + matmul_t(gated, atom_weight(6))
        final = layer_norm(fresh).astype(jnp.bfloat16)
        moved = matmul_t(r.position[...], final)
        for axis in range(moved.shape[0]):
            r.update[axis] = moved[axis : axis + 1, :]

    for name in ("out", "tin", "tout"):
        loads[name].wait()
    def transition(g):
        full = joined(r.transit, g)
        hidden = jax.nn.silu(matmul(full, r.tin[0])) * matmul(full, r.tin[1])
        r.total[g] = matmul(r.gated[g], r.out[...]) + matmul(hidden.astype(jnp.bfloat16), r.tout[...])
        reduce(0, g)

    def diagonal(number):
        if 2 <= number + 1 < groups:
            transit_chains[outer[number + 1]].begin()
        for step in range(last):
            if 0 <= number - step < groups:
                transit_chains[outer[number - step]].arrive(step)
                if step == last - 1:
                    transition(outer[number - step])
        if 0 <= number - last < last - 1:
            for flow in small_chains:
                flow.arrive(number - last)

    kv_flows[inner[0]].relay()
    diagonal(0)
    for number, g in enumerate(inner):
        if number + 1 < groups:
            kv_flows[inner[number + 1]].relay()
        kv_flows[g].complete()
        attention(g)
        if number + 1 != last - 1:
            diagonal(number + 1 if number + 1 < last - 1 else number)
    for number in range(groups, groups + last - 1):
        diagonal(number)
    for flow in small_chains:
        flow.arrive(last - 1)
    for shift in range(1, SQUARE):
        for copy in swaps(shift, False):
            copy.start()
    for stage in range(1, last):
        for g in outer:
            reduce(stage, g)
    for name in ("skip", "atom_cond", "atom_bias"):
        loads[name].wait()
    for halo in halos:
        halo.finish()
    for shift in range(1, SQUARE):
        for copy in swaps(shift, False):
            copy.wait_send()
        for copy in swaps(shift, True):
            copy.wait_recv()
    atom_before()
    for side, present in ((0, me > 0), (1, me < last)):

        @pl.when(present)
        def _():
            for part in range(PARTS):
                take(side, me, part)

    token = (r.act[...].astype(jnp.float32) + r.total[me]).astype(jnp.bfloat16)
    r.token[...] = token
    r.rows_all[seat] = matmul(token, r.project[...].reshape(depth, -1)).astype(jnp.bfloat16)
    rows_flow.begin()
    for flow in cond_chains + attend_chains + transit_chains + small_chains:
        flow.drain()
    for shift in range(1, groups):
        slots(shift, False).wait_send()
    for g in range(groups):
        for side, goes in ((0, g > me), (1, g < me)):

            @pl.when(goes)
            def _():
                for part in range(PARTS):
                    hop(side, g, part).wait_send()

    rows_flow.finish()
    atom_after()


def token_layer(near, weights, bounds):
    groups, ring = lax.axis_size("fsdp"), lax.axis_size("seq")
    rows, depth = near["act"].shape
    width = weights["ada"].shape[1]
    count, channels = weights["skip"].shape
    extended = count + 2 * RIM
    dma = pltpu.SemaphoreType.DMA
    vmem, far = pl.BlockSpec(memory_space=pltpu.VMEM), pl.BlockSpec(memory_space=pl.ANY)
    half_type = jnp.bfloat16
    project_part, atom_part = near["project_part"], near["atom_part"]
    outs = dict(
        token=((rows, depth), half_type),
        update=((near["position"].shape[0], 1, count), jnp.float32),
    )
    packed = (groups, groups, rows // 2, 2 * width)
    chains = 4 + 2 * groups
    high = atom_part.shape[0] // ATOM_MAPS
    padded = high * SQUARE * -(-ATOM_MAPS // SQUARE)
    hops = max(groups - 1, 1)
    length = ring // 2
    scratch = {name: pltpu.VMEM(array.shape, array.dtype) for name, array in weights.items()}
    atoms = lambda height, kind: pltpu.VMEM((height, channels), kind)
    scratch |= dict(
        skip=atoms(extended, half_type),
        atom_cond=atoms(extended, half_type),
        atom_gain=atoms(extended, jnp.float32),
        atom_shift=atoms(extended, jnp.float32),
        atom_key=atoms(extended, half_type),
        atom_value=atoms(extended, half_type),
        atom_query=atoms(count, half_type),
        atom_gate=atoms(count, jnp.float32),
        state=atoms(count, jnp.float32),
        held=atoms(count, jnp.float32),
        hits=pltpu.VMEM((extended, ring * rows), half_type),
        masked=pltpu.VMEM((count // WQ, HA * WQ, WK), jnp.float32),
        owner_rims=pltpu.VMEM((2, 1, near["owner"].shape[1]), jnp.int32),
        rows_all=pltpu.VMEM((ring, rows, channels), half_type),
        atom_pad=pltpu.VMEM((padded, channels), half_type),
        atom_all=pltpu.VMEM((groups, padded, channels), half_type),
        conds=pltpu.VMEM((groups, rows, depth), half_type),
        act_out=pltpu.VMEM(packed[1:], half_type),
        acts=pltpu.VMEM(packed[1:], half_type),
        attend=pltpu.VMEM(packed, half_type),
        transit=pltpu.VMEM(packed, half_type),
        queries=pltpu.VMEM((groups, rows, width), half_type),
        gates=pltpu.VMEM((groups, rows, width), half_type),
        gated=pltpu.VMEM((groups, rows, width), half_type),
        kv=pltpu.VMEM((ring, groups, rows, 2 * width), half_type),
        masks=pltpu.VMEM((ring, 1, rows), jnp.int32),
        project=pltpu.VMEM((groups,) + project_part.shape, half_type),
        total=pltpu.VMEM((groups, rows, depth), jnp.float32),
        sums_out=pltpu.VMEM((groups, rows, depth), half_type),
        sums_in=pltpu.VMEM((2, groups, rows, depth), half_type),
        load=dma((len(weights),)),
        line_send=dma((chains, 2, hops)),
        line_recv=dma((chains, 2, hops)),
        act_send=dma((groups,)),
        act_recv=dma((groups,)),
        seq_send=dma((groups, 2, max(length - 1, 1))),
        seq_recv=dma((groups, 2, max(length - 1, 1))),
        hand_send=dma((groups, 2 * length)),
        hand_recv=dma((groups, 2 * length)),
        spread_send=dma((2, ring)),
        spread_recv=dma((2, ring)),
        halo_send=dma((3, 2)),
        halo_recv=dma((3, 2)),
        swap_send=dma((2, SQUARE)),
        swap_recv=dma((2, SQUARE)),
        sum_send=dma((2, groups, PARTS)),
        sum_recv=dma((2, groups, PARTS)),
    )
    names = ["bounds"] + list(near) + [name + "_hbm" for name in weights] + list(outs) + list(scratch)
    return pl.pallas_call(
        functools.partial(token_kernel, tuple(names), groups, ring),
        out_shape=tuple(jax.ShapeDtypeStruct(*out) for out in outs.values()),
        in_specs=[pl.BlockSpec(memory_space=pltpu.SMEM)] + [vmem] * len(near) + [far] * len(weights),
        out_specs=tuple([vmem] * len(outs)),
        scratch_shapes=list(scratch.values()),
        compiler_params=pltpu.CompilerParams(
            collective_id=1, has_side_effects=True, vmem_limit_bytes=VMEM_LIMIT
        ),
        name="token_layer",
    )(bounds, *near.values(), *weights.values())


def settle_kernel(token_ref, update_ref, token_out, update_out):
    token_out[...] = token_ref[...]
    update_out[...] = update_ref[...]


def settle(token, update):
    vmem = pl.BlockSpec(memory_space=pltpu.VMEM)
    return pl.pallas_call(
        settle_kernel,
        out_shape=tuple(jax.ShapeDtypeStruct(array.shape, array.dtype) for array in (token, update)),
        in_specs=[vmem] * 2,
        out_specs=(vmem, vmem),
        compiler_params=pltpu.CompilerParams(vmem_limit_bytes=VMEM_LIMIT),
        name="settle",
    )(token, update)


def per_device(
    token_act,
    token_cond,
    pair_bias,
    token_mask,
    ada_weights,
    attention_in,
    attention_out,
    transition_in,
    transition_out,
    token_vectors,
    atom_skip,
    atom_cond,
    atom_bias,
    window_bounds,
    atom_token,
    atom_weights,
    token_to_atom,
    atom_vectors,
    position_out,
):
    channels = atom_cond.shape[1]
    near = dict(
        act=token_act[0],
        cond=token_cond[0],
        mask=token_mask[None],
        vectors=token_vectors,
        owner=atom_token.reshape(-1, WK),
        owner_ends=atom_token.reshape(-1, 1, WK),
        atom_part=jnp.swapaxes(atom_weights, 1, 2).reshape(-1, channels),
        project_part=token_to_atom,
        atom_vectors=atom_vectors,
        position=position_out,
    )
    weights = dict(
        ada=jnp.swapaxes(ada_weights, 1, 2),
        attn=jnp.swapaxes(attention_in, 1, 2),
        bias=pair_bias,
        out=attention_out,
        tin=transition_in,
        tout=transition_out,
        atom_bias=atom_bias,
        skip=atom_skip[0],
        atom_cond=atom_cond,
    )
    token_result, update = settle(*token_layer(near, weights, jnp.swapaxes(window_bounds, 0, 1)))
    return (token_result[None], jnp.transpose(update, (1, 0, 2)))


def solution(mesh):
    in_specs = (
        P(("sample", "fsdp"), "seq", None),
        P(("sample", "fsdp"), "seq", None),
        P("fsdp", "seq", None),
        P("seq"),
        P(None, None, "fsdp"),
        P(None, None, "fsdp"),
        P("fsdp", None),
        P(None, None, "fsdp"),
        P("fsdp", None),
        P(),
        P(("sample", "fsdp"), "seq", None),
        P("seq", None),
        P(None, "seq", None),
        P("seq", None),
        P("seq"),
        P(None, None, "fsdp"),
        P("fsdp", None),
        P(),
        P(),
    )
    out_specs = (P(("sample", "fsdp"), "seq", None), P(("sample", "fsdp"), None, "seq"))
    return jax.shard_map(
        per_device, mesh=mesh, in_specs=in_specs, out_specs=out_specs, check_vma=False
    )
```
